32 devices in a mesh: grp: 4 (over z), sp: 8 (over y, x, core).
Axes of the slice: x: 2, y: 2, z: 4, core: 2. Of those that a mesh axis runs over, the one named last changes fastest.
Arguments:
- tokens: bfloat16 [2048, 2880], P(('grp', 'sp')), may hold values from -36 to 36
- query_weight: bfloat16 [2880, 2048], P(None, 'sp'), may hold values from -0.109375 to 0.109375
- key_value_weight: bfloat16 [2880, 1024], replicated, may hold values from -0.109375 to 0.109375
- block_places: int32 [16], replicated, may hold values from 0 to 15, each once
- sinks: float32 [32], replicated, may hold values from -1 to 5
Outputs:
- attended: bfloat16 [2048, 2048], P(('grp', 'sp'))
The draws below stay inside these ranges and needn't reach their ends.
Inputs may be any that keep to these rules, and one draw needn't show every extreme that they name: `block_places`: every sequence block appears once.
All inputs are finite; a program needn't handle non-finite values.
Results may differ from the reference program's by a relative error of at most 0.008.
The reference program's roundings to bfloat16 on the way count: a program that leaves them out, or rounds other values in their place, can miss the bound.
Values may be sent and summed in bfloat16 or wider, within the bound.
A program may use at most 128 MiB of HBM per device.

```python
import jax
import jax.numpy as jnp
from jax import lax

MODEL_WIDTH = 2880
QUERY_HEADS = 32
KEY_VALUE_HEADS = 8
HEAD_SIZE = 64
BLK = 128
NBLK = 16
SEQUENCE_TOKENS = 2048


def draw_tokens(key, part):
    base = jnp.clip(jax.random.normal(key, (SEQUENCE_TOKENS, MODEL_WIDTH), jnp.float32), -6.0, 6.0)
    return base.astype(jnp.bfloat16)


def block_levels(stream_key, extent, split, smallest, high):
    def one(position, shards_of):
        draws = jax.random.uniform(jax.random.fold_in(jax.random.fold_in(stream_key, 6), position), (shards_of,), jnp.float32, smallest / len(split), high / len(split))
        return jnp.repeat(jnp.exp(draws), extent[position] // shards_of).reshape((-1,) + (1,) * (len(extent) - position - 1))

    loudness = one(*split[0])
    for cut in split[1:]:
        loudness = loudness * one(*cut)
    return loudness


def scatter_about(stream_key, extent, width, most, cuts=(), kind=jnp.bfloat16):
    level = block_levels(stream_key, extent, cuts, -0.22, 0.18) if cuts else 1.0
    entries = jax.random.normal(stream_key, extent, jnp.float32) * width * level
    return jnp.minimum(jnp.maximum(entries, -most), most).astype(kind)


def setup_inputs(seed: int = 0) -> dict:
    keys = jax.random.split(jax.random.key(seed), 6)
    tokens = draw_tokens(jax.random.fold_in(keys[5], 71), 0)
    query_weight = scatter_about(keys[1], (MODEL_WIDTH, QUERY_HEADS * HEAD_SIZE), MODEL_WIDTH ** -0.5, 0.109375, ((1, 8),))
    key_value_weight = scatter_about(keys[2], (MODEL_WIDTH, 2 * KEY_VALUE_HEADS * HEAD_SIZE), MODEL_WIDTH ** -0.5, 0.109375)
    block_places = jax.random.permutation(keys[3], NBLK).astype(jnp.int32)
    sinks = jnp.clip(jax.random.uniform(keys[4], (QUERY_HEADS,), jnp.float32, -1.0, 5.0), -1.0, 5.0)
    return {"tokens": tokens, "query_weight": query_weight, "key_value_weight": key_value_weight, "block_places": block_places, "sinks": sinks}


rope_base = 150000.0
neg_large = -1.0e30


def rotate(vectors, angles):
    middle = vectors.shape[-1] // 2
    first_half = vectors[..., :middle]
    second_half = vectors[..., middle:]
    cosine = jnp.cos(angles)
    sine_part = jnp.sin(angles)
    return jnp.concatenate([first_half * cosine - second_half * sine_part, second_half * cosine + first_half * sine_part], axis=-1)


def reference(tokens, query_weight, key_value_weight, block_places, sinks):
    stored = jnp.arange(SEQUENCE_TOKENS, dtype=jnp.int32)
    blocks = stored // BLK
    places = block_places[blocks] * BLK + stored % BLK
    inverse = rope_base ** (-(jnp.arange(HEAD_SIZE // 2, dtype=jnp.float32) * 2.0) / HEAD_SIZE)
    angles = places.astype(jnp.float32)[:, None, None] * inverse[None, None, :]
    queries = jnp.dot(tokens, query_weight, preferred_element_type=jnp.float32).reshape(SEQUENCE_TOKENS, QUERY_HEADS, HEAD_SIZE)
    key_value_pair = jnp.dot(tokens, key_value_weight, preferred_element_type=jnp.float32)
    key_head_rows = key_value_pair[:, :KEY_VALUE_HEADS * HEAD_SIZE].reshape(SEQUENCE_TOKENS, KEY_VALUE_HEADS, HEAD_SIZE)
    value_head_rows = key_value_pair[:, KEY_VALUE_HEADS * HEAD_SIZE:].reshape(SEQUENCE_TOKENS, KEY_VALUE_HEADS, HEAD_SIZE).astype(jnp.bfloat16)
    queries = rotate(queries, angles).astype(jnp.bfloat16)
    key_head_rows = rotate(key_head_rows, angles).astype(jnp.bfloat16)
    query_sharing = QUERY_HEADS // KEY_VALUE_HEADS
    score_scale = HEAD_SIZE ** -0.5

    def single_head(head_number):
        head_keys = lax.dynamic_index_in_dim(key_head_rows, head_number, 1, keepdims=False).astype(jnp.float32)
        head_values = lax.dynamic_index_in_dim(value_head_rows, head_number, 1, keepdims=False).astype(jnp.float32)
        head_queries = lax.dynamic_slice_in_dim(queries, head_number * query_sharing, query_sharing, 1)
        head_sinks = lax.dynamic_slice_in_dim(sinks, head_number * query_sharing, query_sharing, 0)

        def one_block(query_block):
            first_row = query_block * BLK
            query_rows = lax.dynamic_slice_in_dim(head_queries, first_row, BLK, 0).astype(jnp.float32)
            row_places = lax.dynamic_slice_in_dim(places, first_row, BLK, 0)
            scores = jnp.einsum("qgd,kd->gqk", query_rows, head_keys) * score_scale
            allowed = places[None, :] <= row_places[:, None]
            scores = jnp.where(allowed[None], scores, neg_large)
            highest = jnp.maximum(jnp.max(scores, axis=-1, keepdims=True), head_sinks[:, None, None])
            weights = jnp.where(allowed[None], jnp.exp(scores - highest), 0.0)
            totals = jnp.sum(weights, axis=-1) + jnp.exp(head_sinks[:, None] - highest[..., 0])
            rounded = lax.optimization_barrier(weights.astype(jnp.bfloat16)).astype(jnp.float32)
            mixture = jnp.einsum("gqk,kd->qgd", rounded, head_values)
            return mixture / jnp.transpose(totals)[:, :, None]

        return lax.map(one_block, jnp.arange(SEQUENCE_TOKENS // BLK, dtype=jnp.int32))

    layer_output = lax.map(single_head, jnp.arange(KEY_VALUE_HEADS, dtype=jnp.int32))
    layer_output = jnp.transpose(layer_output, (1, 2, 0, 3, 4)).reshape(SEQUENCE_TOKENS, QUERY_HEADS * HEAD_SIZE)
    return layer_output.astype(jnp.bfloat16)
```

```python
import functools

import jax
import jax.numpy as jnp
from jax import lax
from jax.experimental import pallas as pl
from jax.experimental.pallas import tpu as pltpu
from jax.sharding import PartitionSpec as P

QUERY_HEADS = 32
HEAD_SIZE = 64
BPG = 4
LANES = 128

rope_base = 150000.0
neg_large = -1e30


def rotate_heads(x, cosine, sine):
    width = x.shape[1]
    half = HEAD_SIZE // 2
    if width % LANES:
        swapped = jnp.concatenate([x[:, half:], x[:, :half]], axis=1)
        return x * cosine[:, :width] + swapped * sine[:, :width]
    parts = []
    lane = lax.broadcasted_iota(jnp.int32, (x.shape[0], LANES), 1)
    first = lane % HEAD_SIZE < half
    for j in range(width // LANES):
        v = x[:, j * LANES : (j + 1) * LANES]
        swapped = jnp.where(first, pltpu.roll(v, LANES - half, 1), pltpu.roll(v, half, 1))
        parts.append(v * cosine + swapped * sine)
    return parts[0] if len(parts) == 1 else jnp.concatenate(parts, axis=1)


def kernel(
    grp, sp, qheads, kv_total,
    tok, wq_any, kvw_any, inverse_ref, places_ref, sink, out,
    toks, wq, wkv, kvb, q, abuf, obuf, cos_ref, sin_ref, qpos, kpos,
    wsem, tsend, tfwd, trecv, ksend, krecv, osend, orecv,
):
    s = lax.axis_index("sp")
    g = lax.axis_index("grp")
    rows = tok.shape[0]
    group_rows = rows * sp
    chips = sp // 2
    pair = 2 * rows
    qc = qheads * HEAD_SIZE
    c = s // 2
    par = s % 2
    partner = s + 1 - 2 * par
    head = s * kv_total // sp
    hpar = head % 2
    koff = pl.multiple_of(head // 2 * LANES, LANES)
    voff = pl.multiple_of(kv_total * HEAD_SIZE + head // 2 * LANES, LANES)

    wcopies = [
        pltpu.make_async_copy(wq_any, wq, wsem.at[0]),
        pltpu.make_async_copy(
            kvw_any.at[:, pl.ds(koff, LANES)], wkv.at[:, pl.ds(0, LANES)], wsem.at[1]
        ),
        pltpu.make_async_copy(
            kvw_any.at[:, pl.ds(voff, LANES)], wkv.at[:, pl.ds(LANES, LANES)], wsem.at[2]
        ),
    ]

    def send_tok(to):
        return pltpu.make_async_remote_copy(
            src_ref=tok, dst_ref=toks.at[s], send_sem=tsend.at[to], recv_sem=trecv.at[s],
            device_id={"sp": to},
        )

    def forward(slot):
        return pltpu.make_async_remote_copy(
            src_ref=toks.at[slot], dst_ref=toks.at[slot], send_sem=tfwd.at[slot],
            recv_sem=trecv.at[slot], device_id={"sp": partner},
        )

    def send_kv(chip, d):
        span = pl.ds(pl.multiple_of(g * group_rows + chip * pair, pair), pair)
        return pltpu.make_async_remote_copy(
            src_ref=kvb.at[span], dst_ref=kvb.at[span], send_sem=ksend.at[d, chip],
            recv_sem=krecv.at[g, chip], device_id={"grp": (g + d) % grp},
        )

    def recv_kv(chip, d):
        src = (g + d) % grp
        span = pl.ds(pl.multiple_of(src * group_rows + chip * pair, pair), pair)
        return pltpu.make_async_remote_copy(
            src_ref=kvb.at[span], dst_ref=kvb.at[span], send_sem=ksend.at[d, chip],
            recv_sem=krecv.at[src, chip], device_id={"grp": src},
        )

    def send_out(to):
        return pltpu.make_async_remote_copy(
            src_ref=abuf.at[to], dst_ref=obuf.at[s], send_sem=osend.at[to],
            recv_sem=orecv.at[s], device_id={"sp": to},
        )

    def recv_out(src):
        return pltpu.make_async_remote_copy(
            src_ref=abuf.at[src], dst_ref=obuf.at[src], send_sem=osend.at[src],
            recv_sem=orecv.at[src], device_id={"sp": src},
        )

    send_tok(partner).start()

    def start_tok(k, _):
        send_tok((c + k) % chips * 2 + par).start()
        return 0

    lax.fori_loop(1, chips, start_tok, 0)
    for copy in wcopies:
        copy.start()
    toks[s] = tok[...]

    block_rows = group_rows // BPG
    for j in range(kpos.shape[1] // block_rows):
        within = lax.broadcasted_iota(jnp.int32, (1, block_rows), 1)
        kpos[:, j * block_rows : (j + 1) * block_rows] = places_ref[j] * block_rows + within
    wide = lax.broadcasted_iota(jnp.int32, (1, LANES), 1)
    half = HEAD_SIZE // 2
    inverse = inverse_ref[...]
    sign = jnp.where(wide % HEAD_SIZE < half, -1.0, 1.0)
    for j in range(BPG):
        rspan = slice(j * block_rows, (j + 1) * block_rows)
        within = lax.broadcasted_iota(jnp.int32, (block_rows, LANES), 0)
        place = places_ref[g * BPG + j] * block_rows + within
        qpos[rspan, :] = place[:, :1]
        angles = place.astype(jnp.float32) * inverse
        cos_ref[rspan, :] = jnp.cos(angles)
        sin_ref[rspan, :] = jnp.sin(angles) * sign
    for copy in wcopies:
        copy.wait()

    def project(k, _):
        chip = (c + chips - k) % chips

        @pl.when(k > 0)
        def _():
            slot = chip * 2 + par
            forward(slot).wait_recv()
            forward(slot).start()

        forward(chip * 2 + 1 - par).wait_recv()
        x = toks[pl.ds(chip * 2, 2)].reshape(pair, tok.shape[1])
        span = pl.ds(pl.multiple_of(chip * pair, pair), pair)
        cosine = cos_ref[span, :]
        sine = sin_ref[span, :]
        kv = jnp.dot(x, wkv[...], preferred_element_type=jnp.float32)
        keys = rotate_heads(kv[:, :LANES], cosine, sine)
        values = kv[:, LANES:]
        low = hpar == 0
        keys = jnp.where(low, keys, pltpu.roll(keys, HEAD_SIZE, 1))
        values = jnp.where(low, pltpu.roll(values, HEAD_SIZE, 1), values)
        lane = lax.broadcasted_iota(jnp.int32, (pair, LANES), 1)
        joined = jnp.where(lane < HEAD_SIZE, keys, values).astype(jnp.bfloat16)
        kvb[pl.ds(pl.multiple_of(g * group_rows + chip * pair, pair), pair), :] = joined
        for d in range(1, grp):
            send_kv(chip, d).start()
        qf = jnp.dot(x, wq[...], preferred_element_type=jnp.float32)
        qr = (rotate_heads(qf, cosine, sine) * HEAD_SIZE**-0.5).astype(jnp.bfloat16)
        zeros = jnp.zeros((pair, HEAD_SIZE), jnp.bfloat16)
        for h in range(qheads):
            q[h, span, :] = jnp.concatenate(
                [qr[:, h * HEAD_SIZE : (h + 1) * HEAD_SIZE], zeros], axis=1
            )
        return 0

    lax.fori_loop(0, chips, project, 0)

    def arrive(chip, _):
        for d in range(1, grp):
            recv_kv(chip, d).wait_recv()
        return 0

    lax.fori_loop(0, chips, arrive, 0)

    key_count = kvb.shape[0]
    chunk = min(key_count, 2048)
    chunks = key_count // chunk
    block = min(256, group_rows)
    tiles = block // rows

    def attention(b, _):
        span = pl.ds(pl.multiple_of(b * block, block), block)
        places = qpos[span, :]
        outs = []
        for h in range(qheads):
            qh = q[h, span, :]

            def visit(t, state):
                top, total, mix = state
                kspan = pl.ds(pl.multiple_of(t * chunk, chunk), chunk)
                kv = kvb[kspan, :]
                scores = lax.dot_general(
                    qh, kv, (((1,), (1,)), ((), ())), preferred_element_type=jnp.float32
                )
                allowed = kpos[:, kspan] <= places
                scores = jnp.where(allowed, scores, neg_large)
                higher = jnp.maximum(top, jnp.max(scores, axis=1, keepdims=True))
                weights = jnp.exp(scores - higher)
                factor = jnp.exp(top - higher)
                total = total * factor + jnp.sum(weights, axis=1, keepdims=True)
                mix = mix * factor + jnp.dot(
                    weights.astype(jnp.bfloat16), kv, preferred_element_type=jnp.float32
                )
                return higher, total, mix

            state = (
                jnp.full((block, 1), sink[s * qheads + h], jnp.float32),
                jnp.ones((block, 1), jnp.float32),
                jnp.zeros((block, LANES), jnp.float32),
            )
            if chunks == 1:
                state = visit(0, state)
            else:
                state = lax.fori_loop(0, chunks, visit, state)
            outs.append((state[2] / state[1])[:, HEAD_SIZE:])
        att = outs[0] if qheads == 1 else jnp.concatenate(outs, axis=1)
        abuf[pl.ds(b * tiles, tiles)] = att.astype(jnp.bfloat16).reshape(tiles, rows, qc)

        def ship(i, _):
            to = b * tiles + i

            @pl.when(to != s)
            def _():
                send_out(to).start()

            return 0

        lax.fori_loop(0, tiles, ship, 0)
        return 0

    lax.fori_loop(0, group_rows // block, attention, 0)
    obuf[s] = abuf[s]

    def drain(j, _):
        @pl.when(j != s)
        def _():
            recv_out(j).wait_recv()
            send_out(j).wait_send()

        return 0

    lax.fori_loop(0, sp, drain, 0)
    for j in range(sp):
        out[:, j * qc : (j + 1) * qc] = obuf[j]
    send_tok(partner).wait_send()

    def finish(k, _):
        send_tok((c + k) % chips * 2 + par).wait_send()
        forward((c + chips - k) % chips * 2 + par).wait_send()
        return 0

    lax.fori_loop(1, chips, finish, 0)

    def finish_kv(chip, _):
        for d in range(1, grp):
            send_kv(chip, d).wait_send()
        return 0

    lax.fori_loop(0, chips, finish_kv, 0)


def per_device(tokens, query_weight, key_value_weight, block_places, sinks):
    sp = lax.axis_size("sp")
    grp = lax.axis_size("grp")
    rows, width = tokens.shape
    group_rows = rows * sp
    key_count = grp * group_rows
    qc = query_weight.shape[1]
    qheads = qc // HEAD_SIZE
    kv_total = key_value_weight.shape[1] // (2 * HEAD_SIZE)
    freq = jnp.arange(HEAD_SIZE // 2, dtype=jnp.float32)
    inverse = rope_base ** (-(freq * 2.0) / HEAD_SIZE)
    inverse = jnp.tile(inverse, LANES // (HEAD_SIZE // 2)).reshape(1, LANES)

    vmem = pl.BlockSpec(memory_space=pltpu.VMEM)
    hbm = pl.BlockSpec(memory_space=pl.ANY)
    smem = pl.BlockSpec(memory_space=pltpu.SMEM)
    dma = pltpu.SemaphoreType.DMA
    return pl.pallas_call(
        functools.partial(kernel, grp, sp, qheads, kv_total),
        out_shape=jax.ShapeDtypeStruct((rows, qc * sp), jnp.bfloat16),
        in_specs=[vmem, hbm, hbm, vmem, smem, smem],
        out_specs=vmem,
        scratch_shapes=[
            pltpu.VMEM((sp, rows, width), jnp.bfloat16),
            pltpu.VMEM((width, qc), jnp.bfloat16),
            pltpu.VMEM((width, 2 * LANES), jnp.bfloat16),
            pltpu.VMEM((key_count, LANES), jnp.bfloat16),
            pltpu.VMEM((qheads, group_rows, LANES), jnp.bfloat16),
            pltpu.VMEM((sp, rows, qc), jnp.bfloat16),
            pltpu.VMEM((sp, rows, qc), jnp.bfloat16),
            pltpu.VMEM((group_rows, LANES), jnp.float32),
            pltpu.VMEM((group_rows, LANES), jnp.float32),
            pltpu.VMEM((group_rows, 1), jnp.int32),
            pltpu.VMEM((1, key_count), jnp.int32),
            dma((3,)),
            dma((sp,)),
            dma((sp,)),
            dma((sp,)),
            dma((grp, sp // 2)),
            dma((grp, sp // 2)),
            dma((sp,)),
            dma((sp,)),
        ],
        compiler_params=pltpu.CompilerParams(
            has_side_effects=True, vmem_limit_bytes=60 * 1024 * 1024
        ),
    )(tokens, query_weight, key_value_weight, inverse, block_places, sinks)


def plane_kernel(
    grp, sp, qheads,
    tok_any, wq_any, kvw_any, places, sinks, out,
    toks, wq, kvw, kvo, kvb, kaug, vt, qs, sbuf, pbuf, abuf, obuf, cos_ref, sin_ref, kpos,
    wsem, xsend, ysend, psend, rsend, fsend, trecv, ksend, krecv, zsend, zrecv, osend, orecv,
):
    s = lax.axis_index("sp")
    g = lax.axis_index("grp")
    rows, width = toks.shape[1:]
    pieces = xsend.shape[0]
    piece_rows = rows // pieces
    half = pieces // 2
    pair = 2 * rows
    group_rows = rows * sp
    chips = sp // 2
    qc = qheads * HEAD_SIZE
    blocks = grp * BPG
    dim = HEAD_SIZE // 2
    p = s % 2
    c = s // 2
    cx = c + 1 - 2 * (c % 2)
    cy = (c + chips // 2) % chips
    cd = (cx + chips // 2) % chips
    xn, yn, dn, pn = cx * 2 + p, cy * 2 + p, cd * 2 + p, c * 2 + 1 - p
    key_base = g * group_rows

    chip_order = [cx, cy, cd, c]
    wcopies = []
    for k, chip in enumerate(chip_order):
        koff = pl.multiple_of(chip * LANES, LANES)
        voff = pl.multiple_of(sp * HEAD_SIZE + chip * LANES, LANES)
        wcopies.append([
            pltpu.make_async_copy(
                kvw_any.at[:, pl.ds(off, LANES)],
                kvw.at[k, :, pl.ds(part * LANES, LANES)],
                wsem.at[2 + 2 * k + part],
            )
            for part, off in enumerate((koff, voff))
        ])
    tok_copy = pltpu.make_async_copy(tok_any, toks.at[s], wsem.at[0])
    wq_copy = pltpu.make_async_copy(wq_any, wq, wsem.at[1])
    tok_copy.start()
    for pair_copies in wcopies:
        for copy in pair_copies:
            copy.start()
    wq_copy.start()

    barrier = pltpu.get_barrier_semaphore()
    for to in (xn, yn, dn, pn, cd * 2 + 1 - p, cx * 2 + 1 - p, cy * 2 + 1 - p):
        pl.semaphore_signal(barrier, inc=1, device_id={"sp": to})

    @pl.when(g > 0)
    def _():
        pl.semaphore_signal(barrier, inc=1, device_id={"grp": g - 1})

    @pl.when(g < grp - 1)
    def _():
        pl.semaphore_signal(barrier, inc=1, device_id={"grp": g + 1})

    def send_piece(slot, q, to, sem):
        span = pl.ds(q * piece_rows, piece_rows)
        return pltpu.make_async_remote_copy(
            src_ref=toks.at[slot, span], dst_ref=toks.at[slot, span], send_sem=sem,
            recv_sem=trecv.at[slot, q], device_id={"sp": to},
        )

    def send_own(slot, to):
        return pltpu.make_async_remote_copy(
            src_ref=toks.at[slot], dst_ref=toks.at[slot], send_sem=psend.at[0],
            recv_sem=trecv.at[slot, 0], device_id={"sp": to},
        )

    def send_x(q):
        return send_piece(s, q, xn, xsend.at[q])

    def send_y(q):
        return send_piece(s, q, yn, ysend.at[q])

    def relay(q):
        if q >= half:
            return send_piece(xn, q, yn, rsend.at[q])
        return send_piece(yn, q, xn, rsend.at[q])

    def forward(k, q):
        return send_piece((xn, yn, dn)[k], q, pn, fsend.at[k, q])

    def send_head(i, to):
        span = pl.ds(pl.multiple_of(key_base + s * rows, rows), rows)
        return pltpu.make_async_remote_copy(
            src_ref=kvo.at[i], dst_ref=kvb.at[span], send_sem=ksend.at[i],
            recv_sem=krecv.at[s], device_id={"sp": to},
        )

    def recv_head(src):
        span = pl.ds(pl.multiple_of(key_base + src * rows, rows), rows)
        pltpu.make_async_remote_copy(
            src_ref=kvo.at[0], dst_ref=kvb.at[span], send_sem=ksend.at[0],
            recv_sem=krecv.at[src], device_id={"sp": src},
        ).wait_recv()

    def send_chunk(group, chip, to, way):
        span = pl.ds(pl.multiple_of(group * group_rows + chip * pair, pair), pair)
        return pltpu.make_async_remote_copy(
            src_ref=kvb.at[span], dst_ref=kvb.at[span], send_sem=zsend.at[way, chip],
            recv_sem=zrecv.at[group, chip], device_id={"grp": to},
        )

    def share(chip):
        @pl.when(g > 0)
        def _():
            send_chunk(g, chip, g - 1, 0).start()

        @pl.when(g < grp - 1)
        def _():
            send_chunk(g, chip, g + 1, 1).start()

    inner = jnp.logical_and(g > 0, g < grp - 1)
    others = [g + 1 - 2 * (g % 2), 2 - g // 2, 3 - 3 * (g // 2)]
    targets = [3 - g, 3 * (g // 2), 3 * (g // 2)]

    def recv_group(k):
        for chip in range(chips):
            send_chunk(others[k], chip, targets[k], 2 + k).wait_recv()

            @pl.when(inner)
            def _():
                send_chunk(others[k], chip, targets[k], 2 + k).start()

    wide = lax.broadcasted_iota(jnp.int32, (1, LANES), 1)
    inverse = jnp.ones((1, LANES), jnp.float32)
    bit = 1
    while bit < dim:
        factor = rope_base ** (-2.0 * bit / HEAD_SIZE)
        inverse = jnp.where(wide // bit % 2 == 1, inverse * factor, inverse)
        bit *= 2
    sign = jnp.where(wide % HEAD_SIZE < dim, -1.0, 1.0)
    for j in range(BPG):
        rspan = slice(j * pair, (j + 1) * pair)
        within = lax.broadcasted_iota(jnp.int32, (pair, LANES), 0)
        place = places[g * BPG + j] * pair + within
        kpos[rspan, :] = place
        angles = place.astype(jnp.float32) * inverse
        cos_ref[rspan, :] = jnp.cos(angles)
        sin_ref[rspan, :] = jnp.sin(angles) * sign
    block_place = jnp.full((1, LANES), -1, jnp.int32)
    for e in range(blocks):
        block_place = jnp.where(wide == HEAD_SIZE + e, places[e], block_place)

    tok_copy.wait()
    pl.semaphore_wait(barrier, 7 + jnp.minimum(g, 1) + jnp.minimum(grp - 1 - g, 1))
    send_own(s, pn).start()
    send_x(half).start()
    send_y(0).start()

    own_x = toks[s]
    own_span = pl.ds(pl.multiple_of(s * rows, rows), rows)
    own_cos, own_sin = cos_ref[own_span, :], sin_ref[own_span, :]
    low = lax.broadcasted_iota(jnp.int32, (rows, LANES), 1) < HEAD_SIZE
    for k, chip in enumerate(chip_order):
        for copy in wcopies[k]:
            copy.wait()
        kv = jnp.dot(own_x, kvw[k], preferred_element_type=jnp.float32)
        keys = rotate_heads(kv[:, :LANES], own_cos, own_sin)
        values = kv[:, LANES:]
        first = jnp.where(low, keys, pltpu.roll(values, HEAD_SIZE, 1)).astype(jnp.bfloat16)
        second = jnp.where(low, pltpu.roll(keys, HEAD_SIZE, 1), values).astype(jnp.bfloat16)
        if k < chips - 1:
            kvo[2 * k] = first
            kvo[2 * k + 1] = second
            send_head(2 * k, chip * 2).start()
            send_head(2 * k + 1, chip * 2 + 1).start()
        else:
            mine = p == 0
            kvb[pl.ds(pl.multiple_of(key_base + s * rows, rows), rows), :] = jnp.where(mine, first, second)
            kvo[2 * k] = jnp.where(mine, second, first)
            send_head(2 * k, pn).start()

    for q in range(1, half):
        send_x(half + q).start()
        send_y(q).start()
    for q in range(half):
        send_x(q).start()
        send_y(half + q).start()

    quarter = rows // 2
    units = [
        [(c, 0, 0), (c, 0, quarter), (c, 1, 0), (c, 1, quarter)],
        [(cx, 0, quarter), (cx, 1, quarter), (cy, 0, 0), (cy, 1, 0)],
        [(cx, 0, 0), (cx, 1, 0), (cy, 0, quarter), (cy, 1, quarter)],
        [(cd, 0, 0), (cd, 0, quarter), (cd, 1, 0), (cd, 1, quarter)],
    ]

    def seg_rows(ref, seg):
        chip, core, off = seg
        return ref[pl.ds(pl.multiple_of(chip * pair + core * rows + off, quarter), quarter), :]

    def project(u):
        segs = units[u]
        x = jnp.concatenate([toks[chip * 2 + core, off : off + quarter] for chip, core, off in segs], axis=0)
        cosine = jnp.concatenate([seg_rows(cos_ref, seg) for seg in segs], axis=0)
        sine = jnp.concatenate([seg_rows(sin_ref, seg) for seg in segs], axis=0)
        qf = jnp.dot(x, wq[...], preferred_element_type=jnp.float32)
        qr = rotate_heads(qf, cosine, sine) * HEAD_SIZE**-0.5
        hidden = jnp.concatenate([
            jnp.broadcast_to(
                jnp.where(block_place > places[g * BPG + chip], neg_large, 0.0), (quarter, LANES)
            )
            for chip, _, _ in segs
        ], axis=0)
        lower = lax.broadcasted_iota(jnp.int32, (pair, LANES), 1) < HEAD_SIZE
        for h in range(qheads):
            v = qr[:, h // 2 * LANES : (h // 2 + 1) * LANES]
            if h % 2:
                v = pltpu.roll(v, HEAD_SIZE, 1)
            qs[u, h * pair : (h + 1) * pair, :] = jnp.where(lower, v, hidden).astype(jnp.bfloat16)

    def query_places(u):
        lane = lax.broadcasted_iota(jnp.int32, (1, pair), 1)
        place = jnp.zeros((1, pair), jnp.int32)
        for i, (chip, core, off) in enumerate(units[u]):
            base = places[g * BPG + chip] * pair + core * rows + off
            place = jnp.where(lane // quarter == i, base + lane % quarter, place)
        return place

    def prepare(k):
        group = g if k == 0 else others[k - 1]
        lane = lax.broadcasted_iota(jnp.int32, (pair, LANES), 1)
        for j in range(chips):
            kv = kvb[pl.ds(pl.multiple_of(group * group_rows + j * pair, pair), pair), :]
            mark = jnp.where(lane == HEAD_SIZE + group * BPG + j, 1.0, 0.0).astype(jnp.bfloat16)
            span = slice(k * group_rows + j * pair, k * group_rows + (j + 1) * pair)
            kaug[span, :] = jnp.where(lane < HEAD_SIZE, kv, mark)
            vt[:, span] = jnp.transpose(kv)[HEAD_SIZE:]

    sink_row = jnp.concatenate(
        [jnp.full((1, pair), sinks[s * qheads + h], jnp.float32) for h in range(qheads)], axis=1
    )
    tops = [sink_row for _ in units]

    def score(u, k):
        for j in range(0, chips, 2):
            span = slice(k * group_rows + j * pair, k * group_rows + (j + 2) * pair)
            part = lax.dot_general(
                kaug[span, :], qs[u], (((1,), (1,)), ((), ())), preferred_element_type=jnp.float32
            )
            if k == 0:
                seen = kpos[j * pair : (j + 2) * pair, :] <= query_places(u)
                part = jnp.where(jnp.concatenate([seen] * qheads, axis=1), part, neg_large)
            sbuf[u, span, :] = part
            tops[u] = jnp.maximum(tops[u], jnp.max(part, axis=0, keepdims=True))

    def send_out(u, i):
        chip, core, off = units[u][i]
        count = rows if u in (0, 3) else quarter
        src = abuf.at[u, pl.ds(i * quarter, count)]
        dst = obuf.at[pl.ds(off, count), pl.ds(pl.multiple_of(s * qc, qc), qc)]
        return pltpu.make_async_remote_copy(
            src_ref=src, dst_ref=dst, send_sem=osend.at[u, i],
            recv_sem=orecv.at[s, u // 2], device_id={"sp": chip * 2 + core},
        )

    def send_out_partner():
        src = abuf.at[0, pl.ds(pl.multiple_of((1 - p) * rows, rows), rows)]
        dst = obuf.at[:, pl.ds(pl.multiple_of(s * qc, qc), qc)]
        return pltpu.make_async_remote_copy(
            src_ref=src, dst_ref=dst, send_sem=osend.at[0, 0],
            recv_sem=orecv.at[s, 0], device_id={"sp": pn},
        )

    def recv_out(src, off, count, part):
        dst = obuf.at[pl.ds(off, count), pl.ds(pl.multiple_of(src * qc, qc), qc)]
        pltpu.make_async_remote_copy(
            src_ref=abuf.at[0, pl.ds(0, count)], dst_ref=dst, send_sem=osend.at[0, 0],
            recv_sem=orecv.at[src, part], device_id={"sp": src},
        ).wait_recv()

    def attend(u):
        top = tops[u]
        total = jnp.exp(sink_row - top)
        keys = sbuf.shape[1]
        step = 2 * pair
        for j in range(0, keys, step):
            weights = jnp.exp(sbuf[u, j : j + step, :] - top)
            pbuf[j : j + step, :] = weights.astype(jnp.bfloat16)
            total = total + jnp.sum(weights, axis=0, keepdims=True)
        mix = jnp.dot(vt[...], pbuf[...], preferred_element_type=jnp.float32) / total
        heads = [jnp.transpose(mix[:, h * pair : (h + 1) * pair]) for h in range(qheads)]
        abuf[u] = jnp.concatenate(heads, axis=1).astype(jnp.bfloat16)

    def ship(u):
        if u == 0:
            send_out_partner().start()
            obuf[:, pl.ds(pl.multiple_of(s * qc, qc), qc)] = abuf[
                0, pl.ds(pl.multiple_of(p * rows, rows), rows), :
            ]
        elif u == 3:
            send_out(u, 0).start()
            send_out(u, 2).start()
        else:
            for i in range(4):
                send_out(u, i).start()

    def stage(k):
        qx, qy = (k + half) % pieces, k
        forward(0, qx).wait_recv()
        if k < half:
            relay(qx).start()
        forward(0, qx).start()
        forward(1, qy).wait_recv()
        if k < half:
            relay(qy).start()
        forward(1, qy).start()

    def stage_partner(k):
        qx, qy = (k + half) % pieces, k
        send_piece(cx * 2 + 1 - p, qx, pn, fsend.at[0, qx]).wait_recv()
        send_piece(cy * 2 + 1 - p, qy, pn, fsend.at[1, qy]).wait_recv()

    def stage_far(q):
        for r in (q, q + half):
            forward(2, r).wait_recv()
            forward(2, r).start()

    def stage_far_partner(q):
        for r in (q, q + half):
            send_piece(cd * 2 + 1 - p, r, pn, fsend.at[2, r]).wait_recv()

    send_own(pn, pn).wait_recv()
    wq_copy.wait()
    project(0)
    recv_head(pn)
    share(c)
    stage(0)
    for chip in (cx, cy, cd):
        recv_head(chip * 2)
        recv_head(chip * 2 + 1)
        share(chip)
    prepare(0)
    score(0, 0)
    stage(1)
    recv_group(0)
    prepare(1)
    score(0, 1)
    for k in range(half):
        stage_partner(k)
    project(1)
    score(1, 0)
    score(1, 1)
    stage(2)
    recv_group(1)
    prepare(2)
    score(0, 2)
    score(1, 2)
    stage(3)
    for k in range(half, pieces):
        stage_partner(k)
    project(2)
    score(2, 0)
    score(2, 1)
    score(2, 2)
    recv_group(2)
    prepare(3)
    score(0, 3)
    score(1, 3)
    score(2, 3)
    stage_far(0)
    attend(0)
    ship(0)
    attend(1)
    ship(1)
    stage_far(1)
    attend(2)
    ship(2)
    for q in range(half):
        stage_far_partner(q)
    project(3)
    for k in range(grp):
        score(3, k)
    attend(3)
    ship(3)

    recv_out(pn, 0, rows, 0)
    for core in range(2):
        recv_out(cx * 2 + core, quarter, quarter, 0)
        recv_out(cy * 2 + core, 0, quarter, 0)
        recv_out(cx * 2 + core, 0, quarter, 1)
        recv_out(cy * 2 + core, quarter, quarter, 1)
        recv_out(cd * 2 + core, 0, rows, 1)
    out[...] = obuf[...]
    send_own(s, pn).wait_send()
    for q in range(pieces):
        send_x(q).wait_send()
        send_y(q).wait_send()
        relay(q).wait_send()
        for k in range(3):
            forward(k, q).wait_send()
    for i in range(sp - 1):
        send_head(i, pn).wait_send()
    for chip in range(chips):

        @pl.when(g > 0)
        def _():
            send_chunk(g, chip, g - 1, 0).wait_send()

        @pl.when(g < grp - 1)
        def _():
            send_chunk(g, chip, g + 1, 1).wait_send()

        @pl.when(inner)
        def _():
            for k in range(3):
                send_chunk(others[k], chip, targets[k], 2 + k).wait_send()

    send_out_partner().wait_send()
    for i in range(4):
        send_out(1, i).wait_send()
        send_out(2, i).wait_send()
    send_out(3, 0).wait_send()
    send_out(3, 2).wait_send()


def per_plane(tokens, query_weight, key_value_weight, block_places, sinks):
    sp = lax.axis_size("sp")
    grp = lax.axis_size("grp")
    rows, width = tokens.shape
    group_rows = rows * sp
    key_count = grp * group_rows
    qc = query_weight.shape[1]
    qheads = qc // HEAD_SIZE
    pair = 2 * rows
    columns = qheads * pair
    pieces = 4
    hbm = pl.BlockSpec(memory_space=pl.ANY)
    smem = pl.BlockSpec(memory_space=pltpu.SMEM)
    dma = pltpu.SemaphoreType.DMA
    bf16, f32 = jnp.bfloat16, jnp.float32
    return pl.pallas_call(
        functools.partial(plane_kernel, grp, sp, qheads),
        out_shape=jax.ShapeDtypeStruct((rows, qc * sp), bf16),
        in_specs=[hbm, hbm, hbm, smem, smem],
        out_specs=pl.BlockSpec(memory_space=pltpu.VMEM),
        scratch_shapes=[
            pltpu.VMEM((sp, rows, width), bf16),
            pltpu.VMEM((width, qc), bf16),
            pltpu.VMEM((sp // 2, width, 2 * LANES), bf16),
            pltpu.VMEM((sp, rows, LANES), bf16),
            pltpu.VMEM((key_count, LANES), bf16),
            pltpu.VMEM((key_count, LANES), bf16),
            pltpu.VMEM((HEAD_SIZE, key_count), bf16),
            pltpu.VMEM((sp // 2, columns, LANES), bf16),
            pltpu.VMEM((sp // 2, key_count, columns), f32),
            pltpu.VMEM((key_count, columns), bf16),
            pltpu.VMEM((sp // 2, pair, qc), bf16),
            pltpu.VMEM((rows, qc * sp), bf16),
            pltpu.VMEM((group_rows, LANES), f32),
            pltpu.VMEM((group_rows, LANES), f32),
            pltpu.VMEM((group_rows, LANES), jnp.int32),
            dma((2 + sp,)),
            dma((pieces,)),
            dma((pieces,)),
            dma((1,)),
            dma((pieces,)),
            dma((3, pieces)),
            dma((sp, pieces)),
            dma((sp,)),
            dma((sp,)),
            dma((5, sp // 2)),
            dma((grp, sp // 2)),
            dma((4, 4)),
            dma((sp, 2)),
        ],
        compiler_params=pltpu.CompilerParams(
            has_side_effects=True, collective_id=0, vmem_limit_bytes=60 * 1024 * 1024
        ),
    )(tokens, query_weight, key_value_weight, block_places, sinks)


def local_form(tokens, query_weight, key_value_weight, block_places, sinks):
    sp = lax.axis_size("sp")
    grp = lax.axis_size("grp")
    heads = query_weight.shape[1] // HEAD_SIZE
    kv_total = key_value_weight.shape[1] // (2 * HEAD_SIZE)
    square = sp // 2 == BPG and grp == BPG and kv_total == sp and block_places.shape[0] == grp * BPG
    form = per_plane if square and heads * HEAD_SIZE == 2 * LANES else per_device
    return form(tokens, query_weight, key_value_weight, block_places, sinks)


def solution(mesh):
    in_specs = (P(("grp", "sp"), None), P(None, "sp"), P(), P(), P())
    out_specs = P(("grp", "sp"), None)
    return jax.shard_map(
        local_form, mesh=mesh, in_specs=in_specs, out_specs=out_specs, check_vma=False
    )
```

```python
import functools

import jax
import jax.numpy as jnp
from jax import lax
from jax.experimental import pallas as pl
from jax.experimental.pallas import tpu as pltpu
from jax.sharding import PartitionSpec as P

QUERY_HEADS = 32
HEAD_SIZE = 64
BPG = 4
LANES = 128

rope_base = 150000.0
neg_large = -1e30


def rotate_heads(x, cosine, sine):
    width = x.shape[1]
    half = HEAD_SIZE // 2
    if width % LANES:
        swapped = jnp.concatenate([x[:, half:], x[:, :half]], axis=1)
        return x * cosine[:, :width] + swapped * sine[:, :width]
    parts = []
    lane = lax.broadcasted_iota(jnp.int32, (x.shape[0], LANES), 1)
    first = lane % HEAD_SIZE < half
    for j in range(width // LANES):
        v = x[:, j * LANES : (j + 1) * LANES]
        swapped = jnp.where(first, pltpu.roll(v, LANES - half, 1), pltpu.roll(v, half, 1))
        parts.append(v * cosine + swapped * sine)
    return parts[0] if len(parts) == 1 else jnp.concatenate(parts, axis=1)


def kernel(
    grp, sp, qheads, kv_total,
    tok, wq_any, kvw_any, inverse_ref, places_ref, sink, out,
    toks, wq, wkv, kvb, q, abuf, obuf, cos_ref, sin_ref, qpos, kpos,
    wsem, tsend, tfwd, trecv, ksend, krecv, osend, orecv,
):
    s = lax.axis_index("sp")
    g = lax.axis_index("grp")
    rows = tok.shape[0]
    group_rows = rows * sp
    chips = sp // 2
    pair = 2 * rows
    qc = qheads * HEAD_SIZE
    c = s // 2
    par = s % 2
    partner = s + 1 - 2 * par
    head = s * kv_total // sp
    hpar = head % 2
    koff = pl.multiple_of(head // 2 * LANES, LANES)
    voff = pl.multiple_of(kv_total * HEAD_SIZE + head // 2 * LANES, LANES)

    wcopies = [
        pltpu.make_async_copy(wq_any, wq, wsem.at[0]),
        pltpu.make_async_copy(
            kvw_any.at[:, pl.ds(koff, LANES)], wkv.at[:, pl.ds(0, LANES)], wsem.at[1]
        ),
        pltpu.make_async_copy(
            kvw_any.at[:, pl.ds(voff, LANES)], wkv.at[:, pl.ds(LANES, LANES)], wsem.at[2]
        ),
    ]

    def send_tok(to):
        return pltpu.make_async_remote_copy(
            src_ref=tok, dst_ref=toks.at[s], send_sem=tsend.at[to], recv_sem=trecv.at[s],
            device_id={"sp": to},
        )

    def forward(slot):
        return pltpu.make_async_remote_copy(
            src_ref=toks.at[slot], dst_ref=toks.at[slot], send_sem=tfwd.at[slot],
            recv_sem=trecv.at[slot], device_id={"sp": partner},
        )

    def send_kv(chip, d):
        span = pl.ds(pl.multiple_of(g * group_rows + chip * pair, pair), pair)
        return pltpu.make_async_remote_copy(
            src_ref=kvb.at[span], dst_ref=kvb.at[span], send_sem=ksend.at[d, chip],
            recv_sem=krecv.at[g, chip], device_id={"grp": (g + d) % grp},
        )

    def recv_kv(chip, d):
        src = (g + d) % grp
        span = pl.ds(pl.multiple_of(src * group_rows + chip * pair, pair), pair)
        return pltpu.make_async_remote_copy(
            src_ref=kvb.at[span], dst_ref=kvb.at[span], send_sem=ksend.at[d, chip],
            recv_sem=krecv.at[src, chip], device_id={"grp": src},
        )

    def send_out(to):
        return pltpu.make_async_remote_copy(
            src_ref=abuf.at[to], dst_ref=obuf.at[s], send_sem=osend.at[to],
            recv_sem=orecv.at[s], device_id={"sp": to},
        )

    def recv_out(src):
        return pltpu.make_async_remote_copy(
            src_ref=abuf.at[src], dst_ref=obuf.at[src], send_sem=osend.at[src],
            recv_sem=orecv.at[src], device_id={"sp": src},
        )

    send_tok(partner).start()

    def start_tok(k, _):
        send_tok((c + k) % chips * 2 + par).start()
        return 0

    lax.fori_loop(1, chips, start_tok, 0)
    for copy in wcopies:
        copy.start()
    toks[s] = tok[...]

    block_rows = group_rows // BPG
    for j in range(kpos.shape[1] // block_rows):
        within = lax.broadcasted_iota(jnp.int32, (1, block_rows), 1)
        kpos[:, j * block_rows : (j + 1) * block_rows] = places_ref[j] * block_rows + within
    wide = lax.broadcasted_iota(jnp.int32, (1, LANES), 1)
    half = HEAD_SIZE // 2
    inverse = inverse_ref[...]
    sign = jnp.where(wide % HEAD_SIZE < half, -1.0, 1.0)
    for j in range(BPG):
        rspan = slice(j * block_rows, (j + 1) * block_rows)
        within = lax.broadcasted_iota(jnp.int32, (block_rows, LANES), 0)
        place = places_ref[g * BPG + j] * block_rows + within
        qpos[rspan, :] = place[:, :1]
        angles = place.astype(jnp.float32) * inverse
        cos_ref[rspan, :] = jnp.cos(angles)
        sin_ref[rspan, :] = jnp.sin(angles) * sign
    for copy in wcopies:
        copy.wait()

    def project(k, _):
        chip = (c + chips - k) % chips

        @pl.when(k > 0)
        def _():
            slot = chip * 2 + par
            forward(slot).wait_recv()
            forward(slot).start()

        forward(chip * 2 + 1 - par).wait_recv()
        x = toks[pl.ds(chip * 2, 2)].reshape(pair, tok.shape[1])
        span = pl.ds(pl.multiple_of(chip * pair, pair), pair)
        cosine = cos_ref[span, :]
        sine = sin_ref[span, :]
        kv = jnp.dot(x, wkv[...], preferred_element_type=jnp.float32)
        keys = rotate_heads(kv[:, :LANES], cosine, sine)
        values = kv[:, LANES:]
        low = hpar == 0
        keys = jnp.where(low, keys, pltpu.roll(keys, HEAD_SIZE, 1))
        values = jnp.where(low, pltpu.roll(values, HEAD_SIZE, 1), values)
        lane = lax.broadcasted_iota(jnp.int32, (pair, LANES), 1)
        joined = jnp.where(lane < HEAD_SIZE, keys, values).astype(jnp.bfloat16)
        kvb[pl.ds(pl.multiple_of(g * group_rows + chip * pair, pair), pair), :] = joined
        for d in range(1, grp):
            send_kv(chip, d).start()
        qf = jnp.dot(x, wq[...], preferred_element_type=jnp.float32)
        qr = (rotate_heads(qf, cosine, sine) * HEAD_SIZE**-0.5).astype(jnp.bfloat16)
        zeros = jnp.zeros((pair, HEAD_SIZE), jnp.bfloat16)
        for h in range(qheads):
            q[h, span, :] = jnp.concatenate(
                [qr[:, h * HEAD_SIZE : (h + 1) * HEAD_SIZE], zeros], axis=1
            )
        return 0

    lax.fori_loop(0, chips, project, 0)

    def arrive(chip, _):
        for d in range(1, grp):
            recv_kv(chip, d).wait_recv()
        return 0

    lax.fori_loop(0, chips, arrive, 0)

    key_count = kvb.shape[0]
    chunk = min(key_count, 2048)
    chunks = key_count // chunk
    block = min(256, group_rows)
    tiles = block // rows

    def attention(b, _):
        span = pl.ds(pl.multiple_of(b * block, block), block)
        places = qpos[span, :]
        outs = []
        for h in range(qheads):
            qh = q[h, span, :]

            def visit(t, state):
                top, total, mix = state
                kspan = pl.ds(pl.multiple_of(t * chunk, chunk), chunk)
                kv = kvb[kspan, :]
                scores = lax.dot_general(
                    qh, kv, (((1,), (1,)), ((), ())), preferred_element_type=jnp.float32
                )
                allowed = kpos[:, kspan] <= places
                scores = jnp.where(allowed, scores, neg_large)
                higher = jnp.maximum(top, jnp.max(scores, axis=1, keepdims=True))
                weights = jnp.exp(scores - higher)
                factor = jnp.exp(top - higher)
                total = total * factor + jnp.sum(weights, axis=1, keepdims=True)
                mix = mix * factor + jnp.dot(
                    weights.astype(jnp.bfloat16), kv, preferred_element_type=jnp.float32
                )
                return higher, total, mix

            state = (
                jnp.full((block, 1), sink[s * qheads + h], jnp.float32),
                jnp.ones((block, 1), jnp.float32),
                jnp.zeros((block, LANES), jnp.float32),
            )
            if chunks == 1:
                state = visit(0, state)
            else:
                state = lax.fori_loop(0, chunks, visit, state)
            outs.append((state[2] / state[1])[:, HEAD_SIZE:])
        att = outs[0] if qheads == 1 else jnp.concatenate(outs, axis=1)
        abuf[pl.ds(b * tiles, tiles)] = att.astype(jnp.bfloat16).reshape(tiles, rows, qc)

        def ship(i, _):
            to = b * tiles + i

            @pl.when(to != s)
            def _():
                send_out(to).start()

            return 0

        lax.fori_loop(0, tiles, ship, 0)
        return 0

    lax.fori_loop(0, group_rows // block, attention, 0)
    obuf[s] = abuf[s]

    def drain(j, _):
        @pl.when(j != s)
        def _():
            recv_out(j).wait_recv()
            send_out(j).wait_send()

        return 0

    lax.fori_loop(0, sp, drain, 0)
    for j in range(sp):
        out[:, j * qc : (j + 1) * qc] = obuf[j]
    send_tok(partner).wait_send()

    def finish(k, _):
        send_tok((c + k) % chips * 2 + par).wait_send()
        forward((c + chips - k) % chips * 2 + par).wait_send()
        return 0

    lax.fori_loop(1, chips, finish, 0)

    def finish_kv(chip, _):
        for d in range(1, grp):
            send_kv(chip, d).wait_send()
        return 0

    lax.fori_loop(0, chips, finish_kv, 0)


def per_device(tokens, query_weight, key_value_weight, block_places, sinks):
    sp = lax.axis_size("sp")
    grp = lax.axis_size("grp")
    rows, width = tokens.shape
    group_rows = rows * sp
    key_count = grp * group_rows
    qc = query_weight.shape[1]
    qheads = qc // HEAD_SIZE
    kv_total = key_value_weight.shape[1] // (2 * HEAD_SIZE)
    freq = jnp.arange(HEAD_SIZE // 2, dtype=jnp.float32)
    inverse = rope_base ** (-(freq * 2.0) / HEAD_SIZE)
    inverse = jnp.tile(inverse, LANES // (HEAD_SIZE // 2)).reshape(1, LANES)

    vmem = pl.BlockSpec(memory_space=pltpu.VMEM)
    hbm = pl.BlockSpec(memory_space=pl.ANY)
    smem = pl.BlockSpec(memory_space=pltpu.SMEM)
    dma = pltpu.SemaphoreType.DMA
    return pl.pallas_call(
        functools.partial(kernel, grp, sp, qheads, kv_total),
        out_shape=jax.ShapeDtypeStruct((rows, qc * sp), jnp.bfloat16),
        in_specs=[vmem, hbm, hbm, vmem, smem, smem],
        out_specs=vmem,
        scratch_shapes=[
            pltpu.VMEM((sp, rows, width), jnp.bfloat16),
            pltpu.VMEM((width, qc), jnp.bfloat16),
            pltpu.VMEM((width, 2 * LANES), jnp.bfloat16),
            pltpu.VMEM((key_count, LANES), jnp.bfloat16),
            pltpu.VMEM((qheads, group_rows, LANES), jnp.bfloat16),
            pltpu.VMEM((sp, rows, qc), jnp.bfloat16),
            pltpu.VMEM((sp, rows, qc), jnp.bfloat16),
            pltpu.VMEM((group_rows, LANES), jnp.float32),
            pltpu.VMEM((group_rows, LANES), jnp.float32),
            pltpu.VMEM((group_rows, 1), jnp.int32),
            pltpu.VMEM((1, key_count), jnp.int32),
            dma((3,)),
            dma((sp,)),
            dma((sp,)),
            dma((sp,)),
            dma((grp, sp // 2)),
            dma((grp, sp // 2)),
            dma((sp,)),
            dma((sp,)),
        ],
        compiler_params=pltpu.CompilerParams(
            has_side_effects=True, vmem_limit_bytes=60 * 1024 * 1024
        ),
    )(tokens, query_weight, key_value_weight, inverse, block_places, sinks)


def plane_kernel(
    grp, sp, qheads,
    tok_any, wq_any, kvw_any, places_any, sinks_any, out,
    places, sinks,    toks, wq, kvw, kvo, kvb, kaug, vt, qs, sbuf, pbuf, mbuf, abuf, obuf, cos_ref, sin_ref, kpos,
    wsem, xsend, ysend, psend, rsend, fsend, trecv, ksend, krecv, zsend, zrecv, osend, orecv,
):
    s = lax.axis_index("sp")
    g = lax.axis_index("grp")
    rows, width = toks.shape[1:]
    pieces = xsend.shape[0]
    piece_rows = rows // pieces
    half = pieces // 2
    pair = 2 * rows
    group_rows = rows * sp
    chips = sp // 2
    qc = qheads * HEAD_SIZE
    blocks = grp * BPG
    dim = HEAD_SIZE // 2
    p = s % 2
    c = s // 2
    cx = c + 1 - 2 * (c % 2)
    cy = (c + chips // 2) % chips
    cd = (cx + chips // 2) % chips
    xn, yn, dn, pn = cx * 2 + p, cy * 2 + p, cd * 2 + p, c * 2 + 1 - p
    key_base = g * group_rows

    chip_order = [c, cd, cx, cy]
    wcopies = []
    for k, chip in enumerate(chip_order):
        koff = pl.multiple_of(chip * LANES, LANES)
        voff = pl.multiple_of(sp * HEAD_SIZE + chip * LANES, LANES)
        wcopies.append([
            pltpu.make_async_copy(
                kvw_any.at[:, pl.ds(off, LANES)],
                kvw.at[k // 2, :, pl.ds((2 * (k % 2) + part) * LANES, LANES)],
                wsem.at[2 + 2 * k + part],
            )
            for part, off in enumerate((koff, voff))
        ])
    tok_copy = pltpu.make_async_copy(tok_any, toks.at[s], wsem.at[0])
    wq_copy = pltpu.make_async_copy(wq_any, wq, wsem.at[1])
    pcopy = pltpu.make_async_copy(places_any, places, wsem.at[2 + sp])
    scopy = pltpu.make_async_copy(sinks_any, sinks, wsem.at[3 + sp])
    pcopy.start()
    scopy.start()
    tok_copy.start()
    for pair_copies in wcopies:
        for copy in pair_copies:
            copy.start()
    wq_copy.start()

    barrier = pltpu.get_barrier_semaphore()
    for to in (xn, yn, dn, pn, cd * 2 + 1 - p, cx * 2 + 1 - p, cy * 2 + 1 - p):
        pl.semaphore_signal(barrier, inc=1, device_id={"sp": to})

    @pl.when(g > 0)
    def _():
        pl.semaphore_signal(barrier, inc=1, device_id={"grp": g - 1})

    @pl.when(g < grp - 1)
    def _():
        pl.semaphore_signal(barrier, inc=1, device_id={"grp": g + 1})

    def send_piece(slot, q, to, sem):
        span = pl.ds(q * piece_rows, piece_rows)
        return pltpu.make_async_remote_copy(
            src_ref=toks.at[slot, span], dst_ref=toks.at[slot, span], send_sem=sem,
            recv_sem=trecv.at[slot, q], device_id={"sp": to},
        )

    def send_own(slot, to):
        return pltpu.make_async_remote_copy(
            src_ref=toks.at[slot], dst_ref=toks.at[slot], send_sem=psend.at[0],
            recv_sem=trecv.at[slot, 0], device_id={"sp": to},
        )

    def send_x(q):
        return send_piece(s, q, xn, xsend.at[q])

    def send_y(q):
        return send_piece(s, q, yn, ysend.at[q])

    def relay(q):
        if q >= half:
            return send_piece(xn, q, yn, rsend.at[q])
        return send_piece(yn, q, xn, rsend.at[q])

    def forward(k, q):
        return send_piece((xn, yn, dn)[k], q, pn, fsend.at[k, q])

    def send_head(i, to):
        span = pl.ds(pl.multiple_of(key_base + s * rows, rows), rows)
        return pltpu.make_async_remote_copy(
            src_ref=kvo.at[i], dst_ref=kvb.at[span], send_sem=ksend.at[i],
            recv_sem=krecv.at[s], device_id={"sp": to},
        )

    def recv_head(src):
        span = pl.ds(pl.multiple_of(key_base + src * rows, rows), rows)
        pltpu.make_async_remote_copy(
            src_ref=kvo.at[0], dst_ref=kvb.at[span], send_sem=ksend.at[0],
            recv_sem=krecv.at[src], device_id={"sp": src},
        ).wait_recv()

    def send_chunk(group, chip, to, way):
        span = pl.ds(pl.multiple_of(group * group_rows + chip * pair, pair), pair)
        return pltpu.make_async_remote_copy(
            src_ref=kvb.at[span], dst_ref=kvb.at[span], send_sem=zsend.at[way, chip],
            recv_sem=zrecv.at[group, chip], device_id={"grp": to},
        )

    def share(chip):
        @pl.when(g > 0)
        def _():
            send_chunk(g, chip, g - 1, 1).start()

        @pl.when(g < grp - 1)
        def _():
            send_chunk(g, chip, g + 1, 0).start()

    inner = jnp.logical_and(g > 0, g < grp - 1)
    others = [jnp.abs(g - 1), 2 + g // 2 - 2 * (g // 3), 3 - 3 * (g // 2)]
    targets = [g + 1, g - 1, 3 * (g // 2)]

    def pass_on(k, chip):
        return send_chunk(others[k], chip, targets[k], 2 + k)

    def recv_group(k):
        for chip in range(chips):
            send_chunk(others[k], chip, g, 0).wait_recv()

            @pl.when(inner)
            def _():
                pass_on(k, chip).start()

    pcopy.wait()
    scopy.wait()
    wide = lax.broadcasted_iota(jnp.int32, (1, LANES), 1)
    inverse = jnp.ones((1, LANES), jnp.float32)
    bit = 1
    while bit < dim:
        factor = rope_base ** (-2.0 * bit / HEAD_SIZE)
        inverse = jnp.where(wide // bit % 2 == 1, inverse * factor, inverse)
        bit *= 2
    sign = jnp.where(wide % HEAD_SIZE < dim, -1.0, 1.0)
    own_place = places[g * BPG + c] * pair + p * rows + lax.broadcasted_iota(jnp.int32, (rows, LANES), 0)
    own_angles = own_place.astype(jnp.float32) * inverse
    own_cos, own_sin = jnp.cos(own_angles), jnp.sin(own_angles) * sign
    tok_copy.wait()
    pl.semaphore_wait(barrier, 7 + jnp.minimum(g, 1) + jnp.minimum(grp - 1 - g, 1))
    send_own(s, pn).start()
    send_x(half).start()
    send_y(0).start()

    own_x = toks[s]
    low = lax.broadcasted_iota(jnp.int32, (rows, LANES), 1) < HEAD_SIZE
    for k in range(chips):
        if k % 2 == 0:
            for copy in wcopies[k] + wcopies[k + 1]:
                copy.wait()
            both = jnp.dot(own_x, kvw[k // 2], preferred_element_type=jnp.float32)
        kv = both[:, k % 2 * 2 * LANES : (k % 2 + 1) * 2 * LANES]
        keys = rotate_heads(kv[:, :LANES], own_cos, own_sin)
        values = kv[:, LANES:]
        first = jnp.where(low, keys, pltpu.roll(values, HEAD_SIZE, 1)).astype(jnp.bfloat16)
        second = jnp.where(low, pltpu.roll(keys, HEAD_SIZE, 1), values).astype(jnp.bfloat16)
        if k == 0:
            mine = p == 0
            kvb[pl.ds(pl.multiple_of(key_base + s * rows, rows), rows), :] = jnp.where(mine, first, second)
            kvo[0] = jnp.where(mine, second, first)
            send_head(0, pn).start()
        else:
            chip = chip_order[k]
            kvo[2 * k - 1] = first
            kvo[2 * k] = second
            send_head(2 * k - 1, chip * 2).start()
            send_head(2 * k, chip * 2 + 1).start()

    for q in range(1, half):
        send_x(half + q).start()
        send_y(q).start()
    for q in range(half):
        send_x(q).start()
        send_y(half + q).start()

    recv_head(pn)
    share(c)
    for j in range(BPG):
        rspan = slice(j * pair, (j + 1) * pair)
        within = lax.broadcasted_iota(jnp.int32, (pair, LANES), 0)
        place = places[g * BPG + j] * pair + within
        kpos[rspan, :] = place
        angles = place.astype(jnp.float32) * inverse
        cos_ref[rspan, :] = jnp.cos(angles)
        sin_ref[rspan, :] = jnp.sin(angles) * sign
    block_place = jnp.full((1, LANES), -1, jnp.int32)
    for e in range(blocks):
        block_place = jnp.where(wide == HEAD_SIZE + e, places[e], block_place)

    quarter = rows // 2
    units = [
        [(c, 0, 0), (c, 0, quarter), (c, 1, 0), (c, 1, quarter)],
        [(cx, 0, quarter), (cx, 1, quarter), (cy, 0, 0), (cy, 1, 0)],
        [(cx, 0, 0), (cx, 1, 0), (cy, 0, quarter), (cy, 1, quarter)],
        [(cd, 0, 0), (cd, 0, quarter), (cd, 1, 0), (cd, 1, quarter)],
    ]

    def seg_rows(ref, seg):
        chip, core, off = seg
        return ref[pl.ds(pl.multiple_of(chip * pair + core * rows + off, quarter), quarter), :]

    def project(u):
        segs = units[u]
        x = jnp.concatenate([toks[chip * 2 + core, off : off + quarter] for chip, core, off in segs], axis=0)
        cosine = jnp.concatenate([seg_rows(cos_ref, seg) for seg in segs], axis=0)
        sine = jnp.concatenate([seg_rows(sin_ref, seg) for seg in segs], axis=0)
        qf = jnp.dot(x, wq[...], preferred_element_type=jnp.float32)
        qr = rotate_heads(qf, cosine, sine) * HEAD_SIZE**-0.5
        hidden = jnp.concatenate([
            jnp.broadcast_to(
                jnp.where(block_place > places[g * BPG + chip], neg_large, 0.0), (quarter, LANES)
            )
            for chip, _, _ in segs
        ], axis=0)
        lower = lax.broadcasted_iota(jnp.int32, (pair, LANES), 1) < HEAD_SIZE
        for h in range(qheads):
            v = qr[:, h // 2 * LANES : (h // 2 + 1) * LANES]
            if h % 2:
                v = pltpu.roll(v, HEAD_SIZE, 1)
            qs[u, h * pair : (h + 1) * pair, :] = jnp.where(lower, v, hidden).astype(jnp.bfloat16)

    def query_places(u):
        lane = lax.broadcasted_iota(jnp.int32, (1, pair), 1)
        place = jnp.zeros((1, pair), jnp.int32)
        for i, (chip, core, off) in enumerate(units[u]):
            base = places[g * BPG + chip] * pair + core * rows + off
            place = jnp.where(lane // quarter == i, base + lane % quarter, place)
        return place

    def prepare(k):
        group = g if k == 0 else others[k - 1]
        lane = lax.broadcasted_iota(jnp.int32, (pair, LANES), 1)
        for j in range(chips):
            kv = kvb[pl.ds(pl.multiple_of(group * group_rows + j * pair, pair), pair), :]
            mark = jnp.where(lane == HEAD_SIZE + group * BPG + j, 1.0, 0.0).astype(jnp.bfloat16)
            span = slice(k * group_rows + j * pair, k * group_rows + (j + 1) * pair)
            kaug[span, :] = jnp.where(lane < HEAD_SIZE, kv, mark)
            vt[:, span] = jnp.transpose(kv)[HEAD_SIZE:]

    sink_row = jnp.concatenate(
        [jnp.full((1, pair), sinks[s * qheads + h], jnp.float32) for h in range(qheads)], axis=1
    )
    tops = [sink_row for _ in units]

    def part_scores(u, k):
        for j in range(0, chips, 2):
            span = slice(k * group_rows + j * pair, k * group_rows + (j + 2) * pair)
            part = lax.dot_general(
                kaug[span, :], qs[u], (((1,), (1,)), ((), ())), preferred_element_type=jnp.float32
            )
            if k == 0:
                seen = kpos[j * pair : (j + 2) * pair, :] <= query_places(u)
                part = jnp.where(jnp.concatenate([seen] * qheads, axis=1), part, neg_large)
            yield span, part

    def score(u, k):
        for span, part in part_scores(u, k):
            sbuf[u, span, :] = part
            tops[u] = jnp.maximum(tops[u], jnp.max(part, axis=0, keepdims=True))

    bases = [None for _ in units]
    totals = [None for _ in units]

    def absorb(us, stored, fresh, final=False):
        low_key = min(stored + fresh) * group_rows
        high_key = (max(stored + fresh) + 1) * group_rows
        parts = {u: [piece for k in fresh for piece in part_scores(u, k)] for u in us}
        factor, mix = {}, {}
        for u in us:
            for _, part in parts[u]:
                tops[u] = jnp.maximum(tops[u], jnp.max(part, axis=0, keepdims=True))
            if bases[u] is None:
                total = jnp.exp(sink_row - tops[u])
            else:
                factor[u] = jnp.exp(bases[u] - tops[u])
                total = totals[u] * factor[u]
            for k in stored:
                for j in range(0, chips, 2):
                    span = slice(k * group_rows + j * pair, k * group_rows + (j + 2) * pair)
                    weights = jnp.exp(sbuf[u, span, :] - tops[u])
                    pbuf[u, span, :] = weights.astype(jnp.bfloat16)
                    total = total + jnp.sum(weights, axis=0, keepdims=True)
            for span, part in parts[u]:
                weights = jnp.exp(part - tops[u])
                pbuf[u, span, :] = weights.astype(jnp.bfloat16)
                total = total + jnp.sum(weights, axis=0, keepdims=True)
            totals[u], bases[u] = total, tops[u]
        for u in us:
            mix[u] = jnp.dot(
                vt[:, low_key:high_key], pbuf[u, low_key:high_key, :], preferred_element_type=jnp.float32
            )
        for u in us:
            full = mix[u] + mbuf[u] * factor[u] if u in factor else mix[u]
            if not final:
                mbuf[u] = full
                continue
            full = full / totals[u]
            heads = [jnp.transpose(full[:, h * pair : (h + 1) * pair]) for h in range(qheads)]
            abuf[u] = jnp.concatenate(heads, axis=1).astype(jnp.bfloat16)
        if final:
            for u in us:
                ship(u)

    def send_out(u, i):
        chip, core, off = units[u][i]
        count = rows if u in (0, 3) else quarter
        src = abuf.at[u, pl.ds(i * quarter, count)]
        dst = obuf.at[pl.ds(off, count), pl.ds(pl.multiple_of(s * qc, qc), qc)]
        return pltpu.make_async_remote_copy(
            src_ref=src, dst_ref=dst, send_sem=osend.at[u, i],
            recv_sem=orecv.at[s, u // 2], device_id={"sp": chip * 2 + core},
        )

    def send_out_partner():
        src = abuf.at[0, pl.ds(pl.multiple_of((1 - p) * rows, rows), rows)]
        dst = obuf.at[:, pl.ds(pl.multiple_of(s * qc, qc), qc)]
        return pltpu.make_async_remote_copy(
            src_ref=src, dst_ref=dst, send_sem=osend.at[0, 0],
            recv_sem=orecv.at[s, 0], device_id={"sp": pn},
        )

    def recv_out(src, off, count, part):
        dst = obuf.at[pl.ds(off, count), pl.ds(pl.multiple_of(src * qc, qc), qc)]
        pltpu.make_async_remote_copy(
            src_ref=abuf.at[0, pl.ds(0, count)], dst_ref=dst, send_sem=osend.at[0, 0],
            recv_sem=orecv.at[src, part], device_id={"sp": src},
        ).wait_recv()

    def ship(u):
        if u == 0:
            send_out_partner().start()
            obuf[:, pl.ds(pl.multiple_of(s * qc, qc), qc)] = abuf[
                0, pl.ds(pl.multiple_of(p * rows, rows), rows), :
            ]
        elif u == 3:
            send_out(u, 0).start()
            send_out(u, 2).start()
        else:
            for i in range(4):
                send_out(u, i).start()

    def stage(k):
        qx, qy = (k + half) % pieces, k
        forward(0, qx).wait_recv()
        if k < half:
            relay(qx).start()
        forward(0, qx).start()
        forward(1, qy).wait_recv()
        if k < half:
            relay(qy).start()
        forward(1, qy).start()

    def stage_partner(k):
        qx, qy = (k + half) % pieces, k
        send_piece(cx * 2 + 1 - p, qx, pn, fsend.at[0, qx]).wait_recv()
        send_piece(cy * 2 + 1 - p, qy, pn, fsend.at[1, qy]).wait_recv()

    def stage_far(q):
        for r in (q, q + half):
            forward(2, r).wait_recv()
            forward(2, r).start()

    def stage_far_partner(q):
        for r in (q, q + half):
            send_piece(cd * 2 + 1 - p, r, pn, fsend.at[2, r]).wait_recv()

    send_own(pn, pn).wait_recv()
    wq_copy.wait()
    project(0)
    stage(0)
    for chip in (cx, cy, cd):
        recv_head(chip * 2)
        recv_head(chip * 2 + 1)
        share(chip)
    prepare(0)
    score(0, 0)
    stage(1)
    for k in range(half):
        stage_partner(k)
    project(1)
    score(1, 0)
    recv_group(0)
    pl.when(inner)(lambda: recv_group(1))
    prepare(1)
    score(0, 1)
    score(1, 1)
    stage(2)
    absorb((0, 1), [0, 1], [])
    stage(3)
    for k in range(half, pieces):
        stage_partner(k)
    project(2)
    score(2, 0)
    score(2, 1)
    pl.when(jnp.logical_not(inner))(lambda: recv_group(1))
    pl.when(inner)(lambda: recv_group(2))
    stage_far(0)
    prepare(2)
    absorb((0, 1), [], [2])
    stage_far(1)
    absorb((2,), [0, 1], [2])
    for q in range(half):
        stage_far_partner(q)
    project(3)
    for k in range(grp - 1):
        score(3, k)
    pl.when(jnp.logical_not(inner))(lambda: recv_group(2))
    prepare(3)
    absorb((3,), [0, 1, 2], [3], True)
    absorb((1, 2), [], [3], True)
    absorb((0,), [], [3], True)

    recv_out(pn, 0, rows, 0)
    for core in range(2):
        recv_out(cx * 2 + core, quarter, quarter, 0)
        recv_out(cy * 2 + core, 0, quarter, 0)
        recv_out(cx * 2 + core, 0, quarter, 1)
        recv_out(cy * 2 + core, quarter, quarter, 1)
        recv_out(cd * 2 + core, 0, rows, 1)
    out[...] = obuf[...]
    send_own(s, pn).wait_send()
    for q in range(pieces):
        send_x(q).wait_send()
        send_y(q).wait_send()
        relay(q).wait_send()
        for k in range(3):
            forward(k, q).wait_send()
    for i in range(sp - 1):
        send_head(i, pn).wait_send()
    for chip in range(chips):
        @pl.when(g > 0)
        def _():
            send_chunk(g, chip, g - 1, 1).wait_send()

        @pl.when(g < grp - 1)
        def _():
            send_chunk(g, chip, g + 1, 0).wait_send()

        @pl.when(inner)
        def _():
            for k in range(3):
                pass_on(k, chip).wait_send()

    send_out_partner().wait_send()
    for i in range(4):
        send_out(1, i).wait_send()
        send_out(2, i).wait_send()
    send_out(3, 0).wait_send()
    send_out(3, 2).wait_send()


def per_plane(tokens, query_weight, key_value_weight, block_places, sinks):
    sp = lax.axis_size("sp")
    grp = lax.axis_size("grp")
    rows, width = tokens.shape
    group_rows = rows * sp
    key_count = grp * group_rows
    qc = query_weight.shape[1]
    qheads = qc // HEAD_SIZE
    pair = 2 * rows
    columns = qheads * pair
    pieces = 4
    hbm = pl.BlockSpec(memory_space=pl.ANY)
    dma = pltpu.SemaphoreType.DMA
    bf16, f32 = jnp.bfloat16, jnp.float32
    return pl.pallas_call(
        functools.partial(plane_kernel, grp, sp, qheads),
        out_shape=pltpu.VMEM((rows, qc * sp), bf16),
        in_specs=[hbm] * 5,
        out_specs=pl.BlockSpec(memory_space=pltpu.VMEM),
        scratch_shapes=[
            pltpu.SMEM(block_places.shape, block_places.dtype),
            pltpu.SMEM(sinks.shape, sinks.dtype),
            pltpu.VMEM((sp, rows, width), bf16),
            pltpu.VMEM((width, qc), bf16),
            pltpu.VMEM((2, width, 4 * LANES), bf16),
            pltpu.VMEM((sp, rows, LANES), bf16),
            pltpu.VMEM((key_count, LANES), bf16),
            pltpu.VMEM((key_count, LANES), bf16),
            pltpu.VMEM((HEAD_SIZE, key_count), bf16),
            pltpu.VMEM((sp // 2, columns, LANES), bf16),
            pltpu.VMEM((sp // 2, key_count, columns), f32),
            pltpu.VMEM((sp // 2, key_count, columns), bf16),
            pltpu.VMEM((sp // 2, HEAD_SIZE, columns), f32),
            pltpu.VMEM((sp // 2, pair, qc), bf16),
            pltpu.VMEM((rows, qc * sp), bf16),
            pltpu.VMEM((group_rows, LANES), f32),
            pltpu.VMEM((group_rows, LANES), f32),
            pltpu.VMEM((group_rows, LANES), jnp.int32),
            dma((4 + sp,)),
            dma((pieces,)),
            dma((pieces,)),
            dma((1,)),
            dma((pieces,)),
            dma((3, pieces)),
            dma((sp, pieces)),
            dma((sp,)),
            dma((sp,)),
            dma((5, sp // 2)),
            dma((grp, sp // 2)),
            dma((4, 4)),
            dma((sp, 2)),
        ],
        compiler_params=pltpu.CompilerParams(
            has_side_effects=True, collective_id=0, vmem_limit_bytes=60 * 1024 * 1024
        ),
    )(tokens, query_weight, key_value_weight, block_places, sinks)


def local_form(tokens, query_weight, key_value_weight, block_places, sinks):
    sp = lax.axis_size("sp")
    grp = lax.axis_size("grp")
    heads = query_weight.shape[1] // HEAD_SIZE
    kv_total = key_value_weight.shape[1] // (2 * HEAD_SIZE)
    square = sp // 2 == BPG and grp == BPG and kv_total == sp and block_places.shape[0] == grp * BPG
    form = per_plane if square and heads * HEAD_SIZE == 2 * LANES else per_device
    return form(tokens, query_weight, key_value_weight, block_places, sinks)


def solution(mesh):
    in_specs = (P(("grp", "sp"), None), P(None, "sp"), P(), P(), P())
    out_specs = P(("grp", "sp"), None)
    return jax.shard_map(
        local_form, mesh=mesh, in_specs=in_specs, out_specs=out_specs, check_vma=False
    )
```

```python
import functools

import jax
import jax.numpy as jnp
from jax import lax
from jax.experimental import pallas as pl
from jax.experimental.pallas import tpu as pltpu
from jax.sharding import PartitionSpec as P

QUERY_HEADS = 32
HEAD_SIZE = 64
BPG = 4
LANES = 128

rope_base = 150000.0
neg_large = -1e30


def rotate_heads(x, cosine, sine):
    width = x.shape[1]
    half = HEAD_SIZE // 2
    if width % LANES:
        swapped = jnp.concatenate([x[:, half:], x[:, :half]], axis=1)
        return x * cosine[:, :width] + swapped * sine[:, :width]
    parts = []
    lane = lax.broadcasted_iota(jnp.int32, (x.shape[0], LANES), 1)
    first = lane % HEAD_SIZE < half
    for j in range(width // LANES):
        v = x[:, j * LANES : (j + 1) * LANES]
        swapped = jnp.where(first, pltpu.roll(v, LANES - half, 1), pltpu.roll(v, half, 1))
        parts.append(v * cosine + swapped * sine)
    return parts[0] if len(parts) == 1 else jnp.concatenate(parts, axis=1)


def kernel(
    grp, sp, qheads, kv_total,
    tok, wq_any, kvw_any, inverse_ref, places_ref, sink, out,
    toks, wq, wkv, kvb, q, abuf, obuf, cos_ref, sin_ref, qpos, kpos,
    wsem, tsend, tfwd, trecv, ksend, krecv, osend, orecv,
):
    s = lax.axis_index("sp")
    g = lax.axis_index("grp")
    rows = tok.shape[0]
    group_rows = rows * sp
    chips = sp // 2
    pair = 2 * rows
    qc = qheads * HEAD_SIZE
    c = s // 2
    par = s % 2
    partner = s + 1 - 2 * par
    head = s * kv_total // sp
    hpar = head % 2
    koff = pl.multiple_of(head // 2 * LANES, LANES)
    voff = pl.multiple_of(kv_total * HEAD_SIZE + head // 2 * LANES, LANES)

    wcopies = [
        pltpu.make_async_copy(wq_any, wq, wsem.at[0]),
        pltpu.make_async_copy(
            kvw_any.at[:, pl.ds(koff, LANES)], wkv.at[:, pl.ds(0, LANES)], wsem.at[1]
        ),
        pltpu.make_async_copy(
            kvw_any.at[:, pl.ds(voff, LANES)], wkv.at[:, pl.ds(LANES, LANES)], wsem.at[2]
        ),
    ]

    def send_tok(to):
        return pltpu.make_async_remote_copy(
            src_ref=tok, dst_ref=toks.at[s], send_sem=tsend.at[to], recv_sem=trecv.at[s],
            device_id={"sp": to},
        )

    def forward(slot):
        return pltpu.make_async_remote_copy(
            src_ref=toks.at[slot], dst_ref=toks.at[slot], send_sem=tfwd.at[slot],
            recv_sem=trecv.at[slot], device_id={"sp": partner},
        )

    def send_kv(chip, d):
        span = pl.ds(pl.multiple_of(g * group_rows + chip * pair, pair), pair)
        return pltpu.make_async_remote_copy(
            src_ref=kvb.at[span], dst_ref=kvb.at[span], send_sem=ksend.at[d, chip],
            recv_sem=krecv.at[g, chip], device_id={"grp": (g + d) % grp},
        )

    def recv_kv(chip, d):
        src = (g + d) % grp
        span = pl.ds(pl.multiple_of(src * group_rows + chip * pair, pair), pair)
        return pltpu.make_async_remote_copy(
            src_ref=kvb.at[span], dst_ref=kvb.at[span], send_sem=ksend.at[d, chip],
            recv_sem=krecv.at[src, chip], device_id={"grp": src},
        )

    def send_out(to):
        return pltpu.make_async_remote_copy(
            src_ref=abuf.at[to], dst_ref=obuf.at[s], send_sem=osend.at[to],
            recv_sem=orecv.at[s], device_id={"sp": to},
        )

    def recv_out(src):
        return pltpu.make_async_remote_copy(
            src_ref=abuf.at[src], dst_ref=obuf.at[src], send_sem=osend.at[src],
            recv_sem=orecv.at[src], device_id={"sp": src},
        )

    send_tok(partner).start()

    def start_tok(k, _):
        send_tok((c + k) % chips * 2 + par).start()
        return 0

    lax.fori_loop(1, chips, start_tok, 0)
    for copy in wcopies:
        copy.start()
    toks[s] = tok[...]

    block_rows = group_rows // BPG
    for j in range(kpos.shape[1] // block_rows):
        within = lax.broadcasted_iota(jnp.int32, (1, block_rows), 1)
        kpos[:, j * block_rows : (j + 1) * block_rows] = places_ref[j] * block_rows + within
    wide = lax.broadcasted_iota(jnp.int32, (1, LANES), 1)
    half = HEAD_SIZE // 2
    inverse = inverse_ref[...]
    sign = jnp.where(wide % HEAD_SIZE < half, -1.0, 1.0)
    for j in range(BPG):
        rspan = slice(j * block_rows, (j + 1) * block_rows)
        within = lax.broadcasted_iota(jnp.int32, (block_rows, LANES), 0)
        place = places_ref[g * BPG + j] * block_rows + within
        qpos[rspan, :] = place[:, :1]
        angles = place.astype(jnp.float32) * inverse
        cos_ref[rspan, :] = jnp.cos(angles)
        sin_ref[rspan, :] = jnp.sin(angles) * sign
    for copy in wcopies:
        copy.wait()

    def project(k, _):
        chip = (c + chips - k) % chips

        @pl.when(k > 0)
        def _():
            slot = chip * 2 + par
            forward(slot).wait_recv()
            forward(slot).start()

        forward(chip * 2 + 1 - par).wait_recv()
        x = toks[pl.ds(chip * 2, 2)].reshape(pair, tok.shape[1])
        span = pl.ds(pl.multiple_of(chip * pair, pair), pair)
        cosine = cos_ref[span, :]
        sine = sin_ref[span, :]
        kv = jnp.dot(x, wkv[...], preferred_element_type=jnp.float32)
        keys = rotate_heads(kv[:, :LANES], cosine, sine)
        values = kv[:, LANES:]
        low = hpar == 0
        keys = jnp.where(low, keys, pltpu.roll(keys, HEAD_SIZE, 1))
        values = jnp.where(low, pltpu.roll(values, HEAD_SIZE, 1), values)
        lane = lax.broadcasted_iota(jnp.int32, (pair, LANES), 1)
        joined = jnp.where(lane < HEAD_SIZE, keys, values).astype(jnp.bfloat16)
        kvb[pl.ds(pl.multiple_of(g * group_rows + chip * pair, pair), pair), :] = joined
        for d in range(1, grp):
            send_kv(chip, d).start()
        qf = jnp.dot(x, wq[...], preferred_element_type=jnp.float32)
        qr = (rotate_heads(qf, cosine, sine) * HEAD_SIZE**-0.5).astype(jnp.bfloat16)
        zeros = jnp.zeros((pair, HEAD_SIZE), jnp.bfloat16)
        for h in range(qheads):
            q[h, span, :] = jnp.concatenate(
                [qr[:, h * HEAD_SIZE : (h + 1) * HEAD_SIZE], zeros], axis=1
            )
        return 0

    lax.fori_loop(0, chips, project, 0)

    def arrive(chip, _):
        for d in range(1, grp):
            recv_kv(chip, d).wait_recv()
        return 0

    lax.fori_loop(0, chips, arrive, 0)

    key_count = kvb.shape[0]
    chunk = min(key_count, 2048)
    chunks = key_count // chunk
    block = min(256, group_rows)
    tiles = block // rows

    def attention(b, _):
        span = pl.ds(pl.multiple_of(b * block, block), block)
        places = qpos[span, :]
        outs = []
        for h in range(qheads):
            qh = q[h, span, :]

            def visit(t, state):
                top, total, mix = state
                kspan = pl.ds(pl.multiple_of(t * chunk, chunk), chunk)
                kv = kvb[kspan, :]
                scores = lax.dot_general(
                    qh, kv, (((1,), (1,)), ((), ())), preferred_element_type=jnp.float32
                )
                allowed = kpos[:, kspan] <= places
                scores = jnp.where(allowed, scores, neg_large)
                higher = jnp.maximum(top, jnp.max(scores, axis=1, keepdims=True))
                weights = jnp.exp(scores - higher)
                factor = jnp.exp(top - higher)
                total = total * factor + jnp.sum(weights, axis=1, keepdims=True)
                mix = mix * factor + jnp.dot(
                    weights.astype(jnp.bfloat16), kv, preferred_element_type=jnp.float32
                )
                return higher, total, mix

            state = (
                jnp.full((block, 1), sink[s * qheads + h], jnp.float32),
                jnp.ones((block, 1), jnp.float32),
                jnp.zeros((block, LANES), jnp.float32),
            )
            if chunks == 1:
                state = visit(0, state)
            else:
                state = lax.fori_loop(0, chunks, visit, state)
            outs.append((state[2] / state[1])[:, HEAD_SIZE:])
        att = outs[0] if qheads == 1 else jnp.concatenate(outs, axis=1)
        abuf[pl.ds(b * tiles, tiles)] = att.astype(jnp.bfloat16).reshape(tiles, rows, qc)

        def ship(i, _):
            to = b * tiles + i

            @pl.when(to != s)
            def _():
                send_out(to).start()

            return 0

        lax.fori_loop(0, tiles, ship, 0)
        return 0

    lax.fori_loop(0, group_rows // block, attention, 0)
    obuf[s] = abuf[s]

    def drain(j, _):
        @pl.when(j != s)
        def _():
            recv_out(j).wait_recv()
            send_out(j).wait_send()

        return 0

    lax.fori_loop(0, sp, drain, 0)
    for j in range(sp):
        out[:, j * qc : (j + 1) * qc] = obuf[j]
    send_tok(partner).wait_send()

    def finish(k, _):
        send_tok((c + k) % chips * 2 + par).wait_send()
        forward((c + chips - k) % chips * 2 + par).wait_send()
        return 0

    lax.fori_loop(1, chips, finish, 0)

    def finish_kv(chip, _):
        for d in range(1, grp):
            send_kv(chip, d).wait_send()
        return 0

    lax.fori_loop(0, chips, finish_kv, 0)


def per_device(tokens, query_weight, key_value_weight, block_places, sinks):
    sp = lax.axis_size("sp")
    grp = lax.axis_size("grp")
    rows, width = tokens.shape
    group_rows = rows * sp
    key_count = grp * group_rows
    qc = query_weight.shape[1]
    qheads = qc // HEAD_SIZE
    kv_total = key_value_weight.shape[1] // (2 * HEAD_SIZE)
    freq = jnp.arange(HEAD_SIZE // 2, dtype=jnp.float32)
    inverse = rope_base ** (-(freq * 2.0) / HEAD_SIZE)
    inverse = jnp.tile(inverse, LANES // (HEAD_SIZE // 2)).reshape(1, LANES)

    vmem = pl.BlockSpec(memory_space=pltpu.VMEM)
    hbm = pl.BlockSpec(memory_space=pl.ANY)
    smem = pl.BlockSpec(memory_space=pltpu.SMEM)
    dma = pltpu.SemaphoreType.DMA
    return pl.pallas_call(
        functools.partial(kernel, grp, sp, qheads, kv_total),
        out_shape=jax.ShapeDtypeStruct((rows, qc * sp), jnp.bfloat16),
        in_specs=[vmem, hbm, hbm, vmem, smem, smem],
        out_specs=vmem,
        scratch_shapes=[
            pltpu.VMEM((sp, rows, width), jnp.bfloat16),
            pltpu.VMEM((width, qc), jnp.bfloat16),
            pltpu.VMEM((width, 2 * LANES), jnp.bfloat16),
            pltpu.VMEM((key_count, LANES), jnp.bfloat16),
            pltpu.VMEM((qheads, group_rows, LANES), jnp.bfloat16),
            pltpu.VMEM((sp, rows, qc), jnp.bfloat16),
            pltpu.VMEM((sp, rows, qc), jnp.bfloat16),
            pltpu.VMEM((group_rows, LANES), jnp.float32),
            pltpu.VMEM((group_rows, LANES), jnp.float32),
            pltpu.VMEM((group_rows, 1), jnp.int32),
            pltpu.VMEM((1, key_count), jnp.int32),
            dma((3,)),
            dma((sp,)),
            dma((sp,)),
            dma((sp,)),
            dma((grp, sp // 2)),
            dma((grp, sp // 2)),
            dma((sp,)),
            dma((sp,)),
        ],
        compiler_params=pltpu.CompilerParams(
            has_side_effects=True, vmem_limit_bytes=60 * 1024 * 1024
        ),
    )(tokens, query_weight, key_value_weight, inverse, block_places, sinks)


def plane_kernel(
    grp, sp, qheads,
    tok_any, wq_any, kvw_any, places_any, sinks_any, out,
    places, sinks,    toks, wq, kvw, kvo, kvb, kaug, vt, qs, sbuf, pbuf, mbuf, abuf, obuf, cos_ref, sin_ref, kpos,
    wsem, tsend, trecv, drecv, ksend, krecv, zsend, zrecv, osend, orecv, ready,
):
    s = lax.axis_index("sp")
    g = lax.axis_index("grp")
    rows, width = toks.shape[1:]
    pieces = trecv.shape[1]
    piece_rows = rows // pieces
    half = pieces // 2
    pair = 2 * rows
    group_rows = rows * sp
    chips = sp // 2
    qc = qheads * HEAD_SIZE
    blocks = grp * BPG
    dim = HEAD_SIZE // 2
    p = s % 2
    c = s // 2
    cx = c + 1 - 2 * (c % 2)
    cy = (c + chips // 2) % chips
    cd = (cx + chips // 2) % chips
    xn, yn, dn, pn = cx * 2 + p, cy * 2 + p, cd * 2 + p, c * 2 + 1 - p
    key_base = g * group_rows

    chip_order = [c, cx, cy, cd]
    ways = [0, 2, 3, 1]
    wcopies = []
    for k, chip in enumerate(chip_order):
        koff = pl.multiple_of(chip * LANES, LANES)
        voff = pl.multiple_of(sp * HEAD_SIZE + chip * LANES, LANES)
        for part, off in enumerate((koff, voff)):
            wcopies.append(
                pltpu.make_async_copy(
                    kvw_any.at[:, pl.ds(off, LANES)],
                    kvw.at[k // 2, :, pl.ds((2 * (k % 2) + part) * LANES, LANES)],
                    wsem.at[2 + k // 2],
                )
            )
    tok_copy = pltpu.make_async_copy(tok_any, toks.at[s], wsem.at[0])
    wq_copy = pltpu.make_async_copy(wq_any, wq, wsem.at[1])
    pcopy = pltpu.make_async_copy(places_any, places, wsem.at[4])
    scopy = pltpu.make_async_copy(sinks_any, sinks, wsem.at[5])
    pcopy.start()
    scopy.start()
    tok_copy.start()
    for copy in wcopies:
        copy.start()
    wq_copy.start()

    barrier = pltpu.get_barrier_semaphore()
    upper = c >= chips // 2
    for to in (xn, yn, pn, cx * 2 + 1 - p, cy * 2 + 1 - p):
        pl.semaphore_signal(barrier, inc=1, device_id={"sp": to})

    @pl.when(jnp.logical_not(upper))
    def _():
        for core in range(2):
            pl.semaphore_signal(barrier, inc=1, device_id={"sp": cd * 2 + core})

    @pl.when(g < grp - 1)
    def _():
        pl.semaphore_signal(barrier, inc=1, device_id={"grp": g + 1})

    def send_piece(slot, q, to, sem):
        span = pl.ds(q * piece_rows, piece_rows)
        return pltpu.make_async_remote_copy(
            src_ref=toks.at[slot, span], dst_ref=toks.at[slot, span], send_sem=tsend.at[0],
            recv_sem=sem, device_id={"sp": to},
        )

    def send_own(slot, to):
        return pltpu.make_async_remote_copy(
            src_ref=toks.at[slot], dst_ref=toks.at[slot], send_sem=tsend.at[0],
            recv_sem=drecv.at[3], device_id={"sp": to},
        )

    def send_x(q):
        return send_piece(s, q, xn, trecv.at[0, q])

    def send_y(q):
        return send_piece(s, q, yn, trecv.at[1, q])

    def relay(q):
        if q >= half:
            return send_piece(xn, q, yn, trecv.at[2, q])
        return send_piece(yn, q, xn, trecv.at[2, q])

    def arrived(k, q):
        send_piece((xn, yn, dn)[k], q, pn, trecv.at[k, q]).wait_recv()

    def forward(k, q, i):
        return send_piece((xn, yn, dn)[k], q, pn, drecv.at[i])

    def wait_rows(sem, slots, count=rows):
        area = toks.at[pl.ds(0, slots), pl.ds(0, count)]
        pltpu.make_async_remote_copy(
            src_ref=area, dst_ref=area, send_sem=sem, recv_sem=sem, device_id={"sp": pn}
        ).wait_recv()

    def send_head(i, to, way):
        span = pl.ds(pl.multiple_of(key_base + s * rows, rows), rows)
        return pltpu.make_async_remote_copy(
            src_ref=kvo.at[i], dst_ref=kvb.at[span], send_sem=ksend.at[0],
            recv_sem=krecv.at[way], device_id={"sp": to},
        )

    def recv_heads(chip, way):
        span = pl.ds(pl.multiple_of(key_base + chip * pair, pair), rows if way == 0 else pair)
        pltpu.make_async_remote_copy(
            src_ref=kvb.at[span], dst_ref=kvb.at[span], send_sem=ksend.at[0],
            recv_sem=krecv.at[way], device_id={"sp": pn},
        ).wait_recv()

    def send_chunk(group, chip, to, way):
        span = pl.ds(pl.multiple_of(group * group_rows + chip * pair, pair), pair)
        return pltpu.make_async_remote_copy(
            src_ref=kvb.at[span], dst_ref=kvb.at[span], send_sem=zsend.at[way],
            recv_sem=zrecv.at[group, chip], device_id={"grp": to},
        )

    def share(chip):
        @pl.when(g > 0)
        def _():
            send_chunk(g, chip, g - 1, 1).start()

        @pl.when(g < grp - 1)
        def _():
            send_chunk(g, chip, g + 1, 0).start()

    inner = jnp.logical_and(g > 0, g < grp - 1)
    others = [jnp.abs(g - 1), 2 + g // 2 - 2 * (g // 3), 3 - 3 * (g // 2)]
    targets = [g + 1, g - 1, 3 * (g // 2)]

    def pass_on(k, chip):
        return send_chunk(others[k], chip, targets[k], 2)

    outer = jnp.logical_not(inner)

    def recv_group(k, chip_list):
        for chip in chip_list:
            send_chunk(others[k], chip, g, 0).wait_recv()

            @pl.when(inner)
            def _():
                pass_on(k, chip).start()

    pcopy.wait()
    scopy.wait()
    wide = lax.broadcasted_iota(jnp.int32, (1, LANES), 1)
    inverse = jnp.ones((1, LANES), jnp.float32)
    bit = 1
    while bit < dim:
        factor = rope_base ** (-2.0 * bit / HEAD_SIZE)
        inverse = jnp.where(wide // bit % 2 == 1, inverse * factor, inverse)
        bit *= 2
    sign = jnp.where(wide % HEAD_SIZE < dim, -1.0, 1.0)
    own_place = places[g * BPG + c] * pair + p * rows + lax.broadcasted_iota(jnp.int32, (rows, LANES), 0)
    own_angles = own_place.astype(jnp.float32) * inverse
    own_cos, own_sin = jnp.cos(own_angles), jnp.sin(own_angles) * sign
    tok_copy.wait()
    pl.semaphore_wait(barrier, 5 + jnp.minimum(g, 1) + 2 * (c // (chips // 2)))
    send_own(s, pn).start()
    send_x(half).start()
    send_y(0).start()

    @pl.when(g > 0)
    def _():
        pl.semaphore_signal(ready.at[0], inc=1, device_id={"grp": g - 1})

    @pl.when(upper)
    def _():
        for core in range(2):
            pl.semaphore_signal(ready.at[1], inc=1, device_id={"sp": cd * 2 + core})

    own_x = toks[s]
    low = lax.broadcasted_iota(jnp.int32, (rows, LANES), 1) < HEAD_SIZE
    for k in range(chips):
        if k % 2 == 0:
            pltpu.make_async_copy(
                kvw_any.at[:, pl.ds(0, 4 * LANES)], kvw.at[k // 2], wsem.at[2 + k // 2]
            ).wait()
            both = jnp.dot(own_x, kvw[k // 2], preferred_element_type=jnp.float32)
        kv = both[:, k % 2 * 2 * LANES : (k % 2 + 1) * 2 * LANES]
        keys = rotate_heads(kv[:, :LANES], own_cos, own_sin)
        values = kv[:, LANES:]
        first = jnp.where(low, keys, pltpu.roll(values, HEAD_SIZE, 1)).astype(jnp.bfloat16)
        second = jnp.where(low, pltpu.roll(keys, HEAD_SIZE, 1), values).astype(jnp.bfloat16)
        way = ways[k]
        if way == 0:
            mine = p == 0
            kvb[pl.ds(pl.multiple_of(key_base + s * rows, rows), rows), :] = jnp.where(mine, first, second)
            kvo[0] = jnp.where(mine, second, first)
            send_head(0, pn, 0).start()
        else:
            chip = chip_order[k]
            kvo[2 * way - 1] = first
            kvo[2 * way] = second
            if way == 1:
                pl.when(jnp.logical_not(upper))(lambda: pl.semaphore_wait(ready.at[1], 2))
            send_head(2 * way - 1, chip * 2, way).start()
            send_head(2 * way, chip * 2 + 1, way).start()

    for q in range(1, half):
        send_x(half + q).start()
        send_y(q).start()
    for q in range(half):
        send_x(q).start()
        send_y(half + q).start()

    recv_heads(c, 0)
    pl.when(g < grp - 1)(lambda: pl.semaphore_wait(ready.at[0], 1))
    share(c)
    for j in range(BPG):
        rspan = slice(j * pair, (j + 1) * pair)
        within = lax.broadcasted_iota(jnp.int32, (pair, LANES), 0)
        place = places[g * BPG + j] * pair + within
        kpos[rspan, :] = place
        angles = place.astype(jnp.float32) * inverse
        cos_ref[rspan, :] = jnp.cos(angles)
        sin_ref[rspan, :] = jnp.sin(angles) * sign
    block_place = jnp.full((1, LANES), -1, jnp.int32)
    for e in range(blocks):
        block_place = jnp.where(wide == HEAD_SIZE + e, places[e], block_place)

    quarter = rows // 2
    units = [
        [[(c, 0, 0), (c, 0, quarter), (c, 1, 0), (c, 1, quarter)]],
        [[(cx, 0, quarter), (cx, 1, quarter), (cy, 0, 0), (cy, 1, 0)]],
        [[(cx, 0, 0), (cx, 1, 0), (cy, 0, quarter), (cy, 1, quarter)]],
        [[(cd, 0, 0), (cd, 0, quarter), (cd, 1, 0), (cd, 1, quarter)]],
    ]

    def seg_size(u):
        return quarter // len(units[u])

    def seg_rows(ref, seg, count):
        chip, core, off = seg
        return ref[pl.ds(pl.multiple_of(chip * pair + core * rows + off, count), count), :]

    def run(*tasks):
        tasks = list(tasks)
        while tasks:
            for task in list(tasks):
                try:
                    next(task)
                except StopIteration:
                    tasks.remove(task)

    def project(u, part):
        segs, count = units[u][part], seg_size(u)
        size = 4 * count
        x = jnp.concatenate([toks[chip * 2 + core, off : off + count] for chip, core, off in segs], axis=0)
        cosine = jnp.concatenate([seg_rows(cos_ref, seg, count) for seg in segs], axis=0)
        sine = jnp.concatenate([seg_rows(sin_ref, seg, count) for seg in segs], axis=0)
        qf = jnp.dot(x, wq[...], preferred_element_type=jnp.float32)
        yield
        qr = rotate_heads(qf, cosine, sine) * HEAD_SIZE**-0.5
        hidden = jnp.concatenate([
            jnp.broadcast_to(
                jnp.where(block_place > places[g * BPG + chip], neg_large, 0.0), (count, LANES)
            )
            for chip, _, _ in segs
        ], axis=0)
        lower = lax.broadcasted_iota(jnp.int32, (size, LANES), 1) < HEAD_SIZE
        for h in range(qheads):
            v = qr[:, h // 2 * LANES : (h // 2 + 1) * LANES]
            if h % 2:
                v = pltpu.roll(v, HEAD_SIZE, 1)
            base = (part * qheads + h) * size
            qs[u, base : base + size, :] = jnp.where(lower, v, hidden).astype(jnp.bfloat16)
            yield

    def query_places(u, part):
        count = seg_size(u)
        size = 4 * count
        row = lax.broadcasted_iota(jnp.int32, (1, qheads * size), 1) % size
        place = jnp.zeros(row.shape, jnp.int32)
        for i, (chip, core, off) in enumerate(units[u][part]):
            base = places[g * BPG + chip] * pair + core * rows + off
            place = jnp.where(row // count == i, base + row % count, place)
        return place

    def sink_row(u):
        size = 4 * seg_size(u)
        head = lax.broadcasted_iota(jnp.int32, (1, qheads * size), 1) // size
        row = jnp.full(head.shape, sinks[s * qheads], jnp.float32)
        for h in range(1, qheads):
            row = jnp.where(head == h, sinks[s * qheads + h], row)
        return row

    def prepare(k):
        group = g if k == 0 else others[k - 1]
        lane = lax.broadcasted_iota(jnp.int32, (pair, LANES), 1)
        for j in range(chips):
            kv = kvb[pl.ds(pl.multiple_of(group * group_rows + j * pair, pair), pair), :]
            mark = jnp.where(lane == HEAD_SIZE + group * BPG + j, 1.0, 0.0).astype(jnp.bfloat16)
            span = slice(k * group_rows + j * pair, k * group_rows + (j + 1) * pair)
            kaug[span, :] = jnp.where(lane < HEAD_SIZE, kv, mark)
            vt[:, span] = jnp.transpose(kv)[HEAD_SIZE:]

    tops = [[sink_row(u) for _ in units[u]] for u in range(len(units))]

    def joined(rows_of):
        return rows_of[0] if len(rows_of) == 1 else jnp.concatenate(rows_of, axis=1)

    floors = [joined(tops[u]) for u in range(len(units))]

    def part_scores(u, k, part):
        width_of = qheads * 4 * seg_size(u)
        side = slice(part * width_of, (part + 1) * width_of)
        for j in range(0, chips, 2):
            span = slice(k * group_rows + j * pair, k * group_rows + (j + 2) * pair)
            piece = lax.dot_general(
                kaug[span, :], qs[u, side, :], (((1,), (1,)), ((), ())), preferred_element_type=jnp.float32
            )
            if k == 0:
                seen = jnp.concatenate([kpos[j * pair : (j + 2) * pair, :]] * (width_of // LANES), axis=1)
                piece = jnp.where(seen <= query_places(u, part), piece, neg_large)
            sbuf[u, span, side] = piece
            tops[u][part] = jnp.maximum(tops[u][part], jnp.max(piece, axis=0, keepdims=True))
            yield

    def score(u, k):
        for part in range(len(units[u])):
            yield from part_scores(u, k, part)

    bases = [None for _ in units]
    totals = [None for _ in units]

    def absorb(u, stored, fresh, final=False):
        low_key = min(stored + fresh) * group_rows
        high_key = (max(stored + fresh) + 1) * group_rows
        for k in fresh:
            yield from score(u, k)
        top = joined(tops[u])
        factor = None
        if bases[u] is None:
            total = jnp.exp(floors[u] - top)
        else:
            factor = jnp.exp(bases[u] - top)
            total = totals[u] * factor
        for j in range(low_key, high_key, 2 * pair):
            weights = jnp.exp(sbuf[u, j : j + 2 * pair, :] - top)
            pbuf[u, j : j + 2 * pair, :] = weights.astype(jnp.bfloat16)
            total = total + jnp.sum(weights, axis=0, keepdims=True)
            yield
        totals[u], bases[u] = total, top
        mix = jnp.dot(
            vt[:, low_key:high_key], pbuf[u, low_key:high_key, :], preferred_element_type=jnp.float32
        )
        yield
        if factor is not None:
            mix = mix + mbuf[u] * factor
        if not final:
            mbuf[u] = mix
            return
        mix = mix / total
        count = seg_size(u)
        size = 4 * count
        for part in range(len(units[u])):
            tiles = []
            for h in range(0, qheads, LANES // size):
                base = (part * qheads + h) * size
                tile = jnp.transpose(mix[:, base : base + LANES])
                tiles.extend(tile[i : i + size] for i in range(0, LANES, size))
            att = jnp.concatenate(tiles, axis=1).astype(jnp.bfloat16)
            if len(units[u]) == 1:
                abuf[u] = att
                continue
            for i, (_, core, off) in enumerate(units[u][part]):
                abuf[u, core * rows + off : core * rows + off + count, :] = att[i * count : (i + 1) * count]

    def chain(*tasks):
        for task in tasks:
            yield from task

    def send_out(u, i):
        chip, core, off = (cd, i // 2, 0) if u == 3 else units[u][0][i]
        count = rows if u in (0, 3) else quarter
        src = abuf.at[u, pl.ds(i * quarter, count)]
        dst = obuf.at[pl.ds(off, count), pl.ds(pl.multiple_of(s * qc, qc), qc)]
        return pltpu.make_async_remote_copy(
            src_ref=src, dst_ref=dst, send_sem=osend.at[0],
            recv_sem=orecv.at[0], device_id={"sp": chip * 2 + core},
        )

    def send_out_partner():
        src = abuf.at[0, pl.ds(pl.multiple_of((1 - p) * rows, rows), rows)]
        dst = obuf.at[:, pl.ds(pl.multiple_of(s * qc, qc), qc)]
        return pltpu.make_async_remote_copy(
            src_ref=src, dst_ref=dst, send_sem=osend.at[0],
            recv_sem=orecv.at[0], device_id={"sp": pn},
        )

    def wait_out(sem):
        span = pl.ds(0, (sp - 1) * qc)
        pltpu.make_async_remote_copy(
            src_ref=obuf.at[:, span], dst_ref=obuf.at[:, span], send_sem=sem, recv_sem=sem,
            device_id={"sp": pn},
        ).wait_recv()

    def ship(u):
        if u == 0:
            send_out_partner().start()
            obuf[:, pl.ds(pl.multiple_of(s * qc, qc), qc)] = abuf[
                0, pl.ds(pl.multiple_of(p * rows, rows), rows), :
            ]
        elif u == 3:
            send_out(u, 0).start()
            send_out(u, 2).start()
        else:
            for i in range(4):
                send_out(u, i).start()

    def stage(k):
        qx, qy = (k + half) % pieces, k
        arrived(0, qx)
        if k < half:
            relay(qx).start()
        forward(0, qx, k // half).start()
        arrived(1, qy)
        if k < half:
            relay(qy).start()
        forward(1, qy, k // half).start()

    def stage_far(q):
        for r in (q, q + half):
            arrived(2, r)
            forward(2, r, 2).start()

    def partner(i):
        wait_rows(drecv.at[i], 1)

    stage(0)
    partner(3)
    wq_copy.wait()
    run(project(0, 0))
    for chip, way in ((cx, 2), (cy, 3), (cd, 1)):
        recv_heads(chip, way)
        share(chip)
    near, rest = (c,), (cx, cy, cd)
    pl.when(inner)(lambda: recv_group(0, near))
    prepare(0)
    run(score(0, 0))
    pl.when(inner)(lambda: recv_group(1, near))
    stage(1)
    partner(0)
    run(project(1, 0))
    run(score(1, 0))
    pl.when(outer)(lambda: recv_group(0, near))
    recv_group(0, rest)

    @pl.when(inner)
    def _():
        recv_group(1, rest)
        recv_group(2, near)

    stage(2)
    prepare(1)
    run(score(0, 1), score(1, 1))
    stage(3)
    partner(1)
    run(chain(project(2, 0), score(2, 0), score(2, 1)), chain(absorb(0, [0, 1], []), absorb(1, [0, 1], [])))
    pl.when(outer)(lambda: recv_group(1, near + rest))
    pl.when(inner)(lambda: recv_group(2, rest))
    stage_far(0)
    prepare(2)
    run(absorb(0, [], [2]), absorb(1, [], [2]), score(2, 2))
    stage_far(1)
    run(absorb(2, [0, 1, 2], []))
    partner(2)
    run(chain(project(3, 0), score(3, 0), score(3, 1), score(3, 2), absorb(3, [0, 1, 2], [])))
    pl.when(outer)(lambda: recv_group(2, near + rest))
    prepare(3)
    run(absorb(3, [], [3], True), absorb(1, [], [3], True))
    ship(3)
    ship(1)
    run(absorb(2, [], [3], True), absorb(0, [], [3], True))
    ship(2)
    ship(0)

    wait_out(orecv.at[0])
    out[...] = obuf[...]
    wait_rows(tsend.at[0], sp - 1)
    kept = kvo.at[pl.ds(0, sp - 1)]
    pltpu.make_async_remote_copy(
        src_ref=kept, dst_ref=kept, send_sem=ksend.at[0], recv_sem=ksend.at[0], device_id={"sp": pn}
    ).wait_recv()

    def wait_keys(way, count):
        span = pl.ds(0, count)
        pltpu.make_async_remote_copy(
            src_ref=kvb.at[span], dst_ref=kvb.at[span], send_sem=zsend.at[way],
            recv_sem=zsend.at[way], device_id={"grp": g},
        ).wait_recv()

    pl.when(g > 0)(lambda: wait_keys(1, group_rows))
    pl.when(g < grp - 1)(lambda: wait_keys(0, group_rows))
    pl.when(inner)(lambda: wait_keys(2, 3 * group_rows))
    wait_out(osend.at[0])


def per_plane(tokens, query_weight, key_value_weight, block_places, sinks):
    sp = lax.axis_size("sp")
    grp = lax.axis_size("grp")
    rows, width = tokens.shape
    group_rows = rows * sp
    key_count = grp * group_rows
    qc = query_weight.shape[1]
    qheads = qc // HEAD_SIZE
    pair = 2 * rows
    columns = qheads * pair
    pieces = 4
    hbm = pl.BlockSpec(memory_space=pl.ANY)
    dma = pltpu.SemaphoreType.DMA
    bf16, f32 = jnp.bfloat16, jnp.float32
    result = pl.pallas_call(
        functools.partial(plane_kernel, grp, sp, qheads),
        out_shape=pltpu.VMEM((rows, qc * sp), bf16),
        in_specs=[hbm] * 5,
        out_specs=pl.BlockSpec(memory_space=pltpu.VMEM),
        scratch_shapes=[
            pltpu.SMEM(block_places.shape, block_places.dtype),
            pltpu.SMEM(sinks.shape, sinks.dtype),
            pltpu.VMEM((sp, rows, width), bf16),
            pltpu.VMEM((width, qc), bf16),
            pltpu.VMEM((2, width, 4 * LANES), bf16),
            pltpu.VMEM((sp, rows, LANES), bf16),
            pltpu.VMEM((key_count, LANES), bf16),
            pltpu.VMEM((key_count, LANES), bf16),
            pltpu.VMEM((HEAD_SIZE, key_count), bf16),
            pltpu.VMEM((sp // 2, columns, LANES), bf16),
            pltpu.VMEM((sp // 2, key_count, columns), f32),
            pltpu.VMEM((sp // 2, key_count, columns), bf16),
            pltpu.VMEM((sp // 2, HEAD_SIZE, columns), f32),
            pltpu.VMEM((sp // 2, pair, qc), bf16),
            pltpu.VMEM((rows, qc * sp), bf16),
            pltpu.VMEM((group_rows, LANES), f32),
            pltpu.VMEM((group_rows, LANES), f32),
            pltpu.VMEM((group_rows, LANES), jnp.int32),
            dma((6,)),
            dma((1,)),
            dma((3, pieces)),
            dma((5,)),
            dma((1,)),
            dma((sp // 2,)),
            dma((3,)),
            dma((grp, sp // 2)),
            dma((1,)),
            dma((1,)),
            pltpu.SemaphoreType.REGULAR((2,)),
        ],
        compiler_params=pltpu.CompilerParams(
            has_side_effects=True, collective_id=0, vmem_limit_bytes=60 * 1024 * 1024
        ),
    )(tokens, query_weight, key_value_weight, block_places, sinks)
    return result


def write_out(result, out, sem):
    copy = pltpu.make_async_copy(result, out, sem)
    copy.start()
    copy.wait()


def written(result):
    return pl.pallas_call(
        write_out,
        out_shape=jax.ShapeDtypeStruct(result.shape, result.dtype),
        in_specs=[pl.BlockSpec(memory_space=pltpu.VMEM)],
        out_specs=pl.BlockSpec(memory_space=pl.ANY),
        scratch_shapes=[pltpu.SemaphoreType.DMA],
    )(result)


def local_form(tokens, query_weight, key_value_weight, block_places, sinks):
    sp = lax.axis_size("sp")
    grp = lax.axis_size("grp")
    heads = query_weight.shape[1] // HEAD_SIZE
    kv_total = key_value_weight.shape[1] // (2 * HEAD_SIZE)
    square = sp // 2 == BPG and grp == BPG and kv_total == sp and block_places.shape[0] == grp * BPG
    form = per_plane if square and heads * HEAD_SIZE == 2 * LANES else per_device
    return form(tokens, query_weight, key_value_weight, block_places, sinks)


def solution(mesh):
    in_specs = (P(("grp", "sp"), None), P(None, "sp"), P(), P(), P())
    out_specs = P(("grp", "sp"), None)
    return jax.shard_map(
        local_form, mesh=mesh, in_specs=in_specs, out_specs=out_specs, check_vma=False
    )
```

```python
import functools

import jax
import jax.numpy as jnp
from jax import lax
from jax.experimental import pallas as pl
from jax.experimental.pallas import tpu as pltpu
from jax.sharding import PartitionSpec as P

QUERY_HEADS = 32
HEAD_SIZE = 64
BPG = 4
LANES = 128

rope_base = 150000.0
neg_large = -1e30


def rotate_heads(x, cosine, sine):
    width = x.shape[1]
    half = HEAD_SIZE // 2
    if width % LANES:
        swapped = jnp.concatenate([x[:, half:], x[:, :half]], axis=1)
        return x * cosine[:, :width] + swapped * sine[:, :width]
    parts = []
    lane = lax.broadcasted_iota(jnp.int32, (x.shape[0], LANES), 1)
    first = lane % HEAD_SIZE < half
    for j in range(width // LANES):
        v = x[:, j * LANES : (j + 1) * LANES]
        swapped = jnp.where(first, pltpu.roll(v, LANES - half, 1), pltpu.roll(v, half, 1))
        parts.append(v * cosine + swapped * sine)
    return parts[0] if len(parts) == 1 else jnp.concatenate(parts, axis=1)


def kernel(
    grp, sp, qheads, kv_total,
    tok, wq_any, kvw_any, inverse_ref, places_ref, sink, out,
    toks, wq, wkv, kvb, q, abuf, obuf, cos_ref, sin_ref, qpos, kpos,
    wsem, tsend, tfwd, trecv, ksend, krecv, osend, orecv,
):
    s = lax.axis_index("sp")
    g = lax.axis_index("grp")
    rows = tok.shape[0]
    group_rows = rows * sp
    chips = sp // 2
    pair = 2 * rows
    qc = qheads * HEAD_SIZE
    c = s // 2
    par = s % 2
    partner = s + 1 - 2 * par
    head = s * kv_total // sp
    hpar = head % 2
    koff = pl.multiple_of(head // 2 * LANES, LANES)
    voff = pl.multiple_of(kv_total * HEAD_SIZE + head // 2 * LANES, LANES)

    wcopies = [
        pltpu.make_async_copy(wq_any, wq, wsem.at[0]),
        pltpu.make_async_copy(
            kvw_any.at[:, pl.ds(koff, LANES)], wkv.at[:, pl.ds(0, LANES)], wsem.at[1]
        ),
        pltpu.make_async_copy(
            kvw_any.at[:, pl.ds(voff, LANES)], wkv.at[:, pl.ds(LANES, LANES)], wsem.at[2]
        ),
    ]

    def send_tok(to):
        return pltpu.make_async_remote_copy(
            src_ref=tok, dst_ref=toks.at[s], send_sem=tsend.at[to], recv_sem=trecv.at[s],
            device_id={"sp": to},
        )

    def forward(slot):
        return pltpu.make_async_remote_copy(
            src_ref=toks.at[slot], dst_ref=toks.at[slot], send_sem=tfwd.at[slot],
            recv_sem=trecv.at[slot], device_id={"sp": partner},
        )

    def send_kv(chip, d):
        span = pl.ds(pl.multiple_of(g * group_rows + chip * pair, pair), pair)
        return pltpu.make_async_remote_copy(
            src_ref=kvb.at[span], dst_ref=kvb.at[span], send_sem=ksend.at[d, chip],
            recv_sem=krecv.at[g, chip], device_id={"grp": (g + d) % grp},
        )

    def recv_kv(chip, d):
        src = (g + d) % grp
        span = pl.ds(pl.multiple_of(src * group_rows + chip * pair, pair), pair)
        return pltpu.make_async_remote_copy(
            src_ref=kvb.at[span], dst_ref=kvb.at[span], send_sem=ksend.at[d, chip],
            recv_sem=krecv.at[src, chip], device_id={"grp": src},
        )

    def send_out(to):
        return pltpu.make_async_remote_copy(
            src_ref=abuf.at[to], dst_ref=obuf.at[s], send_sem=osend.at[to],
            recv_sem=orecv.at[s], device_id={"sp": to},
        )

    def recv_out(src):
        return pltpu.make_async_remote_copy(
            src_ref=abuf.at[src], dst_ref=obuf.at[src], send_sem=osend.at[src],
            recv_sem=orecv.at[src], device_id={"sp": src},
        )

    send_tok(partner).start()

    def start_tok(k, _):
        send_tok((c + k) % chips * 2 + par).start()
        return 0

    lax.fori_loop(1, chips, start_tok, 0)
    for copy in wcopies:
        copy.start()
    toks[s] = tok[...]

    block_rows = group_rows // BPG
    for j in range(kpos.shape[1] // block_rows):
        within = lax.broadcasted_iota(jnp.int32, (1, block_rows), 1)
        kpos[:, j * block_rows : (j + 1) * block_rows] = places_ref[j] * block_rows + within
    wide = lax.broadcasted_iota(jnp.int32, (1, LANES), 1)
    half = HEAD_SIZE // 2
    inverse = inverse_ref[...]
    sign = jnp.where(wide % HEAD_SIZE < half, -1.0, 1.0)
    for j in range(BPG):
        rspan = slice(j * block_rows, (j + 1) * block_rows)
        within = lax.broadcasted_iota(jnp.int32, (block_rows, LANES), 0)
        place = places_ref[g * BPG + j] * block_rows + within
        qpos[rspan, :] = place[:, :1]
        angles = place.astype(jnp.float32) * inverse
        cos_ref[rspan, :] = jnp.cos(angles)
        sin_ref[rspan, :] = jnp.sin(angles) * sign
    for copy in wcopies:
        copy.wait()

    def project(k, _):
        chip = (c + chips - k) % chips

        @pl.when(k > 0)
        def _():
            slot = chip * 2 + par
            forward(slot).wait_recv()
            forward(slot).start()

        forward(chip * 2 + 1 - par).wait_recv()
        x = toks[pl.ds(chip * 2, 2)].reshape(pair, tok.shape[1])
        span = pl.ds(pl.multiple_of(chip * pair, pair), pair)
        cosine = cos_ref[span, :]
        sine = sin_ref[span, :]
        kv = jnp.dot(x, wkv[...], preferred_element_type=jnp.float32)
        keys = rotate_heads(kv[:, :LANES], cosine, sine)
        values = kv[:, LANES:]
        low = hpar == 0
        keys = jnp.where(low, keys, pltpu.roll(keys, HEAD_SIZE, 1))
        values = jnp.where(low, pltpu.roll(values, HEAD_SIZE, 1), values)
        lane = lax.broadcasted_iota(jnp.int32, (pair, LANES), 1)
        joined = jnp.where(lane < HEAD_SIZE, keys, values).astype(jnp.bfloat16)
        kvb[pl.ds(pl.multiple_of(g * group_rows + chip * pair, pair), pair), :] = joined
        for d in range(1, grp):
            send_kv(chip, d).start()
        qf = jnp.dot(x, wq[...], preferred_element_type=jnp.float32)
        qr = (rotate_heads(qf, cosine, sine) * HEAD_SIZE**-0.5).astype(jnp.bfloat16)
        zeros = jnp.zeros((pair, HEAD_SIZE), jnp.bfloat16)
        for h in range(qheads):
            q[h, span, :] = jnp.concatenate(
                [qr[:, h * HEAD_SIZE : (h + 1) * HEAD_SIZE], zeros], axis=1
            )
        return 0

    lax.fori_loop(0, chips, project, 0)

    def arrive(chip, _):
        for d in range(1, grp):
            recv_kv(chip, d).wait_recv()
        return 0

    lax.fori_loop(0, chips, arrive, 0)

    key_count = kvb.shape[0]
    chunk = min(key_count, 2048)
    chunks = key_count // chunk
    block = min(256, group_rows)
    tiles = block // rows

    def attention(b, _):
        span = pl.ds(pl.multiple_of(b * block, block), block)
        places = qpos[span, :]
        outs = []
        for h in range(qheads):
            qh = q[h, span, :]

            def visit(t, state):
                top, total, mix = state
                kspan = pl.ds(pl.multiple_of(t * chunk, chunk), chunk)
                kv = kvb[kspan, :]
                scores = lax.dot_general(
                    qh, kv, (((1,), (1,)), ((), ())), preferred_element_type=jnp.float32
                )
                allowed = kpos[:, kspan] <= places
                scores = jnp.where(allowed, scores, neg_large)
                higher = jnp.maximum(top, jnp.max(scores, axis=1, keepdims=True))
                weights = jnp.exp(scores - higher)
                factor = jnp.exp(top - higher)
                total = total * factor + jnp.sum(weights, axis=1, keepdims=True)
                mix = mix * factor + jnp.dot(
                    weights.astype(jnp.bfloat16), kv, preferred_element_type=jnp.float32
                )
                return higher, total, mix

            state = (
                jnp.full((block, 1), sink[s * qheads + h], jnp.float32),
                jnp.ones((block, 1), jnp.float32),
                jnp.zeros((block, LANES), jnp.float32),
            )
            if chunks == 1:
                state = visit(0, state)
            else:
                state = lax.fori_loop(0, chunks, visit, state)
            outs.append((state[2] / state[1])[:, HEAD_SIZE:])
        att = outs[0] if qheads == 1 else jnp.concatenate(outs, axis=1)
        abuf[pl.ds(b * tiles, tiles)] = att.astype(jnp.bfloat16).reshape(tiles, rows, qc)

        def ship(i, _):
            to = b * tiles + i

            @pl.when(to != s)
            def _():
                send_out(to).start()

            return 0

        lax.fori_loop(0, tiles, ship, 0)
        return 0

    lax.fori_loop(0, group_rows // block, attention, 0)
    obuf[s] = abuf[s]

    def drain(j, _):
        @pl.when(j != s)
        def _():
            recv_out(j).wait_recv()
            send_out(j).wait_send()

        return 0

    lax.fori_loop(0, sp, drain, 0)
    for j in range(sp):
        out[:, j * qc : (j + 1) * qc] = obuf[j]
    send_tok(partner).wait_send()

    def finish(k, _):
        send_tok((c + k) % chips * 2 + par).wait_send()
        forward((c + chips - k) % chips * 2 + par).wait_send()
        return 0

    lax.fori_loop(1, chips, finish, 0)

    def finish_kv(chip, _):
        for d in range(1, grp):
            send_kv(chip, d).wait_send()
        return 0

    lax.fori_loop(0, chips, finish_kv, 0)


def per_device(tokens, query_weight, key_value_weight, block_places, sinks):
    sp = lax.axis_size("sp")
    grp = lax.axis_size("grp")
    rows, width = tokens.shape
    group_rows = rows * sp
    key_count = grp * group_rows
    qc = query_weight.shape[1]
    qheads = qc // HEAD_SIZE
    kv_total = key_value_weight.shape[1] // (2 * HEAD_SIZE)
    freq = jnp.arange(HEAD_SIZE // 2, dtype=jnp.float32)
    inverse = rope_base ** (-(freq * 2.0) / HEAD_SIZE)
    inverse = jnp.tile(inverse, LANES // (HEAD_SIZE // 2)).reshape(1, LANES)

    vmem = pl.BlockSpec(memory_space=pltpu.VMEM)
    hbm = pl.BlockSpec(memory_space=pl.ANY)
    smem = pl.BlockSpec(memory_space=pltpu.SMEM)
    dma = pltpu.SemaphoreType.DMA
    return pl.pallas_call(
        functools.partial(kernel, grp, sp, qheads, kv_total),
        out_shape=jax.ShapeDtypeStruct((rows, qc * sp), jnp.bfloat16),
        in_specs=[vmem, hbm, hbm, vmem, smem, smem],
        out_specs=vmem,
        scratch_shapes=[
            pltpu.VMEM((sp, rows, width), jnp.bfloat16),
            pltpu.VMEM((width, qc), jnp.bfloat16),
            pltpu.VMEM((width, 2 * LANES), jnp.bfloat16),
            pltpu.VMEM((key_count, LANES), jnp.bfloat16),
            pltpu.VMEM((qheads, group_rows, LANES), jnp.bfloat16),
            pltpu.VMEM((sp, rows, qc), jnp.bfloat16),
            pltpu.VMEM((sp, rows, qc), jnp.bfloat16),
            pltpu.VMEM((group_rows, LANES), jnp.float32),
            pltpu.VMEM((group_rows, LANES), jnp.float32),
            pltpu.VMEM((group_rows, 1), jnp.int32),
            pltpu.VMEM((1, key_count), jnp.int32),
            dma((3,)),
            dma((sp,)),
            dma((sp,)),
            dma((sp,)),
            dma((grp, sp // 2)),
            dma((grp, sp // 2)),
            dma((sp,)),
            dma((sp,)),
        ],
        compiler_params=pltpu.CompilerParams(
            has_side_effects=True, vmem_limit_bytes=60 * 1024 * 1024
        ),
    )(tokens, query_weight, key_value_weight, inverse, block_places, sinks)


def plane_kernel(
    grp, sp, qheads,
    tok_any, wq_any, kvw_any, places_any, sinks_any, out,
    places, sinks,    toks, wq, kvw, kvo, kvb, kaug, vt, qs, sbuf, pbuf, mbuf, abuf, obuf, cos_ref, sin_ref, kpos,
    wsem, tsend, trecv, drecv, ksend, krecv, zsend, zrecv, osend, orecv, ready,
):
    s = lax.axis_index("sp")
    g = lax.axis_index("grp")
    rows, width = toks.shape[1:]
    pieces = trecv.shape[1]
    piece_rows = rows // pieces
    half = pieces // 2
    pair = 2 * rows
    group_rows = rows * sp
    chips = sp // 2
    qc = qheads * HEAD_SIZE
    blocks = grp * BPG
    dim = HEAD_SIZE // 2
    p = s % 2
    c = s // 2
    cx = c + 1 - 2 * (c % 2)
    cy = (c + chips // 2) % chips
    cd = (cx + chips // 2) % chips
    xn, yn, dn, pn = cx * 2 + p, cy * 2 + p, cd * 2 + p, c * 2 + 1 - p
    key_base = g * group_rows

    chip_order = [c, cx, cy, cd]
    ways = [0, 2, 3, 1]
    wcopies = []
    for k, chip in enumerate(chip_order):
        koff = pl.multiple_of(chip * LANES, LANES)
        voff = pl.multiple_of(sp * HEAD_SIZE + chip * LANES, LANES)
        for part, off in enumerate((koff, voff)):
            wcopies.append(
                pltpu.make_async_copy(
                    kvw_any.at[:, pl.ds(off, LANES)],
                    kvw.at[k // 2, :, pl.ds((2 * (k % 2) + part) * LANES, LANES)],
                    wsem.at[2 + k // 2],
                )
            )
    tok_copy = pltpu.make_async_copy(tok_any, toks.at[s], wsem.at[0])
    wq_copy = pltpu.make_async_copy(wq_any, wq, wsem.at[1])
    pcopy = pltpu.make_async_copy(places_any, places, wsem.at[4])
    scopy = pltpu.make_async_copy(sinks_any, sinks, wsem.at[5])
    pcopy.start()
    scopy.start()
    tok_copy.start()
    for copy in wcopies:
        copy.start()
    wq_copy.start()

    barrier = pltpu.get_barrier_semaphore()
    upper = c >= chips // 2
    for to in (xn, yn, pn, cx * 2 + 1 - p, cy * 2 + 1 - p):
        pl.semaphore_signal(barrier, inc=1, device_id={"sp": to})

    @pl.when(jnp.logical_not(upper))
    def _():
        for core in range(2):
            pl.semaphore_signal(barrier, inc=1, device_id={"sp": cd * 2 + core})

    @pl.when(g < grp - 1)
    def _():
        pl.semaphore_signal(barrier, inc=1, device_id={"grp": g + 1})

    def send_piece(slot, q, to, sem):
        span = pl.ds(q * piece_rows, piece_rows)
        return pltpu.make_async_remote_copy(
            src_ref=toks.at[slot, span], dst_ref=toks.at[slot, span], send_sem=tsend.at[0],
            recv_sem=sem, device_id={"sp": to},
        )

    def send_own(slot, to):
        return pltpu.make_async_remote_copy(
            src_ref=toks.at[slot], dst_ref=toks.at[slot], send_sem=tsend.at[0],
            recv_sem=drecv.at[3], device_id={"sp": to},
        )

    def send_x(q):
        return send_piece(s, q, xn, trecv.at[0, q])

    def send_y(q):
        return send_piece(s, q, yn, trecv.at[1, q])

    def relay(q):
        if q >= half:
            return send_piece(xn, q, yn, trecv.at[2, q])
        return send_piece(yn, q, xn, trecv.at[2, q])

    def arrived(k, q):
        send_piece((xn, yn, dn)[k], q, pn, trecv.at[k, q]).wait_recv()

    def forward(k, q, i):
        return send_piece((xn, yn, dn)[k], q, pn, drecv.at[i])

    def wait_rows(sem, slots, count=rows):
        area = toks.at[pl.ds(0, slots), pl.ds(0, count)]
        pltpu.make_async_remote_copy(
            src_ref=area, dst_ref=area, send_sem=sem, recv_sem=sem, device_id={"sp": pn}
        ).wait_recv()

    def send_head(i, to, way):
        span = pl.ds(pl.multiple_of(key_base + s * rows, rows), rows)
        return pltpu.make_async_remote_copy(
            src_ref=kvo.at[i], dst_ref=kvb.at[span], send_sem=ksend.at[0],
            recv_sem=krecv.at[way], device_id={"sp": to},
        )

    def recv_heads(chip, way):
        span = pl.ds(pl.multiple_of(key_base + chip * pair, pair), rows if way == 0 else pair)
        pltpu.make_async_remote_copy(
            src_ref=kvb.at[span], dst_ref=kvb.at[span], send_sem=ksend.at[0],
            recv_sem=krecv.at[way], device_id={"sp": pn},
        ).wait_recv()

    def send_chunk(group, chip, to, way):
        span = pl.ds(pl.multiple_of(group * group_rows + chip * pair, pair), pair)
        return pltpu.make_async_remote_copy(
            src_ref=kvb.at[span], dst_ref=kvb.at[span], send_sem=zsend.at[way],
            recv_sem=zrecv.at[group, chip], device_id={"grp": to},
        )

    def share(chip):
        @pl.when(g > 0)
        def _():
            send_chunk(g, chip, g - 1, 1).start()

        @pl.when(g < grp - 1)
        def _():
            send_chunk(g, chip, g + 1, 0).start()

    inner = jnp.logical_and(g > 0, g < grp - 1)
    others = [jnp.abs(g - 1), 2 + g // 2 - 2 * (g // 3), 3 - 3 * (g // 2)]
    targets = [g + 1, g - 1, 3 * (g // 2)]

    def pass_on(k, chip):
        return send_chunk(others[k], chip, targets[k], 2)

    outer = jnp.logical_not(inner)

    def recv_group(k, chip_list):
        for chip in chip_list:
            send_chunk(others[k], chip, g, 0).wait_recv()

            @pl.when(inner)
            def _():
                pass_on(k, chip).start()

    pcopy.wait()
    scopy.wait()
    wide = lax.broadcasted_iota(jnp.int32, (1, LANES), 1)
    inverse = jnp.ones((1, LANES), jnp.float32)
    bit = 1
    while bit < dim:
        factor = rope_base ** (-2.0 * bit / HEAD_SIZE)
        inverse = jnp.where(wide // bit % 2 == 1, inverse * factor, inverse)
        bit *= 2
    sign = jnp.where(wide % HEAD_SIZE < dim, -1.0, 1.0)
    own_place = places[g * BPG + c] * pair + p * rows + lax.broadcasted_iota(jnp.int32, (rows, LANES), 0)
    own_angles = own_place.astype(jnp.float32) * inverse
    own_cos, own_sin = jnp.cos(own_angles), jnp.sin(own_angles) * sign
    tok_copy.wait()
    pl.semaphore_wait(barrier, 5 + jnp.minimum(g, 1) + 2 * (c // (chips // 2)))
    send_own(s, pn).start()
    send_x(half).start()
    send_y(0).start()

    @pl.when(g > 0)
    def _():
        pl.semaphore_signal(ready.at[0], inc=1, device_id={"grp": g - 1})

    @pl.when(upper)
    def _():
        for core in range(2):
            pl.semaphore_signal(ready.at[1], inc=1, device_id={"sp": cd * 2 + core})

    own_x = toks[s]
    low = lax.broadcasted_iota(jnp.int32, (rows, LANES), 1) < HEAD_SIZE
    for k in range(chips):
        if k % 2 == 0:
            pltpu.make_async_copy(
                kvw_any.at[:, pl.ds(0, 4 * LANES)], kvw.at[k // 2], wsem.at[2 + k // 2]
            ).wait()
            both = jnp.dot(own_x, kvw[k // 2], preferred_element_type=jnp.float32)
        kv = both[:, k % 2 * 2 * LANES : (k % 2 + 1) * 2 * LANES]
        keys = rotate_heads(kv[:, :LANES], own_cos, own_sin)
        values = kv[:, LANES:]
        first = jnp.where(low, keys, pltpu.roll(values, HEAD_SIZE, 1)).astype(jnp.bfloat16)
        second = jnp.where(low, pltpu.roll(keys, HEAD_SIZE, 1), values).astype(jnp.bfloat16)
        way = ways[k]
        if way == 0:
            mine = p == 0
            kvb[pl.ds(pl.multiple_of(key_base + s * rows, rows), rows), :] = jnp.where(mine, first, second)
            kvo[0] = jnp.where(mine, second, first)
            send_head(0, pn, 0).start()
        else:
            chip = chip_order[k]
            kvo[2 * way - 1] = first
            kvo[2 * way] = second
            if way == 1:
                pl.when(jnp.logical_not(upper))(lambda: pl.semaphore_wait(ready.at[1], 2))
            send_head(2 * way - 1, chip * 2, way).start()
            send_head(2 * way, chip * 2 + 1, way).start()

    for q in range(1, half):
        send_x(half + q).start()
        send_y(q).start()
    for q in range(half):
        send_x(q).start()
        send_y(half + q).start()

    recv_heads(c, 0)
    pl.when(g < grp - 1)(lambda: pl.semaphore_wait(ready.at[0], 1))
    share(c)
    for j in range(BPG):
        rspan = slice(j * pair, (j + 1) * pair)
        within = lax.broadcasted_iota(jnp.int32, (pair, LANES), 0)
        place = places[g * BPG + j] * pair + within
        kpos[rspan, :] = place
        angles = place.astype(jnp.float32) * inverse
        cos_ref[rspan, :] = jnp.cos(angles)
        sin_ref[rspan, :] = jnp.sin(angles) * sign
    block_place = jnp.full((1, LANES), -1, jnp.int32)
    for e in range(blocks):
        block_place = jnp.where(wide == HEAD_SIZE + e, places[e], block_place)

    quarter = rows // 2
    units = [
        [[(c, 0, 0), (c, 0, quarter), (c, 1, 0), (c, 1, quarter)]],
        [[(cx, 0, quarter), (cx, 1, quarter), (cy, 0, 0), (cy, 1, 0)]],
        [[(cx, 0, 0), (cx, 1, 0), (cy, 0, quarter), (cy, 1, quarter)]],
        [[(cd, 0, 0), (cd, 0, quarter), (cd, 1, 0), (cd, 1, quarter)]],
    ]

    def seg_size(u):
        return quarter // len(units[u])

    def seg_rows(ref, seg, count):
        chip, core, off = seg
        return ref[pl.ds(pl.multiple_of(chip * pair + core * rows + off, count), count), :]

    def run(*tasks):
        tasks = list(tasks)
        while tasks:
            for task in list(tasks):
                try:
                    next(task)
                except StopIteration:
                    tasks.remove(task)

    def project(u, part):
        segs, count = units[u][part], seg_size(u)
        size = 4 * count
        x = jnp.concatenate([toks[chip * 2 + core, off : off + count] for chip, core, off in segs], axis=0)
        cosine = jnp.concatenate([seg_rows(cos_ref, seg, count) for seg in segs], axis=0)
        sine = jnp.concatenate([seg_rows(sin_ref, seg, count) for seg in segs], axis=0)
        qf = jnp.dot(x, wq[...], preferred_element_type=jnp.float32)
        yield
        qr = rotate_heads(qf, cosine, sine) * HEAD_SIZE**-0.5
        hidden = jnp.concatenate([
            jnp.broadcast_to(
                jnp.where(block_place > places[g * BPG + chip], neg_large, 0.0), (count, LANES)
            )
            for chip, _, _ in segs
        ], axis=0)
        lower = lax.broadcasted_iota(jnp.int32, (size, LANES), 1) < HEAD_SIZE
        for h in range(qheads):
            v = qr[:, h // 2 * LANES : (h // 2 + 1) * LANES]
            if h % 2:
                v = pltpu.roll(v, HEAD_SIZE, 1)
            base = (part * qheads + h) * size
            qs[u, base : base + size, :] = jnp.where(lower, v, hidden).astype(jnp.bfloat16)
            yield

    def query_places(u, part):
        count = seg_size(u)
        size = 4 * count
        row = lax.broadcasted_iota(jnp.int32, (1, qheads * size), 1) % size
        place = jnp.zeros(row.shape, jnp.int32)
        for i, (chip, core, off) in enumerate(units[u][part]):
            base = places[g * BPG + chip] * pair + core * rows + off
            place = jnp.where(row // count == i, base + row % count, place)
        return place

    def sink_row(u):
        size = 4 * seg_size(u)
        head = lax.broadcasted_iota(jnp.int32, (1, qheads * size), 1) // size
        row = jnp.full(head.shape, sinks[s * qheads], jnp.float32)
        for h in range(1, qheads):
            row = jnp.where(head == h, sinks[s * qheads + h], row)
        return row

    def prepare(k):
        group = g if k == 0 else others[k - 1]
        lane = lax.broadcasted_iota(jnp.int32, (pair, LANES), 1)
        for j in range(chips):
            kv = kvb[pl.ds(pl.multiple_of(group * group_rows + j * pair, pair), pair), :]
            mark = jnp.where(lane == HEAD_SIZE + group * BPG + j, 1.0, 0.0).astype(jnp.bfloat16)
            span = slice(k * group_rows + j * pair, k * group_rows + (j + 1) * pair)
            kaug[span, :] = jnp.where(lane < HEAD_SIZE, kv, mark)
            vt[:, span] = jnp.transpose(kv)[HEAD_SIZE:]

    tops = [[sink_row(u) for _ in units[u]] for u in range(len(units))]

    def joined(rows_of):
        return rows_of[0] if len(rows_of) == 1 else jnp.concatenate(rows_of, axis=1)

    floors = [joined(tops[u]) for u in range(len(units))]

    def part_scores(u, k, part):
        width_of = qheads * 4 * seg_size(u)
        side = slice(part * width_of, (part + 1) * width_of)
        span = slice(k * group_rows, (k + 1) * group_rows)
        whole = lax.dot_general(
            kaug[span, :], qs[u, side, :], (((1,), (1,)), ((), ())), preferred_element_type=jnp.float32
        )
        yield
        for j in range(0, group_rows, pair):
            piece = whole[j : j + pair, :]
            if k == 0:
                seen = jnp.concatenate([kpos[j : j + pair, :]] * (width_of // LANES), axis=1)
                piece = jnp.where(seen <= query_places(u, part), piece, neg_large)
            sbuf[u, k * group_rows + j : k * group_rows + j + pair, side] = piece
            tops[u][part] = jnp.maximum(tops[u][part], jnp.max(piece, axis=0, keepdims=True))
            yield

    def score(u, k):
        for part in range(len(units[u])):
            yield from part_scores(u, k, part)

    bases = [None for _ in units]
    totals = [None for _ in units]

    def absorb(u, stored, fresh, final=False):
        low_key = min(stored + fresh) * group_rows
        high_key = (max(stored + fresh) + 1) * group_rows
        for k in fresh:
            yield from score(u, k)
        top = joined(tops[u])
        factor = None
        if bases[u] is None:
            total = jnp.exp(floors[u] - top)
        else:
            factor = jnp.exp(bases[u] - top)
            total = totals[u] * factor
        for j in range(low_key, high_key, 2 * pair):
            weights = jnp.exp(sbuf[u, j : j + 2 * pair, :] - top)
            pbuf[u, j : j + 2 * pair, :] = weights.astype(jnp.bfloat16)
            total = total + jnp.sum(weights, axis=0, keepdims=True)
            yield
        totals[u], bases[u] = total, top
        mix = jnp.dot(
            vt[:, low_key:high_key], pbuf[u, low_key:high_key, :], preferred_element_type=jnp.float32
        )
        yield
        if factor is not None:
            mix = mix + mbuf[u] * factor
        if not final:
            mbuf[u] = mix
            return
        mix = mix / total
        count = seg_size(u)
        size = 4 * count
        for part in range(len(units[u])):
            tiles = []
            for h in range(0, qheads, LANES // size):
                base = (part * qheads + h) * size
                tile = jnp.transpose(mix[:, base : base + LANES])
                tiles.extend(tile[i : i + size] for i in range(0, LANES, size))
            att = jnp.concatenate(tiles, axis=1).astype(jnp.bfloat16)
            if len(units[u]) == 1:
                abuf[u] = att
                continue
            for i, (_, core, off) in enumerate(units[u][part]):
                abuf[u, core * rows + off : core * rows + off + count, :] = att[i * count : (i + 1) * count]

    def chain(*tasks):
        for task in tasks:
            yield from task

    def send_out(u, i):
        chip, core, off = (cd, i // 2, 0) if u == 3 else units[u][0][i]
        count = rows if u in (0, 3) else quarter
        src = abuf.at[u, pl.ds(i * quarter, count)]
        dst = obuf.at[pl.ds(off, count), pl.ds(pl.multiple_of(s * qc, qc), qc)]
        return pltpu.make_async_remote_copy(
            src_ref=src, dst_ref=dst, send_sem=osend.at[0],
            recv_sem=orecv.at[0], device_id={"sp": chip * 2 + core},
        )

    def send_out_partner():
        src = abuf.at[0, pl.ds(pl.multiple_of((1 - p) * rows, rows), rows)]
        dst = obuf.at[:, pl.ds(pl.multiple_of(s * qc, qc), qc)]
        return pltpu.make_async_remote_copy(
            src_ref=src, dst_ref=dst, send_sem=osend.at[0],
            recv_sem=orecv.at[0], device_id={"sp": pn},
        )

    def wait_out(sem):
        span = pl.ds(0, (sp - 1) * qc)
        pltpu.make_async_remote_copy(
            src_ref=obuf.at[:, span], dst_ref=obuf.at[:, span], send_sem=sem, recv_sem=sem,
            device_id={"sp": pn},
        ).wait_recv()

    def ship(u):
        if u == 0:
            send_out_partner().start()
            obuf[:, pl.ds(pl.multiple_of(s * qc, qc), qc)] = abuf[
                0, pl.ds(pl.multiple_of(p * rows, rows), rows), :
            ]
        elif u == 3:
            send_out(u, 0).start()
            send_out(u, 2).start()
        else:
            for i in range(4):
                send_out(u, i).start()

    def stage(k):
        qx, qy = (k + half) % pieces, k
        arrived(0, qx)
        if k < half:
            relay(qx).start()
        forward(0, qx, k // half).start()
        arrived(1, qy)
        if k < half:
            relay(qy).start()
        forward(1, qy, k // half).start()

    def stage_far(q):
        for r in (q, q + half):
            arrived(2, r)
            forward(2, r, 2).start()

    def partner(i):
        wait_rows(drecv.at[i], 1)

    stage(0)
    partner(3)
    wq_copy.wait()
    run(project(0, 0))
    for chip, way in ((cx, 2), (cy, 3), (cd, 1)):
        recv_heads(chip, way)
        share(chip)
    near, rest = (c,), (cx, cy, cd)
    pl.when(inner)(lambda: recv_group(0, near))
    prepare(0)
    run(score(0, 0))
    pl.when(inner)(lambda: recv_group(1, near))
    stage(1)
    partner(0)
    run(project(1, 0))
    run(score(1, 0))
    pl.when(outer)(lambda: recv_group(0, near))
    recv_group(0, rest)

    @pl.when(inner)
    def _():
        recv_group(1, rest)
        recv_group(2, near)

    stage(2)
    prepare(1)
    run(score(0, 1), score(1, 1))
    stage(3)
    partner(1)
    run(chain(project(2, 0), score(2, 0), score(2, 1)), chain(absorb(0, [0, 1], []), absorb(1, [0, 1], [])))
    pl.when(outer)(lambda: recv_group(1, near + rest))
    pl.when(inner)(lambda: recv_group(2, rest))
    stage_far(0)
    pl.when(p == 1)(lambda: stage_far(1))
    prepare(2)
    run(absorb(0, [], [2]), absorb(1, [], [2]), score(2, 2))
    pl.when(p == 0)(lambda: stage_far(1))
    run(absorb(2, [0, 1, 2], []))
    partner(2)
    run(chain(project(3, 0), score(3, 0), score(3, 1), score(3, 2), absorb(3, [0, 1, 2], [])))
    pl.when(outer)(lambda: recv_group(2, near + rest))
    prepare(3)
    run(absorb(3, [], [3], True))
    ship(3)
    run(absorb(1, [], [3], True), absorb(2, [], [3], True))
    ship(1)
    ship(2)
    run(absorb(0, [], [3], True))
    ship(0)

    wait_out(orecv.at[0])
    out[...] = obuf[...]
    wait_rows(tsend.at[0], sp - 1)
    kept = kvo.at[pl.ds(0, sp - 1)]
    pltpu.make_async_remote_copy(
        src_ref=kept, dst_ref=kept, send_sem=ksend.at[0], recv_sem=ksend.at[0], device_id={"sp": pn}
    ).wait_recv()

    def wait_keys(way, count):
        span = pl.ds(0, count)
        pltpu.make_async_remote_copy(
            src_ref=kvb.at[span], dst_ref=kvb.at[span], send_sem=zsend.at[way],
            recv_sem=zsend.at[way], device_id={"grp": g},
        ).wait_recv()

    pl.when(g > 0)(lambda: wait_keys(1, group_rows))
    pl.when(g < grp - 1)(lambda: wait_keys(0, group_rows))
    pl.when(inner)(lambda: wait_keys(2, 3 * group_rows))
    wait_out(osend.at[0])


def per_plane(tokens, query_weight, key_value_weight, block_places, sinks):
    sp = lax.axis_size("sp")
    grp = lax.axis_size("grp")
    rows, width = tokens.shape
    group_rows = rows * sp
    key_count = grp * group_rows
    qc = query_weight.shape[1]
    qheads = qc // HEAD_SIZE
    pair = 2 * rows
    columns = qheads * pair
    pieces = 4
    hbm = pl.BlockSpec(memory_space=pl.ANY)
    dma = pltpu.SemaphoreType.DMA
    bf16, f32 = jnp.bfloat16, jnp.float32
    result = pl.pallas_call(
        functools.partial(plane_kernel, grp, sp, qheads),
        out_shape=pltpu.VMEM((rows, qc * sp), bf16),
        in_specs=[hbm] * 5,
        out_specs=pl.BlockSpec(memory_space=pltpu.VMEM),
        scratch_shapes=[
            pltpu.SMEM(block_places.shape, block_places.dtype),
            pltpu.SMEM(sinks.shape, sinks.dtype),
            pltpu.VMEM((sp, rows, width), bf16),
            pltpu.VMEM((width, qc), bf16),
            pltpu.VMEM((2, width, 4 * LANES), bf16),
            pltpu.VMEM((sp, rows, LANES), bf16),
            pltpu.VMEM((key_count, LANES), bf16),
            pltpu.VMEM((key_count, LANES), bf16),
            pltpu.VMEM((HEAD_SIZE, key_count), bf16),
            pltpu.VMEM((sp // 2, columns, LANES), bf16),
            pltpu.VMEM((sp // 2, key_count, columns), f32),
            pltpu.VMEM((sp // 2, key_count, columns), bf16),
            pltpu.VMEM((sp // 2, HEAD_SIZE, columns), f32),
            pltpu.VMEM((sp // 2, pair, qc), bf16),
            pltpu.VMEM((rows, qc * sp), bf16),
            pltpu.VMEM((group_rows, LANES), f32),
            pltpu.VMEM((group_rows, LANES), f32),
            pltpu.VMEM((group_rows, LANES), jnp.int32),
            dma((6,)),
            dma((1,)),
            dma((3, pieces)),
            dma((5,)),
            dma((1,)),
            dma((sp // 2,)),
            dma((3,)),
            dma((grp, sp // 2)),
            dma((1,)),
            dma((1,)),
            pltpu.SemaphoreType.REGULAR((2,)),
        ],
        compiler_params=pltpu.CompilerParams(
            has_side_effects=True, collective_id=0, vmem_limit_bytes=60 * 1024 * 1024
        ),
    )(tokens, query_weight, key_value_weight, block_places, sinks)
    return result


def write_out(result, out, sem):
    copy = pltpu.make_async_copy(result, out, sem)
    copy.start()
    copy.wait()


def written(result):
    return pl.pallas_call(
        write_out,
        out_shape=jax.ShapeDtypeStruct(result.shape, result.dtype),
        in_specs=[pl.BlockSpec(memory_space=pltpu.VMEM)],
        out_specs=pl.BlockSpec(memory_space=pl.ANY),
        scratch_shapes=[pltpu.SemaphoreType.DMA],
    )(result)


def local_form(tokens, query_weight, key_value_weight, block_places, sinks):
    sp = lax.axis_size("sp")
    grp = lax.axis_size("grp")
    heads = query_weight.shape[1] // HEAD_SIZE
    kv_total = key_value_weight.shape[1] // (2 * HEAD_SIZE)
    square = sp // 2 == BPG and grp == BPG and kv_total == sp and block_places.shape[0] == grp * BPG
    form = per_plane if square and heads * HEAD_SIZE == 2 * LANES else per_device
    return form(tokens, query_weight, key_value_weight, block_places, sinks)


def solution(mesh):
    in_specs = (P(("grp", "sp"), None), P(None, "sp"), P(), P(), P())
    out_specs = P(("grp", "sp"), None)
    return jax.shard_map(
        local_form, mesh=mesh, in_specs=in_specs, out_specs=out_specs, check_vma=False
    )
```

```python
import functools

import jax
import jax.numpy as jnp
from jax import lax
from jax.experimental import pallas as pl
from jax.experimental.pallas import tpu as pltpu
from jax.sharding import PartitionSpec as P

QUERY_HEADS = 32
HEAD_SIZE = 64
BPG = 4
LANES = 128

rope_base = 150000.0
neg_large = -1e30


def rotate_heads(x, cosine, sine):
    width = x.shape[1]
    half = HEAD_SIZE // 2
    if width % LANES:
        swapped = jnp.concatenate([x[:, half:], x[:, :half]], axis=1)
        return x * cosine[:, :width] + swapped * sine[:, :width]
    parts = []
    lane = lax.broadcasted_iota(jnp.int32, (x.shape[0], LANES), 1)
    first = lane % HEAD_SIZE < half
    for j in range(width // LANES):
        v = x[:, j * LANES : (j + 1) * LANES]
        swapped = jnp.where(first, pltpu.roll(v, LANES - half, 1), pltpu.roll(v, half, 1))
        parts.append(v * cosine + swapped * sine)
    return parts[0] if len(parts) == 1 else jnp.concatenate(parts, axis=1)


def kernel(
    grp, sp, qheads, kv_total,
    tok, wq_any, kvw_any, inverse_ref, places_ref, sink, out,
    toks, wq, wkv, kvb, q, abuf, obuf, cos_ref, sin_ref, qpos, kpos,
    wsem, tsend, tfwd, trecv, ksend, krecv, osend, orecv,
):
    s = lax.axis_index("sp")
    g = lax.axis_index("grp")
    rows = tok.shape[0]
    group_rows = rows * sp
    chips = sp // 2
    pair = 2 * rows
    qc = qheads * HEAD_SIZE
    c = s // 2
    par = s % 2
    partner = s + 1 - 2 * par
    head = s * kv_total // sp
    hpar = head % 2
    koff = pl.multiple_of(head // 2 * LANES, LANES)
    voff = pl.multiple_of(kv_total * HEAD_SIZE + head // 2 * LANES, LANES)

    wcopies = [
        pltpu.make_async_copy(wq_any, wq, wsem.at[0]),
        pltpu.make_async_copy(
            kvw_any.at[:, pl.ds(koff, LANES)], wkv.at[:, pl.ds(0, LANES)], wsem.at[1]
        ),
        pltpu.make_async_copy(
            kvw_any.at[:, pl.ds(voff, LANES)], wkv.at[:, pl.ds(LANES, LANES)], wsem.at[2]
        ),
    ]

    def send_tok(to):
        return pltpu.make_async_remote_copy(
            src_ref=tok, dst_ref=toks.at[s], send_sem=tsend.at[to], recv_sem=trecv.at[s],
            device_id={"sp": to},
        )

    def forward(slot):
        return pltpu.make_async_remote_copy(
            src_ref=toks.at[slot], dst_ref=toks.at[slot], send_sem=tfwd.at[slot],
            recv_sem=trecv.at[slot], device_id={"sp": partner},
        )

    def send_kv(chip, d):
        span = pl.ds(pl.multiple_of(g * group_rows + chip * pair, pair), pair)
        return pltpu.make_async_remote_copy(
            src_ref=kvb.at[span], dst_ref=kvb.at[span], send_sem=ksend.at[d, chip],
            recv_sem=krecv.at[g, chip], device_id={"grp": (g + d) % grp},
        )

    def recv_kv(chip, d):
        src = (g + d) % grp
        span = pl.ds(pl.multiple_of(src * group_rows + chip * pair, pair), pair)
        return pltpu.make_async_remote_copy(
            src_ref=kvb.at[span], dst_ref=kvb.at[span], send_sem=ksend.at[d, chip],
            recv_sem=krecv.at[src, chip], device_id={"grp": src},
        )

    def send_out(to):
        return pltpu.make_async_remote_copy(
            src_ref=abuf.at[to], dst_ref=obuf.at[s], send_sem=osend.at[to],
            recv_sem=orecv.at[s], device_id={"sp": to},
        )

    def recv_out(src):
        return pltpu.make_async_remote_copy(
            src_ref=abuf.at[src], dst_ref=obuf.at[src], send_sem=osend.at[src],
            recv_sem=orecv.at[src], device_id={"sp": src},
        )

    send_tok(partner).start()

    def start_tok(k, _):
        send_tok((c + k) % chips * 2 + par).start()
        return 0

    lax.fori_loop(1, chips, start_tok, 0)
    for copy in wcopies:
        copy.start()
    toks[s] = tok[...]

    block_rows = group_rows // BPG
    for j in range(kpos.shape[1] // block_rows):
        within = lax.broadcasted_iota(jnp.int32, (1, block_rows), 1)
        kpos[:, j * block_rows : (j + 1) * block_rows] = places_ref[j] * block_rows + within
    wide = lax.broadcasted_iota(jnp.int32, (1, LANES), 1)
    half = HEAD_SIZE // 2
    inverse = inverse_ref[...]
    sign = jnp.where(wide % HEAD_SIZE < half, -1.0, 1.0)
    for j in range(BPG):
        rspan = slice(j * block_rows, (j + 1) * block_rows)
        within = lax.broadcasted_iota(jnp.int32, (block_rows, LANES), 0)
        place = places_ref[g * BPG + j] * block_rows + within
        qpos[rspan, :] = place[:, :1]
        angles = place.astype(jnp.float32) * inverse
        cos_ref[rspan, :] = jnp.cos(angles)
        sin_ref[rspan, :] = jnp.sin(angles) * sign
    for copy in wcopies:
        copy.wait()

    def project(k, _):
        chip = (c + chips - k) % chips

        @pl.when(k > 0)
        def _():
            slot = chip * 2 + par
            forward(slot).wait_recv()
            forward(slot).start()

        forward(chip * 2 + 1 - par).wait_recv()
        x = toks[pl.ds(chip * 2, 2)].reshape(pair, tok.shape[1])
        span = pl.ds(pl.multiple_of(chip * pair, pair), pair)
        cosine = cos_ref[span, :]
        sine = sin_ref[span, :]
        kv = jnp.dot(x, wkv[...], preferred_element_type=jnp.float32)
        keys = rotate_heads(kv[:, :LANES], cosine, sine)
        values = kv[:, LANES:]
        low = hpar == 0
        keys = jnp.where(low, keys, pltpu.roll(keys, HEAD_SIZE, 1))
        values = jnp.where(low, pltpu.roll(values, HEAD_SIZE, 1), values)
        lane = lax.broadcasted_iota(jnp.int32, (pair, LANES), 1)
        joined = jnp.where(lane < HEAD_SIZE, keys, values).astype(jnp.bfloat16)
        kvb[pl.ds(pl.multiple_of(g * group_rows + chip * pair, pair), pair), :] = joined
        for d in range(1, grp):
            send_kv(chip, d).start()
        qf = jnp.dot(x, wq[...], preferred_element_type=jnp.float32)
        qr = (rotate_heads(qf, cosine, sine) * HEAD_SIZE**-0.5).astype(jnp.bfloat16)
        zeros = jnp.zeros((pair, HEAD_SIZE), jnp.bfloat16)
        for h in range(qheads):
            q[h, span, :] = jnp.concatenate(
                [qr[:, h * HEAD_SIZE : (h + 1) * HEAD_SIZE], zeros], axis=1
            )
        return 0

    lax.fori_loop(0, chips, project, 0)

    def arrive(chip, _):
        for d in range(1, grp):
            recv_kv(chip, d).wait_recv()
        return 0

    lax.fori_loop(0, chips, arrive, 0)

    key_count = kvb.shape[0]
    chunk = min(key_count, 2048)
    chunks = key_count // chunk
    block = min(256, group_rows)
    tiles = block // rows

    def attention(b, _):
        span = pl.ds(pl.multiple_of(b * block, block), block)
        places = qpos[span, :]
        outs = []
        for h in range(qheads):
            qh = q[h, span, :]

            def visit(t, state):
                top, total, mix = state
                kspan = pl.ds(pl.multiple_of(t * chunk, chunk), chunk)
                kv = kvb[kspan, :]
                scores = lax.dot_general(
                    qh, kv, (((1,), (1,)), ((), ())), preferred_element_type=jnp.float32
                )
                allowed = kpos[:, kspan] <= places
                scores = jnp.where(allowed, scores, neg_large)
                higher = jnp.maximum(top, jnp.max(scores, axis=1, keepdims=True))
                weights = jnp.exp(scores - higher)
                factor = jnp.exp(top - higher)
                total = total * factor + jnp.sum(weights, axis=1, keepdims=True)
                mix = mix * factor + jnp.dot(
                    weights.astype(jnp.bfloat16), kv, preferred_element_type=jnp.float32
                )
                return higher, total, mix

            state = (
                jnp.full((block, 1), sink[s * qheads + h], jnp.float32),
                jnp.ones((block, 1), jnp.float32),
                jnp.zeros((block, LANES), jnp.float32),
            )
            if chunks == 1:
                state = visit(0, state)
            else:
                state = lax.fori_loop(0, chunks, visit, state)
            outs.append((state[2] / state[1])[:, HEAD_SIZE:])
        att = outs[0] if qheads == 1 else jnp.concatenate(outs, axis=1)
        abuf[pl.ds(b * tiles, tiles)] = att.astype(jnp.bfloat16).reshape(tiles, rows, qc)

        def ship(i, _):
            to = b * tiles + i

            @pl.when(to != s)
            def _():
                send_out(to).start()

            return 0

        lax.fori_loop(0, tiles, ship, 0)
        return 0

    lax.fori_loop(0, group_rows // block, attention, 0)
    obuf[s] = abuf[s]

    def drain(j, _):
        @pl.when(j != s)
        def _():
            recv_out(j).wait_recv()
            send_out(j).wait_send()

        return 0

    lax.fori_loop(0, sp, drain, 0)
    for j in range(sp):
        out[:, j * qc : (j + 1) * qc] = obuf[j]
    send_tok(partner).wait_send()

    def finish(k, _):
        send_tok((c + k) % chips * 2 + par).wait_send()
        forward((c + chips - k) % chips * 2 + par).wait_send()
        return 0

    lax.fori_loop(1, chips, finish, 0)

    def finish_kv(chip, _):
        for d in range(1, grp):
            send_kv(chip, d).wait_send()
        return 0

    lax.fori_loop(0, chips, finish_kv, 0)


def per_device(tokens, query_weight, key_value_weight, block_places, sinks):
    sp = lax.axis_size("sp")
    grp = lax.axis_size("grp")
    rows, width = tokens.shape
    group_rows = rows * sp
    key_count = grp * group_rows
    qc = query_weight.shape[1]
    qheads = qc // HEAD_SIZE
    kv_total = key_value_weight.shape[1] // (2 * HEAD_SIZE)
    freq = jnp.arange(HEAD_SIZE // 2, dtype=jnp.float32)
    inverse = rope_base ** (-(freq * 2.0) / HEAD_SIZE)
    inverse = jnp.tile(inverse, LANES // (HEAD_SIZE // 2)).reshape(1, LANES)

    vmem = pl.BlockSpec(memory_space=pltpu.VMEM)
    hbm = pl.BlockSpec(memory_space=pl.ANY)
    smem = pl.BlockSpec(memory_space=pltpu.SMEM)
    dma = pltpu.SemaphoreType.DMA
    return pl.pallas_call(
        functools.partial(kernel, grp, sp, qheads, kv_total),
        out_shape=jax.ShapeDtypeStruct((rows, qc * sp), jnp.bfloat16),
        in_specs=[vmem, hbm, hbm, vmem, smem, smem],
        out_specs=vmem,
        scratch_shapes=[
            pltpu.VMEM((sp, rows, width), jnp.bfloat16),
            pltpu.VMEM((width, qc), jnp.bfloat16),
            pltpu.VMEM((width, 2 * LANES), jnp.bfloat16),
            pltpu.VMEM((key_count, LANES), jnp.bfloat16),
            pltpu.VMEM((qheads, group_rows, LANES), jnp.bfloat16),
            pltpu.VMEM((sp, rows, qc), jnp.bfloat16),
            pltpu.VMEM((sp, rows, qc), jnp.bfloat16),
            pltpu.VMEM((group_rows, LANES), jnp.float32),
            pltpu.VMEM((group_rows, LANES), jnp.float32),
            pltpu.VMEM((group_rows, 1), jnp.int32),
            pltpu.VMEM((1, key_count), jnp.int32),
            dma((3,)),
            dma((sp,)),
            dma((sp,)),
            dma((sp,)),
            dma((grp, sp // 2)),
            dma((grp, sp // 2)),
            dma((sp,)),
            dma((sp,)),
        ],
        compiler_params=pltpu.CompilerParams(
            has_side_effects=True, vmem_limit_bytes=60 * 1024 * 1024
        ),
    )(tokens, query_weight, key_value_weight, inverse, block_places, sinks)


def plane_kernel(
    grp, sp, qheads,
    tok_any, wq_any, kvw_any, places_any, sinks_any, out,
    places, sinks,    toks, wq, kvw, kvo, kvb, kaug, vt, qs, sbuf, pbuf, mbuf, abuf, obuf, cos_ref, sin_ref, kpos,
    wsem, tsend, trecv, drecv, ksend, krecv, zsend, zrecv, osend, orecv, ready,
):
    s = lax.axis_index("sp")
    g = lax.axis_index("grp")
    rows, width = toks.shape[1:]
    pieces = trecv.shape[1]
    piece_rows = rows // pieces
    half = pieces // 2
    pair = 2 * rows
    group_rows = rows * sp
    chips = sp // 2
    qc = qheads * HEAD_SIZE
    blocks = grp * BPG
    dim = HEAD_SIZE // 2
    p = s % 2
    c = s // 2
    cx = c + 1 - 2 * (c % 2)
    cy = (c + chips // 2) % chips
    cd = (cx + chips // 2) % chips
    xn, yn, dn, pn = cx * 2 + p, cy * 2 + p, cd * 2 + p, c * 2 + 1 - p
    key_base = g * group_rows

    chip_order = [c, cx, cy, cd]
    ways = [0, 2, 3, 1]
    wcopies = []
    for k, chip in enumerate(chip_order):
        koff = pl.multiple_of(chip * LANES, LANES)
        voff = pl.multiple_of(sp * HEAD_SIZE + chip * LANES, LANES)
        for part, off in enumerate((koff, voff)):
            wcopies.append(
                pltpu.make_async_copy(
                    kvw_any.at[:, pl.ds(off, LANES)],
                    kvw.at[k // 2, :, pl.ds((2 * (k % 2) + part) * LANES, LANES)],
                    wsem.at[2 + k // 2],
                )
            )
    tok_copy = pltpu.make_async_copy(tok_any, toks.at[s], wsem.at[0])
    wq_copy = pltpu.make_async_copy(wq_any, wq, wsem.at[1])
    pcopy = pltpu.make_async_copy(places_any, places, wsem.at[4])
    scopy = pltpu.make_async_copy(sinks_any, sinks, wsem.at[5])
    pcopy.start()
    scopy.start()
    tok_copy.start()
    for copy in wcopies:
        copy.start()
    wq_copy.start()

    barrier = pltpu.get_barrier_semaphore()
    upper = c >= chips // 2
    for to in (xn, yn, pn, cx * 2 + 1 - p, cy * 2 + 1 - p):
        pl.semaphore_signal(barrier, inc=1, device_id={"sp": to})

    @pl.when(jnp.logical_not(upper))
    def _():
        for core in range(2):
            pl.semaphore_signal(barrier, inc=1, device_id={"sp": cd * 2 + core})

    @pl.when(g < grp - 1)
    def _():
        pl.semaphore_signal(barrier, inc=1, device_id={"grp": g + 1})

    def send_piece(slot, q, to, sem):
        span = pl.ds(q * piece_rows, piece_rows)
        return pltpu.make_async_remote_copy(
            src_ref=toks.at[slot, span], dst_ref=toks.at[slot, span], send_sem=tsend.at[0],
            recv_sem=sem, device_id={"sp": to},
        )

    def send_own(slot, to):
        return pltpu.make_async_remote_copy(
            src_ref=toks.at[slot], dst_ref=toks.at[slot], send_sem=tsend.at[0],
            recv_sem=drecv.at[3], device_id={"sp": to},
        )

    def send_x(q):
        return send_piece(s, q, xn, trecv.at[0, q])

    def send_y(q):
        return send_piece(s, q, yn, trecv.at[1, q])

    def relay(q):
        if q >= half:
            return send_piece(xn, q, yn, trecv.at[2, q])
        return send_piece(yn, q, xn, trecv.at[2, q])

    def arrived(k, q):
        send_piece((xn, yn, dn)[k], q, pn, trecv.at[k, q]).wait_recv()

    def forward(k, q, i):
        return send_piece((xn, yn, dn)[k], q, pn, drecv.at[i])

    def wait_rows(sem, slots, count=rows):
        area = toks.at[pl.ds(0, slots), pl.ds(0, count)]
        pltpu.make_async_remote_copy(
            src_ref=area, dst_ref=area, send_sem=sem, recv_sem=sem, device_id={"sp": pn}
        ).wait_recv()

    def send_head(i, to, way):
        span = pl.ds(pl.multiple_of(key_base + s * rows, rows), rows)
        return pltpu.make_async_remote_copy(
            src_ref=kvo.at[i], dst_ref=kvb.at[span], send_sem=ksend.at[0],
            recv_sem=krecv.at[way], device_id={"sp": to},
        )

    def recv_heads(chip, way):
        span = pl.ds(pl.multiple_of(key_base + chip * pair, pair), rows if way == 0 else pair)
        pltpu.make_async_remote_copy(
            src_ref=kvb.at[span], dst_ref=kvb.at[span], send_sem=ksend.at[0],
            recv_sem=krecv.at[way], device_id={"sp": pn},
        ).wait_recv()

    def send_chunk(group, chip, to, way):
        span = pl.ds(pl.multiple_of(group * group_rows + chip * pair, pair), pair)
        return pltpu.make_async_remote_copy(
            src_ref=kvb.at[span], dst_ref=kvb.at[span], send_sem=zsend.at[way],
            recv_sem=zrecv.at[group, chip], device_id={"grp": to},
        )

    def share(chip):
        @pl.when(g > 0)
        def _():
            send_chunk(g, chip, g - 1, 1).start()

        @pl.when(g < grp - 1)
        def _():
            send_chunk(g, chip, g + 1, 0).start()

    inner = jnp.logical_and(g > 0, g < grp - 1)
    others = [jnp.abs(g - 1), 2 + g // 2 - 2 * (g // 3), 3 - 3 * (g // 2)]
    targets = [g + 1, g - 1, 3 * (g // 2)]

    def pass_on(k, chip):
        return send_chunk(others[k], chip, targets[k], 2)

    outer = jnp.logical_not(inner)

    def recv_group(k, chip_list):
        for chip in chip_list:
            send_chunk(others[k], chip, g, 0).wait_recv()

            @pl.when(inner)
            def _():
                pass_on(k, chip).start()

    pcopy.wait()
    scopy.wait()
    wide = lax.broadcasted_iota(jnp.int32, (1, LANES), 1)
    inverse = jnp.ones((1, LANES), jnp.float32)
    bit = 1
    while bit < dim:
        factor = rope_base ** (-2.0 * bit / HEAD_SIZE)
        inverse = jnp.where(wide // bit % 2 == 1, inverse * factor, inverse)
        bit *= 2
    sign = jnp.where(wide % HEAD_SIZE < dim, -1.0, 1.0)
    own_place = places[g * BPG + c] * pair + p * rows + lax.broadcasted_iota(jnp.int32, (rows, LANES), 0)
    own_angles = own_place.astype(jnp.float32) * inverse
    own_cos, own_sin = jnp.cos(own_angles), jnp.sin(own_angles) * sign
    tok_copy.wait()
    pl.semaphore_wait(barrier, 5 + jnp.minimum(g, 1) + 2 * (c // (chips // 2)))
    send_own(s, pn).start()
    send_x(half).start()
    send_y(0).start()

    @pl.when(g > 0)
    def _():
        pl.semaphore_signal(ready.at[0], inc=1, device_id={"grp": g - 1})

    @pl.when(upper)
    def _():
        for core in range(2):
            pl.semaphore_signal(ready.at[1], inc=1, device_id={"sp": cd * 2 + core})

    own_x = toks[s]
    low = lax.broadcasted_iota(jnp.int32, (rows, LANES), 1) < HEAD_SIZE
    for k in range(chips):
        if k % 2 == 0:
            pltpu.make_async_copy(
                kvw_any.at[:, pl.ds(0, 4 * LANES)], kvw.at[k // 2], wsem.at[2 + k // 2]
            ).wait()
            both = jnp.dot(own_x, kvw[k // 2], preferred_element_type=jnp.float32)
        kv = both[:, k % 2 * 2 * LANES : (k % 2 + 1) * 2 * LANES]
        keys = rotate_heads(kv[:, :LANES], own_cos, own_sin)
        values = kv[:, LANES:]
        first = jnp.where(low, keys, pltpu.roll(values, HEAD_SIZE, 1)).astype(jnp.bfloat16)
        second = jnp.where(low, pltpu.roll(keys, HEAD_SIZE, 1), values).astype(jnp.bfloat16)
        way = ways[k]
        if way == 0:
            mine = p == 0
            kvb[pl.ds(pl.multiple_of(key_base + s * rows, rows), rows), :] = jnp.where(mine, first, second)
            kvo[0] = jnp.where(mine, second, first)
            send_head(0, pn, 0).start()
        else:
            chip = chip_order[k]
            kvo[2 * way - 1] = first
            kvo[2 * way] = second
            if way == 1:
                pl.when(jnp.logical_not(upper))(lambda: pl.semaphore_wait(ready.at[1], 2))
            send_head(2 * way - 1, chip * 2, way).start()
            send_head(2 * way, chip * 2 + 1, way).start()

    for q in range(1, half):
        send_x(half + q).start()
        send_y(q).start()
    for q in range(half):
        send_x(q).start()
        send_y(half + q).start()

    recv_heads(c, 0)
    pl.when(g < grp - 1)(lambda: pl.semaphore_wait(ready.at[0], 1))
    share(c)
    for j in range(BPG):
        rspan = slice(j * pair, (j + 1) * pair)
        within = lax.broadcasted_iota(jnp.int32, (pair, LANES), 0)
        place = places[g * BPG + j] * pair + within
        kpos[rspan, :] = place
        angles = place.astype(jnp.float32) * inverse
        cos_ref[rspan, :] = jnp.cos(angles)
        sin_ref[rspan, :] = jnp.sin(angles) * sign
    block_place = jnp.full((1, LANES), -1, jnp.int32)
    for e in range(blocks):
        block_place = jnp.where(wide == HEAD_SIZE + e, places[e], block_place)

    quarter = rows // 2
    units = [
        [[(c, 0, 0), (c, 0, quarter), (c, 1, 0), (c, 1, quarter)]],
        [[(cx, 0, quarter), (cx, 1, quarter), (cy, 0, 0), (cy, 1, 0)]],
        [[(cx, 0, 0), (cx, 1, 0), (cy, 0, quarter), (cy, 1, quarter)]],
        [[(cd, 0, 0), (cd, 0, quarter), (cd, 1, 0), (cd, 1, quarter)]],
    ]

    def seg_size(u):
        return quarter // len(units[u])

    def seg_rows(ref, seg, count):
        chip, core, off = seg
        return ref[pl.ds(pl.multiple_of(chip * pair + core * rows + off, count), count), :]

    def run(*tasks):
        tasks = list(tasks)
        while tasks:
            for task in list(tasks):
                try:
                    next(task)
                except StopIteration:
                    tasks.remove(task)

    def project(u, part):
        segs, count = units[u][part], seg_size(u)
        size = 4 * count
        x = jnp.concatenate([toks[chip * 2 + core, off : off + count] for chip, core, off in segs], axis=0)
        cosine = jnp.concatenate([seg_rows(cos_ref, seg, count) for seg in segs], axis=0)
        sine = jnp.concatenate([seg_rows(sin_ref, seg, count) for seg in segs], axis=0)
        qf = jnp.dot(x, wq[...], preferred_element_type=jnp.float32)
        yield
        qr = rotate_heads(qf, cosine, sine) * HEAD_SIZE**-0.5
        hidden = jnp.concatenate([
            jnp.broadcast_to(
                jnp.where(block_place > places[g * BPG + chip], neg_large, 0.0), (count, LANES)
            )
            for chip, _, _ in segs
        ], axis=0)
        lower = lax.broadcasted_iota(jnp.int32, (size, LANES), 1) < HEAD_SIZE
        for h in range(qheads):
            v = qr[:, h // 2 * LANES : (h // 2 + 1) * LANES]
            if h % 2:
                v = pltpu.roll(v, HEAD_SIZE, 1)
            base = (part * qheads + h) * size
            qs[u, base : base + size, :] = jnp.where(lower, v, hidden).astype(jnp.bfloat16)
            yield

    def query_places(u, part):
        count = seg_size(u)
        size = 4 * count
        row = lax.broadcasted_iota(jnp.int32, (1, qheads * size), 1) % size
        place = jnp.zeros(row.shape, jnp.int32)
        for i, (chip, core, off) in enumerate(units[u][part]):
            base = places[g * BPG + chip] * pair + core * rows + off
            place = jnp.where(row // count == i, base + row % count, place)
        return place

    def sink_row(u):
        size = 4 * seg_size(u)
        head = lax.broadcasted_iota(jnp.int32, (1, qheads * size), 1) // size
        row = jnp.full(head.shape, sinks[s * qheads], jnp.float32)
        for h in range(1, qheads):
            row = jnp.where(head == h, sinks[s * qheads + h], row)
        return row

    def prepare(k):
        group = g if k == 0 else others[k - 1]
        lane = lax.broadcasted_iota(jnp.int32, (pair, LANES), 1)
        for j in range(chips):
            kv = kvb[pl.ds(pl.multiple_of(group * group_rows + j * pair, pair), pair), :]
            mark = jnp.where(lane == HEAD_SIZE + group * BPG + j, 1.0, 0.0).astype(jnp.bfloat16)
            span = slice(k * group_rows + j * pair, k * group_rows + (j + 1) * pair)
            kaug[span, :] = jnp.where(lane < HEAD_SIZE, kv, mark)
            vt[:, span] = jnp.transpose(kv)[HEAD_SIZE:]

    tops = [[sink_row(u) for _ in units[u]] for u in range(len(units))]

    def joined(rows_of):
        return rows_of[0] if len(rows_of) == 1 else jnp.concatenate(rows_of, axis=1)

    floors = [joined(tops[u]) for u in range(len(units))]

    def part_scores(u, k, part):
        width_of = qheads * 4 * seg_size(u)
        side = slice(part * width_of, (part + 1) * width_of)
        span = slice(k * group_rows, (k + 1) * group_rows)
        whole = lax.dot_general(
            kaug[span, :], qs[u, side, :], (((1,), (1,)), ((), ())), preferred_element_type=jnp.float32
        )
        yield
        for j in range(0, group_rows, pair):
            piece = whole[j : j + pair, :]
            if k == 0:
                seen = jnp.concatenate([kpos[j : j + pair, :]] * (width_of // LANES), axis=1)
                piece = jnp.where(seen <= query_places(u, part), piece, neg_large)
            sbuf[u, k * group_rows + j : k * group_rows + j + pair, side] = piece
            tops[u][part] = jnp.maximum(tops[u][part], jnp.max(piece, axis=0, keepdims=True))
            yield

    def score(u, k):
        for part in range(len(units[u])):
            yield from part_scores(u, k, part)

    bases = [None for _ in units]
    totals = [None for _ in units]

    def absorb(u, stored, fresh, final=False):
        low_key = min(stored + fresh) * group_rows
        high_key = (max(stored + fresh) + 1) * group_rows
        for k in fresh:
            yield from score(u, k)
        top = joined(tops[u])
        factor = None
        if bases[u] is None:
            total = jnp.exp(floors[u] - top)
        else:
            factor = jnp.exp(bases[u] - top)
            total = totals[u] * factor
        for j in range(low_key, high_key, 2 * pair):
            weights = jnp.exp(sbuf[u, j : j + 2 * pair, :] - top)
            pbuf[u, j : j + 2 * pair, :] = weights.astype(jnp.bfloat16)
            total = total + jnp.sum(weights, axis=0, keepdims=True)
            yield
        totals[u], bases[u] = total, top
        mix = jnp.dot(
            vt[:, low_key:high_key], pbuf[u, low_key:high_key, :], preferred_element_type=jnp.float32
        )
        yield
        if factor is not None:
            mix = mix + mbuf[u] * factor
        if not final:
            mbuf[u] = mix
            return
        mix = mix / total
        count = seg_size(u)
        size = 4 * count
        for part in range(len(units[u])):
            tiles = []
            for h in range(0, qheads, LANES // size):
                base = (part * qheads + h) * size
                tile = jnp.transpose(mix[:, base : base + LANES])
                tiles.extend(tile[i : i + size] for i in range(0, LANES, size))
            att = jnp.concatenate(tiles, axis=1).astype(jnp.bfloat16)
            if len(units[u]) == 1:
                abuf[u] = att
                continue
            for i, (_, core, off) in enumerate(units[u][part]):
                abuf[u, core * rows + off : core * rows + off + count, :] = att[i * count : (i + 1) * count]

    def chain(*tasks):
        for task in tasks:
            yield from task

    def send_out(u, i):
        chip, core, off = (cd, i // 2, 0) if u == 3 else units[u][0][i]
        count = rows if u in (0, 3) else quarter
        src = abuf.at[u, pl.ds(i * quarter, count)]
        dst = obuf.at[pl.ds(off, count), pl.ds(pl.multiple_of(s * qc, qc), qc)]
        return pltpu.make_async_remote_copy(
            src_ref=src, dst_ref=dst, send_sem=osend.at[0],
            recv_sem=orecv.at[0], device_id={"sp": chip * 2 + core},
        )

    def send_out_partner():
        src = abuf.at[0, pl.ds(pl.multiple_of((1 - p) * rows, rows), rows)]
        dst = obuf.at[:, pl.ds(pl.multiple_of(s * qc, qc), qc)]
        return pltpu.make_async_remote_copy(
            src_ref=src, dst_ref=dst, send_sem=osend.at[0],
            recv_sem=orecv.at[0], device_id={"sp": pn},
        )

    def wait_out(sem):
        span = pl.ds(0, (sp - 1) * qc)
        pltpu.make_async_remote_copy(
            src_ref=obuf.at[:, span], dst_ref=obuf.at[:, span], send_sem=sem, recv_sem=sem,
            device_id={"sp": pn},
        ).wait_recv()

    def ship(u):
        if u == 0:
            send_out_partner().start()
            obuf[:, pl.ds(pl.multiple_of(s * qc, qc), qc)] = abuf[
                0, pl.ds(pl.multiple_of(p * rows, rows), rows), :
            ]
        elif u == 3:
            send_out(u, 0).start()
            send_out(u, 2).start()
        else:
            for i in range(4):
                send_out(u, i).start()

    def stage(k):
        qx, qy = (k + half) % pieces, k
        arrived(0, qx)
        if k < half:
            relay(qx).start()
        forward(0, qx, k // half).start()
        arrived(1, qy)
        if k < half:
            relay(qy).start()
        forward(1, qy, k // half).start()

    def stage_far(q):
        for r in (q, q + half):
            arrived(2, r)
            forward(2, r, 2).start()

    def partner(i):
        wait_rows(drecv.at[i], 1)

    stage(0)
    partner(3)
    wq_copy.wait()
    run(project(0, 0))
    for chip, way in ((cx, 2), (cy, 3), (cd, 1)):
        recv_heads(chip, way)
        share(chip)
    near, rest = (c,), (cx, cy, cd)
    pl.when(inner)(lambda: recv_group(0, near))
    prepare(0)
    run(score(0, 0))
    pl.when(inner)(lambda: recv_group(1, near))
    stage(1)
    partner(0)
    run(project(1, 0))
    run(score(1, 0))
    pl.when(outer)(lambda: recv_group(0, near))
    recv_group(0, rest)

    @pl.when(inner)
    def _():
        recv_group(1, rest)
        recv_group(2, near)

    stage(2)
    prepare(1)
    run(score(0, 1), score(1, 1))
    stage(3)
    partner(1)
    run(chain(project(2, 0), score(2, 0)), absorb(1, [0, 1], []))
    pl.when(inner)(lambda: recv_group(2, (cx,)))
    run(score(2, 1))
    pl.when(outer)(lambda: recv_group(1, near + rest))
    pl.when(inner)(lambda: recv_group(2, (cy, cd)))
    stage_far(0)
    pl.when(p == 1)(lambda: stage_far(1))
    prepare(2)
    run(absorb(1, [], [2]), score(0, 2), score(2, 2))
    pl.when(p == 0)(lambda: stage_far(1))
    run(absorb(2, [0, 1, 2], []))
    partner(2)
    run(chain(project(3, 0), score(3, 0), score(3, 1), score(3, 2), absorb(3, [0, 1, 2], [])))
    pl.when(outer)(lambda: recv_group(2, near + rest))
    prepare(3)
    run(absorb(3, [], [3], True))
    ship(3)
    run(absorb(1, [], [3], True), absorb(2, [], [3], True))
    ship(1)
    ship(2)
    run(absorb(0, [0, 1, 2], [3], True))
    ship(0)

    wait_out(orecv.at[0])
    out[...] = obuf[...]
    wait_rows(tsend.at[0], sp - 1)
    kept = kvo.at[pl.ds(0, sp - 1)]
    pltpu.make_async_remote_copy(
        src_ref=kept, dst_ref=kept, send_sem=ksend.at[0], recv_sem=ksend.at[0], device_id={"sp": pn}
    ).wait_recv()

    def wait_keys(way, count):
        span = pl.ds(0, count)
        pltpu.make_async_remote_copy(
            src_ref=kvb.at[span], dst_ref=kvb.at[span], send_sem=zsend.at[way],
            recv_sem=zsend.at[way], device_id={"grp": g},
        ).wait_recv()

    pl.when(g > 0)(lambda: wait_keys(1, group_rows))
    pl.when(g < grp - 1)(lambda: wait_keys(0, group_rows))
    pl.when(inner)(lambda: wait_keys(2, 3 * group_rows))
    wait_out(osend.at[0])


def per_plane(tokens, query_weight, key_value_weight, block_places, sinks):
    sp = lax.axis_size("sp")
    grp = lax.axis_size("grp")
    rows, width = tokens.shape
    group_rows = rows * sp
    key_count = grp * group_rows
    qc = query_weight.shape[1]
    qheads = qc // HEAD_SIZE
    pair = 2 * rows
    columns = qheads * pair
    pieces = 4
    hbm = pl.BlockSpec(memory_space=pl.ANY)
    dma = pltpu.SemaphoreType.DMA
    bf16, f32 = jnp.bfloat16, jnp.float32
    result = pl.pallas_call(
        functools.partial(plane_kernel, grp, sp, qheads),
        out_shape=pltpu.VMEM((rows, qc * sp), bf16),
        in_specs=[hbm] * 5,
        out_specs=pl.BlockSpec(memory_space=pltpu.VMEM),
        scratch_shapes=[
            pltpu.SMEM(block_places.shape, block_places.dtype),
            pltpu.SMEM(sinks.shape, sinks.dtype),
            pltpu.VMEM((sp, rows, width), bf16),
            pltpu.VMEM((width, qc), bf16),
            pltpu.VMEM((2, width, 4 * LANES), bf16),
            pltpu.VMEM((sp, rows, LANES), bf16),
            pltpu.VMEM((key_count, LANES), bf16),
            pltpu.VMEM((key_count, LANES), bf16),
            pltpu.VMEM((HEAD_SIZE, key_count), bf16),
            pltpu.VMEM((sp // 2, columns, LANES), bf16),
            pltpu.VMEM((sp // 2, key_count, columns), f32),
            pltpu.VMEM((sp // 2, key_count, columns), bf16),
            pltpu.VMEM((sp // 2, HEAD_SIZE, columns), f32),
            pltpu.VMEM((sp // 2, pair, qc), bf16),
            pltpu.VMEM((rows, qc * sp), bf16),
            pltpu.VMEM((group_rows, LANES), f32),
            pltpu.VMEM((group_rows, LANES), f32),
            pltpu.VMEM((group_rows, LANES), jnp.int32),
            dma((6,)),
            dma((1,)),
            dma((3, pieces)),
            dma((5,)),
            dma((1,)),
            dma((sp // 2,)),
            dma((3,)),
            dma((grp, sp // 2)),
            dma((1,)),
            dma((1,)),
            pltpu.SemaphoreType.REGULAR((2,)),
        ],
        compiler_params=pltpu.CompilerParams(
            has_side_effects=True, collective_id=0, vmem_limit_bytes=60 * 1024 * 1024
        ),
    )(tokens, query_weight, key_value_weight, block_places, sinks)
    return result


def write_out(result, out, sem):
    copy = pltpu.make_async_copy(result, out, sem)
    copy.start()
    copy.wait()


def written(result):
    return pl.pallas_call(
        write_out,
        out_shape=jax.ShapeDtypeStruct(result.shape, result.dtype),
        in_specs=[pl.BlockSpec(memory_space=pltpu.VMEM)],
        out_specs=pl.BlockSpec(memory_space=pl.ANY),
        scratch_shapes=[pltpu.SemaphoreType.DMA],
    )(result)


def local_form(tokens, query_weight, key_value_weight, block_places, sinks):
    sp = lax.axis_size("sp")
    grp = lax.axis_size("grp")
    heads = query_weight.shape[1] // HEAD_SIZE
    kv_total = key_value_weight.shape[1] // (2 * HEAD_SIZE)
    square = sp // 2 == BPG and grp == BPG and kv_total == sp and block_places.shape[0] == grp * BPG
    form = per_plane if square and heads * HEAD_SIZE == 2 * LANES else per_device
    return form(tokens, query_weight, key_value_weight, block_places, sinks)


def solution(mesh):
    in_specs = (P(("grp", "sp"), None), P(None, "sp"), P(), P(), P())
    out_specs = P(("grp", "sp"), None)
    return jax.shard_map(
        local_form, mesh=mesh, in_specs=in_specs, out_specs=out_specs, check_vma=False
    )
```

```python
import functools

import jax
import jax.numpy as jnp
from jax import lax
from jax.experimental import pallas as pl
from jax.experimental.pallas import tpu as pltpu
from jax.sharding import PartitionSpec as P

QUERY_HEADS = 32
HEAD_SIZE = 64
BPG = 4
LANES = 128

rope_base = 150000.0
neg_large = -1e30


def rotate_heads(x, cosine, sine):
    width = x.shape[1]
    half = HEAD_SIZE // 2
    if width % LANES:
        swapped = jnp.concatenate([x[:, half:], x[:, :half]], axis=1)
        return x * cosine[:, :width] + swapped * sine[:, :width]
    parts = []
    lane = lax.broadcasted_iota(jnp.int32, (x.shape[0], LANES), 1)
    first = lane % HEAD_SIZE < half
    for j in range(width // LANES):
        v = x[:, j * LANES : (j + 1) * LANES]
        swapped = jnp.where(first, pltpu.roll(v, LANES - half, 1), pltpu.roll(v, half, 1))
        parts.append(v * cosine + swapped * sine)
    return parts[0] if len(parts) == 1 else jnp.concatenate(parts, axis=1)


def kernel(
    grp, sp, qheads, kv_total,
    tok, wq_any, kvw_any, inverse_ref, places_ref, sink, out,
    toks, wq, wkv, kvb, q, abuf, obuf, cos_ref, sin_ref, qpos, kpos,
    wsem, tsend, tfwd, trecv, ksend, krecv, osend, orecv,
):
    s = lax.axis_index("sp")
    g = lax.axis_index("grp")
    rows = tok.shape[0]
    group_rows = rows * sp
    chips = sp // 2
    pair = 2 * rows
    qc = qheads * HEAD_SIZE
    c = s // 2
    par = s % 2
    partner = s + 1 - 2 * par
    head = s * kv_total // sp
    hpar = head % 2
    koff = pl.multiple_of(head // 2 * LANES, LANES)
    voff = pl.multiple_of(kv_total * HEAD_SIZE + head // 2 * LANES, LANES)

    wcopies = [
        pltpu.make_async_copy(wq_any, wq, wsem.at[0]),
        pltpu.make_async_copy(
            kvw_any.at[:, pl.ds(koff, LANES)], wkv.at[:, pl.ds(0, LANES)], wsem.at[1]
        ),
        pltpu.make_async_copy(
            kvw_any.at[:, pl.ds(voff, LANES)], wkv.at[:, pl.ds(LANES, LANES)], wsem.at[2]
        ),
    ]

    def send_tok(to):
        return pltpu.make_async_remote_copy(
            src_ref=tok, dst_ref=toks.at[s], send_sem=tsend.at[to], recv_sem=trecv.at[s],
            device_id={"sp": to},
        )

    def forward(slot):
        return pltpu.make_async_remote_copy(
            src_ref=toks.at[slot], dst_ref=toks.at[slot], send_sem=tfwd.at[slot],
            recv_sem=trecv.at[slot], device_id={"sp": partner},
        )

    def send_kv(chip, d):
        span = pl.ds(pl.multiple_of(g * group_rows + chip * pair, pair), pair)
        return pltpu.make_async_remote_copy(
            src_ref=kvb.at[span], dst_ref=kvb.at[span], send_sem=ksend.at[d, chip],
            recv_sem=krecv.at[g, chip], device_id={"grp": (g + d) % grp},
        )

    def recv_kv(chip, d):
        src = (g + d) % grp
        span = pl.ds(pl.multiple_of(src * group_rows + chip * pair, pair), pair)
        return pltpu.make_async_remote_copy(
            src_ref=kvb.at[span], dst_ref=kvb.at[span], send_sem=ksend.at[d, chip],
            recv_sem=krecv.at[src, chip], device_id={"grp": src},
        )

    def send_out(to):
        return pltpu.make_async_remote_copy(
            src_ref=abuf.at[to], dst_ref=obuf.at[s], send_sem=osend.at[to],
            recv_sem=orecv.at[s], device_id={"sp": to},
        )

    def recv_out(src):
        return pltpu.make_async_remote_copy(
            src_ref=abuf.at[src], dst_ref=obuf.at[src], send_sem=osend.at[src],
            recv_sem=orecv.at[src], device_id={"sp": src},
        )

    send_tok(partner).start()

    def start_tok(k, _):
        send_tok((c + k) % chips * 2 + par).start()
        return 0

    lax.fori_loop(1, chips, start_tok, 0)
    for copy in wcopies:
        copy.start()
    toks[s] = tok[...]

    block_rows = group_rows // BPG
    for j in range(kpos.shape[1] // block_rows):
        within = lax.broadcasted_iota(jnp.int32, (1, block_rows), 1)
        kpos[:, j * block_rows : (j + 1) * block_rows] = places_ref[j] * block_rows + within
    wide = lax.broadcasted_iota(jnp.int32, (1, LANES), 1)
    half = HEAD_SIZE // 2
    inverse = inverse_ref[...]
    sign = jnp.where(wide % HEAD_SIZE < half, -1.0, 1.0)
    for j in range(BPG):
        rspan = slice(j * block_rows, (j + 1) * block_rows)
        within = lax.broadcasted_iota(jnp.int32, (block_rows, LANES), 0)
        place = places_ref[g * BPG + j] * block_rows + within
        qpos[rspan, :] = place[:, :1]
        angles = place.astype(jnp.float32) * inverse
        cos_ref[rspan, :] = jnp.cos(angles)
        sin_ref[rspan, :] = jnp.sin(angles) * sign
    for copy in wcopies:
        copy.wait()

    def project(k, _):
        chip = (c + chips - k) % chips

        @pl.when(k > 0)
        def _():
            slot = chip * 2 + par
            forward(slot).wait_recv()
            forward(slot).start()

        forward(chip * 2 + 1 - par).wait_recv()
        x = toks[pl.ds(chip * 2, 2)].reshape(pair, tok.shape[1])
        span = pl.ds(pl.multiple_of(chip * pair, pair), pair)
        cosine = cos_ref[span, :]
        sine = sin_ref[span, :]
        kv = jnp.dot(x, wkv[...], preferred_element_type=jnp.float32)
        keys = rotate_heads(kv[:, :LANES], cosine, sine)
        values = kv[:, LANES:]
        low = hpar == 0
        keys = jnp.where(low, keys, pltpu.roll(keys, HEAD_SIZE, 1))
        values = jnp.where(low, pltpu.roll(values, HEAD_SIZE, 1), values)
        lane = lax.broadcasted_iota(jnp.int32, (pair, LANES), 1)
        joined = jnp.where(lane < HEAD_SIZE, keys, values).astype(jnp.bfloat16)
        kvb[pl.ds(pl.multiple_of(g * group_rows + chip * pair, pair), pair), :] = joined
        for d in range(1, grp):
            send_kv(chip, d).start()
        qf = jnp.dot(x, wq[...], preferred_element_type=jnp.float32)
        qr = (rotate_heads(qf, cosine, sine) * HEAD_SIZE**-0.5).astype(jnp.bfloat16)
        zeros = jnp.zeros((pair, HEAD_SIZE), jnp.bfloat16)
        for h in range(qheads):
            q[h, span, :] = jnp.concatenate(
                [qr[:, h * HEAD_SIZE : (h + 1) * HEAD_SIZE], zeros], axis=1
            )
        return 0

    lax.fori_loop(0, chips, project, 0)

    def arrive(chip, _):
        for d in range(1, grp):
            recv_kv(chip, d).wait_recv()
        return 0

    lax.fori_loop(0, chips, arrive, 0)

    key_count = kvb.shape[0]
    chunk = min(key_count, 2048)
    chunks = key_count // chunk
    block = min(256, group_rows)
    tiles = block // rows

    def attention(b, _):
        span = pl.ds(pl.multiple_of(b * block, block), block)
        places = qpos[span, :]
        outs = []
        for h in range(qheads):
            qh = q[h, span, :]

            def visit(t, state):
                top, total, mix = state
                kspan = pl.ds(pl.multiple_of(t * chunk, chunk), chunk)
                kv = kvb[kspan, :]
                scores = lax.dot_general(
                    qh, kv, (((1,), (1,)), ((), ())), preferred_element_type=jnp.float32
                )
                allowed = kpos[:, kspan] <= places
                scores = jnp.where(allowed, scores, neg_large)
                higher = jnp.maximum(top, jnp.max(scores, axis=1, keepdims=True))
                weights = jnp.exp(scores - higher)
                factor = jnp.exp(top - higher)
                total = total * factor + jnp.sum(weights, axis=1, keepdims=True)
                mix = mix * factor + jnp.dot(
                    weights.astype(jnp.bfloat16), kv, preferred_element_type=jnp.float32
                )
                return higher, total, mix

            state = (
                jnp.full((block, 1), sink[s * qheads + h], jnp.float32),
                jnp.ones((block, 1), jnp.float32),
                jnp.zeros((block, LANES), jnp.float32),
            )
            if chunks == 1:
                state = visit(0, state)
            else:
                state = lax.fori_loop(0, chunks, visit, state)
            outs.append((state[2] / state[1])[:, HEAD_SIZE:])
        att = outs[0] if qheads == 1 else jnp.concatenate(outs, axis=1)
        abuf[pl.ds(b * tiles, tiles)] = att.astype(jnp.bfloat16).reshape(tiles, rows, qc)

        def ship(i, _):
            to = b * tiles + i

            @pl.when(to != s)
            def _():
                send_out(to).start()

            return 0

        lax.fori_loop(0, tiles, ship, 0)
        return 0

    lax.fori_loop(0, group_rows // block, attention, 0)
    obuf[s] = abuf[s]

    def drain(j, _):
        @pl.when(j != s)
        def _():
            recv_out(j).wait_recv()
            send_out(j).wait_send()

        return 0

    lax.fori_loop(0, sp, drain, 0)
    for j in range(sp):
        out[:, j * qc : (j + 1) * qc] = obuf[j]
    send_tok(partner).wait_send()

    def finish(k, _):
        send_tok((c + k) % chips * 2 + par).wait_send()
        forward((c + chips - k) % chips * 2 + par).wait_send()
        return 0

    lax.fori_loop(1, chips, finish, 0)

    def finish_kv(chip, _):
        for d in range(1, grp):
            send_kv(chip, d).wait_send()
        return 0

    lax.fori_loop(0, chips, finish_kv, 0)


def per_device(tokens, query_weight, key_value_weight, block_places, sinks):
    sp = lax.axis_size("sp")
    grp = lax.axis_size("grp")
    rows, width = tokens.shape
    group_rows = rows * sp
    key_count = grp * group_rows
    qc = query_weight.shape[1]
    qheads = qc // HEAD_SIZE
    kv_total = key_value_weight.shape[1] // (2 * HEAD_SIZE)
    freq = jnp.arange(HEAD_SIZE // 2, dtype=jnp.float32)
    inverse = rope_base ** (-(freq * 2.0) / HEAD_SIZE)
    inverse = jnp.tile(inverse, LANES // (HEAD_SIZE // 2)).reshape(1, LANES)

    vmem = pl.BlockSpec(memory_space=pltpu.VMEM)
    hbm = pl.BlockSpec(memory_space=pl.ANY)
    smem = pl.BlockSpec(memory_space=pltpu.SMEM)
    dma = pltpu.SemaphoreType.DMA
    return pl.pallas_call(
        functools.partial(kernel, grp, sp, qheads, kv_total),
        out_shape=jax.ShapeDtypeStruct((rows, qc * sp), jnp.bfloat16),
        in_specs=[vmem, hbm, hbm, vmem, smem, smem],
        out_specs=vmem,
        scratch_shapes=[
            pltpu.VMEM((sp, rows, width), jnp.bfloat16),
            pltpu.VMEM((width, qc), jnp.bfloat16),
            pltpu.VMEM((width, 2 * LANES), jnp.bfloat16),
            pltpu.VMEM((key_count, LANES), jnp.bfloat16),
            pltpu.VMEM((qheads, group_rows, LANES), jnp.bfloat16),
            pltpu.VMEM((sp, rows, qc), jnp.bfloat16),
            pltpu.VMEM((sp, rows, qc), jnp.bfloat16),
            pltpu.VMEM((group_rows, LANES), jnp.float32),
            pltpu.VMEM((group_rows, LANES), jnp.float32),
            pltpu.VMEM((group_rows, 1), jnp.int32),
            pltpu.VMEM((1, key_count), jnp.int32),
            dma((3,)),
            dma((sp,)),
            dma((sp,)),
            dma((sp,)),
            dma((grp, sp // 2)),
            dma((grp, sp // 2)),
            dma((sp,)),
            dma((sp,)),
        ],
        compiler_params=pltpu.CompilerParams(
            has_side_effects=True, vmem_limit_bytes=60 * 1024 * 1024
        ),
    )(tokens, query_weight, key_value_weight, inverse, block_places, sinks)


def plane_kernel(
    grp, sp, qheads,
    tok_any, wq_any, kvw_any, places_any, sinks_any, out,
    places, sinks,    toks, wq, kvw, kvo, kvb, kaug, vt, qs, sbuf, pbuf, mbuf, abuf, obuf, cos_ref, sin_ref, kpos,
    wsem, tsend, trecv, drecv, ksend, krecv, zsend, zrecv, osend, orecv, ready,
):
    s = lax.axis_index("sp")
    g = lax.axis_index("grp")
    rows, width = toks.shape[1:]
    pieces = trecv.shape[1]
    piece_rows = rows // pieces
    half = pieces // 2
    pair = 2 * rows
    group_rows = rows * sp
    chips = sp // 2
    qc = qheads * HEAD_SIZE
    blocks = grp * BPG
    dim = HEAD_SIZE // 2
    p = s % 2
    c = s // 2
    cx = c + 1 - 2 * (c % 2)
    cy = (c + chips // 2) % chips
    cd = (cx + chips // 2) % chips
    xn, yn, dn, pn = cx * 2 + p, cy * 2 + p, cd * 2 + p, c * 2 + 1 - p
    key_base = g * group_rows

    chip_order = [c, cx, cy, cd]
    ways = [0, 2, 3, 1]
    wcopies = []
    for k, chip in enumerate(chip_order):
        koff = pl.multiple_of(chip * LANES, LANES)
        voff = pl.multiple_of(sp * HEAD_SIZE + chip * LANES, LANES)
        for part, off in enumerate((koff, voff)):
            wcopies.append(
                pltpu.make_async_copy(
                    kvw_any.at[:, pl.ds(off, LANES)],
                    kvw.at[k // 2, :, pl.ds((2 * (k % 2) + part) * LANES, LANES)],
                    wsem.at[2 + k // 2],
                )
            )
    def load_piece(q, sem):
        span = pl.ds(q * piece_rows, piece_rows)
        return pltpu.make_async_copy(tok_any.at[span], toks.at[s, span], wsem.at[sem])

    def wait_pieces(sem, count):
        span = pl.ds(0, count * piece_rows)
        pltpu.make_async_copy(tok_any.at[span], toks.at[s, span], wsem.at[sem]).wait()

    first_pieces = (half, 0)
    other_pieces = [q for q in range(pieces) if q not in first_pieces]
    wq_copy = pltpu.make_async_copy(wq_any, wq, wsem.at[1])
    pcopy = pltpu.make_async_copy(places_any, places, wsem.at[4])
    scopy = pltpu.make_async_copy(sinks_any, sinks, wsem.at[5])
    pcopy.start()
    scopy.start()
    for q in first_pieces:
        load_piece(q, 0).start()
    for q in other_pieces:
        load_piece(q, 6).start()
    for copy in wcopies:
        copy.start()
    wq_copy.start()

    barrier = pltpu.get_barrier_semaphore()
    upper = c >= chips // 2
    for to in (xn, yn, pn, cx * 2 + 1 - p, cy * 2 + 1 - p):
        pl.semaphore_signal(barrier, inc=1, device_id={"sp": to})

    @pl.when(jnp.logical_not(upper))
    def _():
        for core in range(2):
            pl.semaphore_signal(barrier, inc=1, device_id={"sp": cd * 2 + core})

    @pl.when(g < grp - 1)
    def _():
        pl.semaphore_signal(barrier, inc=1, device_id={"grp": g + 1})

    def send_piece(slot, q, to, sem):
        span = pl.ds(q * piece_rows, piece_rows)
        return pltpu.make_async_remote_copy(
            src_ref=toks.at[slot, span], dst_ref=toks.at[slot, span], send_sem=tsend.at[0],
            recv_sem=sem, device_id={"sp": to},
        )

    def send_own(slot, to):
        return pltpu.make_async_remote_copy(
            src_ref=toks.at[slot], dst_ref=toks.at[slot], send_sem=tsend.at[0],
            recv_sem=drecv.at[3], device_id={"sp": to},
        )

    def send_x(q):
        return send_piece(s, q, xn, trecv.at[0, q])

    def send_y(q):
        return send_piece(s, q, yn, trecv.at[1, q])

    def relay(q):
        if q >= half:
            return send_piece(xn, q, yn, trecv.at[2, q])
        return send_piece(yn, q, xn, trecv.at[2, q])

    def arrived(k, q):
        send_piece((xn, yn, dn)[k], q, pn, trecv.at[k, q]).wait_recv()

    def forward(k, q, i):
        return send_piece((xn, yn, dn)[k], q, pn, drecv.at[i])

    def wait_rows(sem, slots, count=rows):
        area = toks.at[pl.ds(0, slots), pl.ds(0, count)]
        pltpu.make_async_remote_copy(
            src_ref=area, dst_ref=area, send_sem=sem, recv_sem=sem, device_id={"sp": pn}
        ).wait_recv()

    def send_head(i, to, way):
        span = pl.ds(pl.multiple_of(key_base + s * rows, rows), rows)
        return pltpu.make_async_remote_copy(
            src_ref=kvo.at[i], dst_ref=kvb.at[span], send_sem=ksend.at[0],
            recv_sem=krecv.at[way], device_id={"sp": to},
        )

    def recv_heads(chip, way):
        span = pl.ds(pl.multiple_of(key_base + chip * pair, pair), rows if way == 0 else pair)
        pltpu.make_async_remote_copy(
            src_ref=kvb.at[span], dst_ref=kvb.at[span], send_sem=ksend.at[0],
            recv_sem=krecv.at[way], device_id={"sp": pn},
        ).wait_recv()

    def send_chunk(group, chip, to, way):
        span = pl.ds(pl.multiple_of(group * group_rows + chip * pair, pair), pair)
        return pltpu.make_async_remote_copy(
            src_ref=kvb.at[span], dst_ref=kvb.at[span], send_sem=zsend.at[way],
            recv_sem=zrecv.at[group, chip], device_id={"grp": to},
        )

    def share(chip):
        @pl.when(g > 0)
        def _():
            send_chunk(g, chip, g - 1, 1).start()

        @pl.when(g < grp - 1)
        def _():
            send_chunk(g, chip, g + 1, 0).start()

    inner = jnp.logical_and(g > 0, g < grp - 1)
    others = [jnp.abs(g - 1), 2 + g // 2 - 2 * (g // 3), 3 - 3 * (g // 2)]
    targets = [g + 1, g - 1, 3 * (g // 2)]

    def pass_on(k, chip):
        return send_chunk(others[k], chip, targets[k], 2)

    outer = jnp.logical_not(inner)

    def recv_group(k, chip_list):
        for chip in chip_list:
            send_chunk(others[k], chip, g, 0).wait_recv()

            @pl.when(inner)
            def _():
                pass_on(k, chip).start()

    pcopy.wait()
    scopy.wait()
    wide = lax.broadcasted_iota(jnp.int32, (1, LANES), 1)
    inverse = jnp.ones((1, LANES), jnp.float32)
    bit = 1
    while bit < dim:
        factor = rope_base ** (-2.0 * bit / HEAD_SIZE)
        inverse = jnp.where(wide // bit % 2 == 1, inverse * factor, inverse)
        bit *= 2
    sign = jnp.where(wide % HEAD_SIZE < dim, -1.0, 1.0)
    own_place = places[g * BPG + c] * pair + p * rows + lax.broadcasted_iota(jnp.int32, (rows, LANES), 0)
    own_angles = own_place.astype(jnp.float32) * inverse
    own_cos, own_sin = jnp.cos(own_angles), jnp.sin(own_angles) * sign
    wait_pieces(0, 2)
    pl.semaphore_wait(barrier, 5 + jnp.minimum(g, 1) + 2 * (c // (chips // 2)))
    send_x(half).start()
    send_y(0).start()
    wait_pieces(6, pieces - 2)
    send_own(s, pn).start()

    @pl.when(g > 0)
    def _():
        pl.semaphore_signal(ready.at[0], inc=1, device_id={"grp": g - 1})

    @pl.when(upper)
    def _():
        for core in range(2):
            pl.semaphore_signal(ready.at[1], inc=1, device_id={"sp": cd * 2 + core})

    own_x = toks[s]
    low = lax.broadcasted_iota(jnp.int32, (rows, LANES), 1) < HEAD_SIZE
    for k in range(chips):
        if k % 2 == 0:
            pltpu.make_async_copy(
                kvw_any.at[:, pl.ds(0, 4 * LANES)], kvw.at[k // 2], wsem.at[2 + k // 2]
            ).wait()
            both = jnp.dot(own_x, kvw[k // 2], preferred_element_type=jnp.float32)
        kv = both[:, k % 2 * 2 * LANES : (k % 2 + 1) * 2 * LANES]
        keys = rotate_heads(kv[:, :LANES], own_cos, own_sin)
        values = kv[:, LANES:]
        first = jnp.where(low, keys, pltpu.roll(values, HEAD_SIZE, 1)).astype(jnp.bfloat16)
        second = jnp.where(low, pltpu.roll(keys, HEAD_SIZE, 1), values).astype(jnp.bfloat16)
        way = ways[k]
        if way == 0:
            mine = p == 0
            kvb[pl.ds(pl.multiple_of(key_base + s * rows, rows), rows), :] = jnp.where(mine, first, second)
            kvo[0] = jnp.where(mine, second, first)
            send_head(0, pn, 0).start()
        else:
            chip = chip_order[k]
            kvo[2 * way - 1] = first
            kvo[2 * way] = second
            if way == 1:
                pl.when(jnp.logical_not(upper))(lambda: pl.semaphore_wait(ready.at[1], 2))
            send_head(2 * way - 1, chip * 2, way).start()
            send_head(2 * way, chip * 2 + 1, way).start()

    for q in range(1, half):
        send_x(half + q).start()
        send_y(q).start()
    for q in range(half):
        send_x(q).start()
        send_y(half + q).start()

    recv_heads(c, 0)
    pl.when(g < grp - 1)(lambda: pl.semaphore_wait(ready.at[0], 1))
    share(c)
    for j in range(BPG):
        rspan = slice(j * pair, (j + 1) * pair)
        within = lax.broadcasted_iota(jnp.int32, (pair, LANES), 0)
        place = places[g * BPG + j] * pair + within
        kpos[rspan, :] = place
        angles = place.astype(jnp.float32) * inverse
        cos_ref[rspan, :] = jnp.cos(angles)
        sin_ref[rspan, :] = jnp.sin(angles) * sign
    block_place = jnp.full((1, LANES), -1, jnp.int32)
    for e in range(blocks):
        block_place = jnp.where(wide == HEAD_SIZE + e, places[e], block_place)

    quarter = rows // 2
    units = [
        [[(c, 0, 0), (c, 0, quarter), (c, 1, 0), (c, 1, quarter)]],
        [[(cx, 0, quarter), (cx, 1, quarter), (cy, 0, 0), (cy, 1, 0)]],
        [[(cx, 0, 0), (cx, 1, 0), (cy, 0, quarter), (cy, 1, quarter)]],
        [[(cd, 0, 0), (cd, 0, quarter), (cd, 1, 0), (cd, 1, quarter)]],
    ]

    def seg_size(u):
        return quarter // len(units[u])

    def seg_rows(ref, seg, count):
        chip, core, off = seg
        return ref[pl.ds(pl.multiple_of(chip * pair + core * rows + off, count), count), :]

    def run(*tasks):
        tasks = list(tasks)
        while tasks:
            for task in list(tasks):
                try:
                    next(task)
                except StopIteration:
                    tasks.remove(task)

    def project(u, part):
        segs, count = units[u][part], seg_size(u)
        size = 4 * count
        x = jnp.concatenate([toks[chip * 2 + core, off : off + count] for chip, core, off in segs], axis=0)
        cosine = jnp.concatenate([seg_rows(cos_ref, seg, count) for seg in segs], axis=0)
        sine = jnp.concatenate([seg_rows(sin_ref, seg, count) for seg in segs], axis=0)
        qf = jnp.dot(x, wq[...], preferred_element_type=jnp.float32)
        yield
        qr = rotate_heads(qf, cosine, sine) * HEAD_SIZE**-0.5
        hidden = jnp.concatenate([
            jnp.broadcast_to(
                jnp.where(block_place > places[g * BPG + chip], neg_large, 0.0), (count, LANES)
            )
            for chip, _, _ in segs
        ], axis=0)
        lower = lax.broadcasted_iota(jnp.int32, (size, LANES), 1) < HEAD_SIZE
        for h in range(qheads):
            v = qr[:, h // 2 * LANES : (h // 2 + 1) * LANES]
            if h % 2:
                v = pltpu.roll(v, HEAD_SIZE, 1)
            base = (part * qheads + h) * size
            qs[u, base : base + size, :] = jnp.where(lower, v, hidden).astype(jnp.bfloat16)
            yield

    def query_places(u, part):
        count = seg_size(u)
        size = 4 * count
        row = lax.broadcasted_iota(jnp.int32, (1, qheads * size), 1) % size
        place = jnp.zeros(row.shape, jnp.int32)
        for i, (chip, core, off) in enumerate(units[u][part]):
            base = places[g * BPG + chip] * pair + core * rows + off
            place = jnp.where(row // count == i, base + row % count, place)
        return place

    def sink_row(u):
        size = 4 * seg_size(u)
        head = lax.broadcasted_iota(jnp.int32, (1, qheads * size), 1) // size
        row = jnp.full(head.shape, sinks[s * qheads], jnp.float32)
        for h in range(1, qheads):
            row = jnp.where(head == h, sinks[s * qheads + h], row)
        return row

    def prepare(k):
        group = g if k == 0 else others[k - 1]
        lane = lax.broadcasted_iota(jnp.int32, (pair, LANES), 1)
        for j in range(chips):
            kv = kvb[pl.ds(pl.multiple_of(group * group_rows + j * pair, pair), pair), :]
            mark = jnp.where(lane == HEAD_SIZE + group * BPG + j, 1.0, 0.0).astype(jnp.bfloat16)
            span = slice(k * group_rows + j * pair, k * group_rows + (j + 1) * pair)
            kaug[span, :] = jnp.where(lane < HEAD_SIZE, kv, mark)
            vt[:, span] = jnp.transpose(kv)[HEAD_SIZE:]

    tops = [[sink_row(u) for _ in units[u]] for u in range(len(units))]

    def joined(rows_of):
        return rows_of[0] if len(rows_of) == 1 else jnp.concatenate(rows_of, axis=1)

    floors = [joined(tops[u]) for u in range(len(units))]

    def part_scores(u, k, part):
        width_of = qheads * 4 * seg_size(u)
        side = slice(part * width_of, (part + 1) * width_of)
        span = slice(k * group_rows, (k + 1) * group_rows)
        whole = lax.dot_general(
            kaug[span, :], qs[u, side, :], (((1,), (1,)), ((), ())), preferred_element_type=jnp.float32
        )
        yield
        for j in range(0, group_rows, pair):
            piece = whole[j : j + pair, :]
            if k == 0:
                seen = jnp.concatenate([kpos[j : j + pair, :]] * (width_of // LANES), axis=1)
                piece = jnp.where(seen <= query_places(u, part), piece, neg_large)
            sbuf[u, k * group_rows + j : k * group_rows + j + pair, side] = piece
            tops[u][part] = jnp.maximum(tops[u][part], jnp.max(piece, axis=0, keepdims=True))
            yield

    def score(u, k):
        for part in range(len(units[u])):
            yield from part_scores(u, k, part)

    bases = [None for _ in units]
    totals = [None for _ in units]

    def absorb(u, stored, fresh, final=False):
        low_key = min(stored + fresh) * group_rows
        high_key = (max(stored + fresh) + 1) * group_rows
        for k in fresh:
            yield from score(u, k)
        top = joined(tops[u])
        factor = None
        if bases[u] is None:
            total = jnp.exp(floors[u] - top)
        else:
            factor = jnp.exp(bases[u] - top)
            total = totals[u] * factor
        for j in range(low_key, high_key, 2 * pair):
            weights = jnp.exp(sbuf[u, j : j + 2 * pair, :] - top)
            pbuf[u, j : j + 2 * pair, :] = weights.astype(jnp.bfloat16)
            total = total + jnp.sum(weights, axis=0, keepdims=True)
            yield
        totals[u], bases[u] = total, top
        mix = jnp.dot(
            vt[:, low_key:high_key], pbuf[u, low_key:high_key, :], preferred_element_type=jnp.float32
        )
        yield
        if factor is not None:
            mix = mix + mbuf[u] * factor
        if not final:
            mbuf[u] = mix
            return
        mix = mix / total
        count = seg_size(u)
        size = 4 * count
        for part in range(len(units[u])):
            tiles = []
            for h in range(0, qheads, LANES // size):
                base = (part * qheads + h) * size
                tile = jnp.transpose(mix[:, base : base + LANES])
                tiles.extend(tile[i : i + size] for i in range(0, LANES, size))
            att = jnp.concatenate(tiles, axis=1).astype(jnp.bfloat16)
            if len(units[u]) == 1:
                abuf[u] = att
                continue
            for i, (_, core, off) in enumerate(units[u][part]):
                abuf[u, core * rows + off : core * rows + off + count, :] = att[i * count : (i + 1) * count]

    def chain(*tasks):
        for task in tasks:
            yield from task

    def send_out(u, i):
        chip, core, off = (cd, i // 2, 0) if u == 3 else units[u][0][i]
        count = rows if u in (0, 3) else quarter
        src = abuf.at[u, pl.ds(i * quarter, count)]
        dst = obuf.at[pl.ds(off, count), pl.ds(pl.multiple_of(s * qc, qc), qc)]
        return pltpu.make_async_remote_copy(
            src_ref=src, dst_ref=dst, send_sem=osend.at[0],
            recv_sem=orecv.at[0], device_id={"sp": chip * 2 + core},
        )

    def send_out_partner():
        src = abuf.at[0, pl.ds(pl.multiple_of((1 - p) * rows, rows), rows)]
        dst = obuf.at[:, pl.ds(pl.multiple_of(s * qc, qc), qc)]
        return pltpu.make_async_remote_copy(
            src_ref=src, dst_ref=dst, send_sem=osend.at[0],
            recv_sem=orecv.at[0], device_id={"sp": pn},
        )

    def wait_out(sem):
        span = pl.ds(0, (sp - 1) * qc)
        pltpu.make_async_remote_copy(
            src_ref=obuf.at[:, span], dst_ref=obuf.at[:, span], send_sem=sem, recv_sem=sem,
            device_id={"sp": pn},
        ).wait_recv()

    def ship(u):
        if u == 0:
            send_out_partner().start()
            obuf[:, pl.ds(pl.multiple_of(s * qc, qc), qc)] = abuf[
                0, pl.ds(pl.multiple_of(p * rows, rows), rows), :
            ]
        elif u == 3:
            send_out(u, 0).start()
            send_out(u, 2).start()
        else:
            for i in range(4):
                send_out(u, i).start()

    def stage(k):
        qx, qy = (k + half) % pieces, k
        arrived(0, qx)
        if k < half:
            relay(qx).start()
        forward(0, qx, k // half).start()
        arrived(1, qy)
        if k < half:
            relay(qy).start()
        forward(1, qy, k // half).start()

    def stage_far(q):
        for r in (q, q + half):
            arrived(2, r)
            forward(2, r, 2).start()

    def partner(i):
        wait_rows(drecv.at[i], 1)

    stage(0)
    partner(3)
    wq_copy.wait()
    run(project(0, 0))
    for chip, way in ((cx, 2), (cy, 3), (cd, 1)):
        recv_heads(chip, way)
        share(chip)
    near, rest = (c,), (cx, cy, cd)
    pl.when(inner)(lambda: recv_group(0, near))
    prepare(0)
    run(score(0, 0))
    pl.when(inner)(lambda: recv_group(1, near))
    stage(1)
    partner(0)
    run(project(1, 0))
    run(score(1, 0))
    pl.when(outer)(lambda: recv_group(0, near))
    recv_group(0, rest)

    @pl.when(inner)
    def _():
        recv_group(1, rest)
        recv_group(2, near)

    stage(2)
    prepare(1)
    run(score(0, 1), score(1, 1))
    stage(3)
    partner(1)
    run(chain(project(2, 0), score(2, 0)), absorb(1, [0, 1], []))
    pl.when(inner)(lambda: recv_group(2, (cx,)))
    run(score(2, 1))
    pl.when(outer)(lambda: recv_group(1, near + rest))
    pl.when(inner)(lambda: recv_group(2, (cy, cd)))
    stage_far(0)
    pl.when(p == 1)(lambda: stage_far(1))
    prepare(2)
    run(absorb(1, [], [2]), score(0, 2), score(2, 2))
    pl.when(p == 0)(lambda: stage_far(1))
    run(absorb(2, [0, 1, 2], []))
    partner(2)
    run(chain(project(3, 0), score(3, 0), score(3, 1), score(3, 2), absorb(3, [0, 1, 2], [])))
    pl.when(outer)(lambda: recv_group(2, near + rest))
    prepare(3)
    run(absorb(3, [], [3], True))
    ship(3)
    run(absorb(1, [], [3], True), absorb(2, [], [3], True))
    ship(1)
    ship(2)
    run(absorb(0, [0, 1, 2], [3], True))
    ship(0)

    wait_out(orecv.at[0])
    out[...] = obuf[...]
    wait_rows(tsend.at[0], sp - 1)
    kept = kvo.at[pl.ds(0, sp - 1)]
    pltpu.make_async_remote_copy(
        src_ref=kept, dst_ref=kept, send_sem=ksend.at[0], recv_sem=ksend.at[0], device_id={"sp": pn}
    ).wait_recv()

    def wait_keys(way, count):
        span = pl.ds(0, count)
        pltpu.make_async_remote_copy(
            src_ref=kvb.at[span], dst_ref=kvb.at[span], send_sem=zsend.at[way],
            recv_sem=zsend.at[way], device_id={"grp": g},
        ).wait_recv()

    pl.when(g > 0)(lambda: wait_keys(1, group_rows))
    pl.when(g < grp - 1)(lambda: wait_keys(0, group_rows))
    pl.when(inner)(lambda: wait_keys(2, 3 * group_rows))
    wait_out(osend.at[0])


def per_plane(tokens, query_weight, key_value_weight, block_places, sinks):
    sp = lax.axis_size("sp")
    grp = lax.axis_size("grp")
    rows, width = tokens.shape
    group_rows = rows * sp
    key_count = grp * group_rows
    qc = query_weight.shape[1]
    qheads = qc // HEAD_SIZE
    pair = 2 * rows
    columns = qheads * pair
    pieces = 4
    hbm = pl.BlockSpec(memory_space=pl.ANY)
    dma = pltpu.SemaphoreType.DMA
    bf16, f32 = jnp.bfloat16, jnp.float32
    result = pl.pallas_call(
        functools.partial(plane_kernel, grp, sp, qheads),
        out_shape=pltpu.VMEM((rows, qc * sp), bf16),
        in_specs=[hbm] * 5,
        out_specs=pl.BlockSpec(memory_space=pltpu.VMEM),
        scratch_shapes=[
            pltpu.SMEM(block_places.shape, block_places.dtype),
            pltpu.SMEM(sinks.shape, sinks.dtype),
            pltpu.VMEM((sp, rows, width), bf16),
            pltpu.VMEM((width, qc), bf16),
            pltpu.VMEM((2, width, 4 * LANES), bf16),
            pltpu.VMEM((sp, rows, LANES), bf16),
            pltpu.VMEM((key_count, LANES), bf16),
            pltpu.VMEM((key_count, LANES), bf16),
            pltpu.VMEM((HEAD_SIZE, key_count), bf16),
            pltpu.VMEM((sp // 2, columns, LANES), bf16),
            pltpu.VMEM((sp // 2, key_count, columns), f32),
            pltpu.VMEM((sp // 2, key_count, columns), bf16),
            pltpu.VMEM((sp // 2, HEAD_SIZE, columns), f32),
            pltpu.VMEM((sp // 2, pair, qc), bf16),
            pltpu.VMEM((rows, qc * sp), bf16),
            pltpu.VMEM((group_rows, LANES), f32),
            pltpu.VMEM((group_rows, LANES), f32),
            pltpu.VMEM((group_rows, LANES), jnp.int32),
            dma((7,)),
            dma((1,)),
            dma((3, pieces)),
            dma((4,)),
            dma((1,)),
            dma((sp // 2,)),
            dma((3,)),
            dma((grp, sp // 2)),
            dma((1,)),
            dma((1,)),
            pltpu.SemaphoreType.REGULAR((2,)),
        ],
        compiler_params=pltpu.CompilerParams(
            has_side_effects=True, collective_id=0, vmem_limit_bytes=60 * 1024 * 1024
        ),
    )(tokens, query_weight, key_value_weight, block_places, sinks)
    return result


def write_out(result, out, sem):
    copy = pltpu.make_async_copy(result, out, sem)
    copy.start()
    copy.wait()


def written(result):
    return pl.pallas_call(
        write_out,
        out_shape=jax.ShapeDtypeStruct(result.shape, result.dtype),
        in_specs=[pl.BlockSpec(memory_space=pltpu.VMEM)],
        out_specs=pl.BlockSpec(memory_space=pl.ANY),
        scratch_shapes=[pltpu.SemaphoreType.DMA],
    )(result)


def local_form(tokens, query_weight, key_value_weight, block_places, sinks):
    sp = lax.axis_size("sp")
    grp = lax.axis_size("grp")
    heads = query_weight.shape[1] // HEAD_SIZE
    kv_total = key_value_weight.shape[1] // (2 * HEAD_SIZE)
    square = sp // 2 == BPG and grp == BPG and kv_total == sp and block_places.shape[0] == grp * BPG
    form = per_plane if square and heads * HEAD_SIZE == 2 * LANES else per_device
    return form(tokens, query_weight, key_value_weight, block_places, sinks)


def solution(mesh):
    in_specs = (P(("grp", "sp"), None), P(None, "sp"), P(), P(), P())
    out_specs = P(("grp", "sp"), None)
    return jax.shard_map(
        local_form, mesh=mesh, in_specs=in_specs, out_specs=out_specs, check_vma=False
    )
```
